32 devices in a mesh: clips: 2 (over x), context: 4 (over y, core), tensor: 4 (over z).
Axes of the slice: x: 2, y: 2, z: 4, core: 2. Of those that a mesh axis runs over, the one named last changes fastest.
Arguments:
- inputs: bfloat16 [2, 2048, 1024], P('clips', 'context'), may hold values from -6 to 6
- gain_first: float32 [1024], replicated, may hold values from 0.5 to 1.5
- first_in: float32 [1024, 4096], P(('clips', 'context'), 'tensor'), may hold values from -0.1875 to 0.1875
- first_out: float32 [4096, 1024], P('tensor', ('clips', 'context')), may hold values from -0.09375 to 0.09375
- gain_attend: float32 [1024], replicated, may hold values from 0.5 to 1.5
- attend_in: float32 [3, 1024, 1024], P(None, ('clips', 'context'), 'tensor'), may hold values from -0.1875 to 0.1875
- attend_out: float32 [1024, 1024], P('tensor', ('clips', 'context')), may hold values from -2 to 2
- relative: float32 [73, 64], replicated, may hold values from -6 to 6
- gain_convolve: float32 [1024], replicated, may hold values from 0.5 to 1.5
- convolve_in: float32 [2, 1024, 1024], P(None, ('clips', 'context'), 'tensor'), may hold values from -0.1875 to 0.1875
- depthwise: float32 [31, 1024], P(None, 'tensor'), may hold values from -1 to 1
- gain_middle: float32 [1024], P('tensor'), may hold values from 0.5 to 1.5
- convolve_out: float32 [1024, 1024], P('tensor', ('clips', 'context')), may hold values from -0.1875 to 0.1875
- gain_second: float32 [1024], replicated, may hold values from 0.5 to 1.5
- second_in: float32 [1024, 4096], P(('clips', 'context'), 'tensor'), may hold values from -0.1875 to 0.1875
- second_out: float32 [4096, 1024], P('tensor', ('clips', 'context')), may hold values from -0.09375 to 0.09375
- gain_final: float32 [1024], replicated, may hold values from 0.5 to 1.5
- cotangent: bfloat16 [2, 2048, 1024], P('clips', 'context'), may hold values from -6 to 6
Outputs:
- layer_out: bfloat16 [2, 2048, 1024], P('clips', 'context')
- grad_inputs: float32 [2, 2048, 1024], P('clips', 'context')
- grad_gain_first: float32 [1024], replicated
- grad_first_in: float32 [1024, 4096], P(('clips', 'context'), 'tensor')
- grad_first_out: float32 [4096, 1024], P('tensor', ('clips', 'context'))
- grad_gain_attend: float32 [1024], replicated
- grad_attend_in: float32 [3, 1024, 1024], P(None, ('clips', 'context'), 'tensor')
- grad_attend_out: float32 [1024, 1024], P('tensor', ('clips', 'context'))
- grad_relative: float32 [73, 64], replicated
- grad_gain_convolve: float32 [1024], replicated
- grad_convolve_in: float32 [2, 1024, 1024], P(None, ('clips', 'context'), 'tensor')
- grad_depthwise: float32 [31, 1024], P(None, 'tensor')
- grad_gain_middle: float32 [1024], P('tensor')
- grad_convolve_out: float32 [1024, 1024], P('tensor', ('clips', 'context'))
- grad_gain_second: float32 [1024], replicated
- grad_second_in: float32 [1024, 4096], P(('clips', 'context'), 'tensor')
- grad_second_out: float32 [4096, 1024], P('tensor', ('clips', 'context'))
- grad_gain_final: float32 [1024], replicated
The draws below stay inside these ranges and needn't reach their ends.
All inputs are finite; a program needn't handle non-finite values.
Results may differ from the reference program's by a relative error of at most 0.035.
Values may be sent and summed in bfloat16 or wider, within the bound.
A program may use at most 128 MiB of HBM per device.

```python
import math
import jax
import jax.numpy as jnp
from jax import lax

D = 1024
HEADS = 16
HEAD_DIM = 64
FF = 4096
KSIZE = 31
LEFT = 64
RIGHT = 8
REL = 73
LENGTH = 2048
CLIPS = 2


def block_scale(own_key, dims, shards, least, high):
    gain = 1.0
    for axis_at, parts in shards:
        draws = jax.random.uniform(jax.random.fold_in(jax.random.fold_in(own_key, 6), axis_at), (parts,), jnp.float32, least / len(shards), high / len(shards))
        gain = gain * jnp.repeat(jnp.exp(draws), dims[axis_at] // parts).reshape((-1,) + (1,) * (len(dims) - 1 - axis_at))
    return gain


def normal_values(key, extent, width, limit, split=(), kind=jnp.bfloat16):
    entries = width * jax.random.normal(key, extent, jnp.float32)
    if split:
        entries = entries * block_scale(key, extent, split, -0.22, 0.18)
    return jnp.clip(entries, -limit, limit).astype(kind)


def setup_inputs(seed: int = 0) -> dict:
    streams_of = jax.random.split(jax.random.key(seed), 19)
    inputs = normal_values(streams_of[0], (CLIPS, LENGTH, D), 1.0, 6.0, ((0, 2), (1, 4)))
    gain_first = jnp.clip(1.0 + 0.1 * jax.random.normal(streams_of[1], (D,), jnp.float32), 0.5, 1.5)
    first_in = normal_values(streams_of[2], (D, FF), D ** -0.5, 0.1875, ((0, 8), (1, 4)), jnp.float32)
    first_out = normal_values(streams_of[3], (FF, D), FF ** -0.5, 0.09375, ((0, 4), (1, 8)), jnp.float32)
    gain_attend = jnp.clip(1.0 + 0.1 * jax.random.normal(streams_of[4], (D,), jnp.float32), 0.5, 1.5)
    attend_in = normal_values(streams_of[5], (3, D, D), D ** -0.5, 0.1875, ((1, 8), (2, 4)), jnp.float32)
    attend_out = normal_values(streams_of[6], (D, D), (max(D // 128, 1)) ** -0.5, 2.0, ((0, 4), (1, 8)), jnp.float32)
    relative = normal_values(streams_of[7], (REL, HEAD_DIM), 1.0, 6.0, (), jnp.float32)
    gain_convolve = jnp.clip(1.0 + 0.1 * jax.random.normal(streams_of[8], (D,), jnp.float32), 0.5, 1.5)
    convolve_in = normal_values(streams_of[9], (2, D, D), D ** -0.5, 0.1875, ((1, 8), (2, 4)), jnp.float32)
    depthwise = normal_values(streams_of[10], (KSIZE, D), KSIZE ** -0.5, 1.0, ((1, 4),), jnp.float32)
    gain_middle = jnp.clip(1.0 + 0.1 * jax.random.normal(streams_of[11], (D,), jnp.float32), 0.5, 1.5)
    convolve_out = normal_values(streams_of[12], (D, D), D ** -0.5, 0.1875, ((0, 4), (1, 8)), jnp.float32)
    gain_second = jnp.clip(1.0 + 0.1 * jax.random.normal(streams_of[13], (D,), jnp.float32), 0.5, 1.5)
    second_in = normal_values(streams_of[14], (D, FF), D ** -0.5, 0.1875, ((0, 8), (1, 4)), jnp.float32)
    second_out = normal_values(streams_of[15], (FF, D), FF ** -0.5, 0.09375, ((0, 4), (1, 8)), jnp.float32)
    gain_final = jnp.clip(1.0 + 0.1 * jax.random.normal(streams_of[16], (D,), jnp.float32), 0.5, 1.5)
    cotangent = normal_values(streams_of[17], (CLIPS, LENGTH, D), 1.0, 6.0, ((0, 2), (1, 4)))
    return {"inputs": inputs, "gain_first": gain_first, "first_in": first_in, "first_out": first_out, "gain_attend": gain_attend, "attend_in": attend_in, "attend_out": attend_out, "relative": relative, "gain_convolve": gain_convolve, "convolve_in": convolve_in, "depthwise": depthwise, "gain_middle": gain_middle, "convolve_out": convolve_out, "gain_second": gain_second, "second_in": second_in, "second_out": second_out, "gain_final": gain_final, "cotangent": cotangent}


epsilon = 1e-05
highest = lax.Precision.HIGHEST

@jax.custom_vjp
def low(v):
    return lax.optimization_barrier(v.astype(jnp.bfloat16)).astype(jnp.float32)

@jax.custom_vjp
def low_back(v):
    return v

def low_keep(v):
    return (low(v), None)

def low_pass(kept, grad):
    return (grad,)

def back_keep(v):
    return (v, None)

def back_low(kept, grad):
    return (low(grad),)
low.defvjp(low_keep, low_pass)
low_back.defvjp(back_keep, back_low)

def matmul(former, latter):
    return jnp.dot(former, latter, precision=highest)

def layer_norm(rows_in, gain_vec):
    row_mean = lax.optimization_barrier(jnp.mean(rows_in, axis=-1, keepdims=True))
    centred = rows_in - row_mean
    variance = lax.optimization_barrier(jnp.mean(centred * centred, axis=-1, keepdims=True))
    return centred * lax.rsqrt(variance + epsilon) * gain_vec

def feed_forward(rows_in, gain_vec, weight_in, weight_out):
    normed = low(layer_norm(rows_in, gain_vec))
    hidden = low_back(matmul(normed, low(weight_in)))
    active = low(jax.nn.silu(hidden))
    return low_back(matmul(active, low(weight_out)))

def attention(rows_in, gain_vec, weight_in, weight_out, relative):
    length = rows_in.shape[0]
    normed = low(layer_norm(rows_in, gain_vec))
    weights = low(weight_in)
    query_heads = low(low_back(matmul(normed, weights[0]))).reshape(length, HEADS, HEAD_DIM)
    key_heads = low(low_back(matmul(normed, weights[1]))).reshape(length, HEADS, HEAD_DIM)
    value_heads = low(low_back(matmul(normed, weights[2]))).reshape(length, HEADS, HEAD_DIM)
    rel_table = low(relative)
    content = jnp.einsum('ihd,jhd->hij', query_heads, key_heads, precision=highest)
    rel_scores = jnp.einsum('ihd,md->him', query_heads, rel_table, precision=highest)
    positions = jnp.arange(length, dtype=jnp.int32)
    distance = jnp.clip(positions[None, :] - positions[:, None], -LEFT, RIGHT) + LEFT
    bin_index = jnp.broadcast_to(distance[None], content.shape)
    rel_bias = jnp.take_along_axis(rel_scores, bin_index, axis=2)
    logits = low_back((content + rel_bias) * (1.0 / math.sqrt(HEAD_DIM)))
    row_max = lax.optimization_barrier(jnp.max(logits, axis=-1, keepdims=True))
    log_total = row_max + jnp.log(lax.optimization_barrier(jnp.sum(jnp.exp(logits - row_max), axis=-1, keepdims=True)))
    attend_prob = low(jnp.exp(logits - log_total))
    mixed = jnp.einsum('hij,jhd->ihd', attend_prob, value_heads, precision=highest)
    mixed = low(low_back(mixed)).reshape(length, D)
    return low_back(matmul(mixed, low(weight_out)))

def convolution(rows_in, gain_vec, weight_in, depthwise, gain_middle, weight_out):
    length = rows_in.shape[0]
    normed = low(layer_norm(rows_in, gain_vec))
    weights = low(weight_in)
    unit_half = low_back(matmul(normed, weights[0]))
    gate_half = low_back(matmul(normed, weights[1]))
    gated = unit_half * jax.nn.sigmoid(gate_half)
    padded = jnp.concatenate([jnp.zeros((KSIZE - 1, D), jnp.float32), gated], axis=0)
    mixed = depthwise[0] * padded[0:length]
    for offset in range(1, KSIZE):
        mixed = mixed + depthwise[offset] * padded[offset:offset + length]
    active = low(jax.nn.silu(layer_norm(mixed, gain_middle)))
    return low_back(matmul(active, low(weight_out)))

def forward(rows_in, gain_first, first_in, first_out, gain_attend, attend_in, attend_out, relative, gain_convolve, convolve_in, depthwise, gain_middle, convolve_out, gain_second, second_in, second_out, gain_final):
    rows_in = rows_in + 0.5 * feed_forward(rows_in, gain_first, first_in, first_out)
    rows_in = rows_in + attention(rows_in, gain_attend, attend_in, attend_out, relative)
    rows_in = rows_in + convolution(rows_in, gain_convolve, convolve_in, depthwise, gain_middle, convolve_out)
    rows_in = rows_in + 0.5 * feed_forward(rows_in, gain_second, second_in, second_out)
    return layer_norm(rows_in, gain_final)

def reference(inputs, gain_first, first_in, first_out, gain_attend, attend_in, attend_out, relative, gain_convolve, convolve_in, depthwise, gain_middle, convolve_out, gain_second, second_in, second_out, gain_final, cotangent):
    params = (gain_first, first_in, first_out, gain_attend, attend_in, attend_out, relative, gain_convolve, convolve_in, depthwise, gain_middle, convolve_out, gain_second, second_in, second_out, gain_final)

    def per_clip(grad_sums, clip_pair):
        one_clip, one_seed = clip_pair
        layer_value, pullback = jax.vjp(forward, one_clip, *params)
        pulled = pullback(one_seed)
        grad_sums = tuple((total + extra for total, extra in zip(grad_sums, pulled[1:])))
        return (grad_sums, (layer_value.astype(jnp.bfloat16), pulled[0]))
    zero_sums = tuple((jnp.zeros_like(entry) for entry in params))
    grad_sums, (layer_out, grad_inputs) = lax.scan(per_clip, zero_sums, (inputs.astype(jnp.float32), cotangent.astype(jnp.float32)))
    return (layer_out, grad_inputs, grad_sums[0], grad_sums[1], grad_sums[2], grad_sums[3], grad_sums[4], grad_sums[5], grad_sums[6], grad_sums[7], grad_sums[8], grad_sums[9], grad_sums[10], grad_sums[11], grad_sums[12], grad_sums[13], grad_sums[14], grad_sums[15])
```

```python
from functools import partial
import math

import jax
import jax.numpy as jnp
from jax import lax
from jax.experimental import pallas as pl
from jax.experimental.pallas import tpu as pltpu
from jax.sharding import PartitionSpec as P

D = 1024
HEAD_DIM = 64
LEFT = 64
RIGHT = 8


epsilon = 1e-05
highest = lax.Precision.HIGHEST


def shifted_2(value, axis, steps):
    count = lax.axis_size(axis)
    initial, last = (max(0, -steps), min(count, count - steps))
    return lax.ppermute(value, axis, [(source, source + steps) for source in range(initial, last)])


def dot_rows(former, latter):
    return jnp.dot(former, latter, preferred_element_type=jnp.float32)


def dot_inner(former, latter):
    return lax.dot_general(
        former, latter, (((0,), (0,)), ((), ())), preferred_element_type=jnp.float32
    )


def dot_outer(former, latter):
    return lax.dot_general(
        former, latter, (((1,), (1,)), ((), ())), preferred_element_type=jnp.float32
    )


def layer_norm(rows_in, gain_vec):
    row_mean = jnp.mean(rows_in, axis=-1, keepdims=True)
    centred = rows_in - row_mean
    variance = jnp.mean(centred * centred, axis=-1, keepdims=True)
    return centred * lax.rsqrt(variance + epsilon) * gain_vec


def norm_back(rows_in, gain_vec, upstream):
    unused, pullback = jax.vjp(layer_norm, rows_in, gain_vec)
    return pullback(upstream)


def gate_unit(unit_half, gate_half):
    return unit_half * jax.nn.sigmoid(gate_half)


def fetch(weight_in, weight_out):
    return (
        lax.all_gather(weight_in.astype(jnp.bfloat16), ("clips", "context"), axis=1, tiled=True),
        lax.all_gather(weight_out.astype(jnp.bfloat16), ("clips", "context"), axis=1, tiled=True),
    )


def weights_back(weight_in, weight_out):
    result_pair = (
        lax.all_gather(weight_in.astype(jnp.bfloat16), ("clips", "context"), axis=1, tiled=True),
        lax.all_gather(weight_out.astype(jnp.bfloat16), ("clips", "context"), axis=1, tiled=True),
    )
    return result_pair


def scatter_sum(grad, axis):
    summed = lax.psum_scatter(
        grad.astype(jnp.bfloat16), ("clips", "context"), scatter_dimension=axis, tiled=True
    )
    return summed.astype(jnp.float32)


def send_grads(grad_in, grad_out):
    return (scatter_sum(grad_in, 1), scatter_sum(grad_out, 1))


def branch_total(partial_sum):
    return lax.psum(partial_sum.astype(jnp.bfloat16), "tensor").astype(jnp.float32)


def input_total(partial_sum):
    return lax.psum(partial_sum.astype(jnp.bfloat16), "tensor").astype(jnp.float32)


def ffn_forward(rows_in, gain_vec, weight_in, weight_out):
    normed = layer_norm(rows_in, gain_vec).astype(jnp.bfloat16)
    hidden = dot_rows(normed, weight_in)
    active = jax.nn.silu(hidden).astype(jnp.bfloat16)
    return (branch_total(dot_rows(active, weight_out)), (normed, hidden, active))


def ffn_backward(rows_in, gain_vec, weight_in, weight_out, saved, upstream):
    normed, hidden, active = saved
    branch_grad = (0.5 * upstream).astype(jnp.bfloat16)
    grad_out = dot_inner(active, branch_grad)
    unused, pullback = jax.vjp(jax.nn.silu, hidden)
    hidden_grad = pullback(dot_outer(branch_grad, weight_out))[0].astype(jnp.bfloat16)
    grad_in = dot_inner(normed, hidden_grad)
    normed_grad = input_total(dot_outer(hidden_grad, weight_in))
    rows_grad, gain_grad = norm_back(rows_in, gain_vec, normed_grad)
    return (upstream + rows_grad, gain_grad, grad_in, grad_out)


QB = 128
BAND = 3 * QB
SPAN = 4 * QB
NT = (((1,), (1,)), ((), ()))


def span_table(relative):
    table = relative.astype(jnp.bfloat16)
    low = jnp.broadcast_to(table[:1], (2 * QB - 1 - LEFT, table.shape[1]))
    high = jnp.broadcast_to(table[-1:], (SPAN - (2 * QB - 1 - LEFT) - table.shape[0], table.shape[1]))
    spread = jnp.concatenate([low, table, high], axis=0)
    return jnp.concatenate([spread, spread], axis=1)


def fill_scores(first_block, q_mask, k_ref, span_ref, s_ref, edge_ref):
    keys = k_ref.shape[0]
    s_ref[:, QB : QB + keys] = lax.dot_general(q_mask, k_ref[...], NT, preferred_element_type=jnp.float32)
    spread = lax.dot_general(q_mask, span_ref[...], NT, preferred_element_type=jnp.float32)
    edge_ref[0] = jnp.broadcast_to(spread[:, :1], (QB, QB))
    edge_ref[1] = jnp.zeros((QB, QB), jnp.float32)
    edge_ref[2] = jnp.broadcast_to(spread[:, SPAN - 1 :], (QB, QB))
    skewed = pltpu.roll(spread, SPAN - (QB - 1), 1, stride=1, stride_axis=0)
    at = pl.ds(pl.multiple_of(first_block * QB, QB), BAND)
    s_ref[:, at] = s_ref[:, at] + skewed[:, :BAND]


def edge_of(block, first_block):
    return jnp.where(block < first_block - 1, 0, jnp.where(block > first_block + 1, 2, 1))


def forward_kernel(pos_ref, q_ref, k_ref, v_ref, span_ref, o_ref, lse_ref, s_ref, edge_ref, p_ref):
    keys = k_ref.shape[0]
    blocks = keys // QB
    first_block = pos_ref[0] * pl.num_programs(1) + pl.program_id(1)
    lane = lax.broadcasted_iota(jnp.int32, (QB, 2 * HEAD_DIM), 1)
    outs, lses = [], []
    for half in range(2):
        mine = (lane < HEAD_DIM) if half == 0 else (lane >= HEAD_DIM)
        q_mask = jnp.where(mine, q_ref[...], jnp.zeros_like(q_ref))
        fill_scores(first_block, q_mask, k_ref, span_ref, s_ref, edge_ref)
        top = None
        for block in range(blocks):
            z = s_ref[:, (block + 1) * QB : (block + 2) * QB] + edge_ref[edge_of(block, first_block)]
            top = z if top is None else jnp.maximum(top, z)
        top = jnp.max(top, axis=1, keepdims=True)
        edge_ref[...] = edge_ref[...] - top[None]
        total = None
        for block in range(blocks):
            z = s_ref[:, (block + 1) * QB : (block + 2) * QB] + edge_ref[edge_of(block, first_block)]
            p = jnp.exp(z)
            total = p if total is None else total + p
            p_ref[:, block * QB : (block + 1) * QB] = p.astype(jnp.bfloat16)
        total = jnp.sum(total, axis=1, keepdims=True)
        out = jnp.dot(p_ref[...], v_ref[...], preferred_element_type=jnp.float32) / total
        outs.append(out)
        lses.append(jnp.broadcast_to(top + jnp.log(total), (QB, 2 * HEAD_DIM)))
    low = lane < HEAD_DIM
    o_ref[...] = jnp.where(low, outs[0], outs[1]).astype(o_ref.dtype)
    lse_ref[...] = jnp.where(low, lses[0], lses[1])


def attention_forward(position, q, k, v, span):
    rows, width = q.shape
    keys = k.shape[0]
    pairs = width // (2 * HEAD_DIM)
    two = 2 * HEAD_DIM
    row_spec = pl.BlockSpec((QB, two), lambda p, b, pos: (b, p))
    key_spec = pl.BlockSpec((keys, two), lambda p, b, pos: (0, p))
    return pl.pallas_call(
        forward_kernel,
        out_shape=(
            jax.ShapeDtypeStruct((rows, width), jnp.bfloat16),
            jax.ShapeDtypeStruct((rows, width), jnp.float32),
        ),
        grid_spec=pltpu.PrefetchScalarGridSpec(
            num_scalar_prefetch=1,
            grid=(pairs, rows // QB),
            in_specs=[row_spec, key_spec, key_spec, pl.BlockSpec((SPAN, two), lambda p, b, pos: (0, 0))],
            out_specs=(row_spec, row_spec),
            scratch_shapes=[
                pltpu.VMEM((QB, keys + 2 * QB), jnp.float32),
                pltpu.VMEM((3, QB, QB), jnp.float32),
                pltpu.VMEM((QB, keys), jnp.bfloat16),
            ],
        ),
        compiler_params=pltpu.CompilerParams(vmem_limit_bytes=40 << 20),
        cost_estimate=pl.CostEstimate(flops=8 * rows * keys * width, bytes_accessed=4 * (keys + rows) * width, transcendentals=0),
        name="attention_forward",
    )(position.reshape(1), q, k, v, span)


def backward_kernel(pos_ref, q_ref, qt_ref, g_ref, gt_ref, o_ref, lse_ref, k_ref, v_ref, span_ref,
                    dq_ref, dkt_ref, dvt_ref, bins_ref, ends_ref,
                    s_ref, edge_ref, d_ref, p_ref, z_ref, wide_ref, dk_acc, dv_acc):
    keys = k_ref.shape[0]
    blocks = keys // QB
    step = pl.program_id(1)
    first_block = pos_ref[0] * pl.num_programs(1) + step
    lane = lax.broadcasted_iota(jnp.int32, (QB, 2 * HEAD_DIM), 1)

    @pl.when((pl.program_id(0) == 0) & (step == 0))
    def _():
        bins_ref[...] = jnp.zeros_like(bins_ref)
        ends_ref[...] = jnp.zeros_like(ends_ref)

    @pl.when(step == 0)
    def _():
        dk_acc[...] = jnp.zeros_like(dk_acc)
        dv_acc[...] = jnp.zeros_like(dv_acc)
        wide_ref[:, : 2 * HEAD_DIM] = k_ref[...]

    @pl.when((pl.program_id(0) == 0) & (step == 0))
    def _():
        z_ref[:, :QB] = jnp.zeros((QB, QB), jnp.bfloat16)
        z_ref[:, QB + keys :] = jnp.zeros((QB, QB), jnp.bfloat16)

    row_at = lax.broadcasted_iota(jnp.int32, (keys, QB), 0)
    col_at = lax.broadcasted_iota(jnp.int32, (keys, QB), 1)
    below = (row_at < (first_block - 1) * QB) & (col_at == 0)
    above = (row_at >= (first_block + 2) * QB) & (col_at == 1)
    wide_ref[:, 2 * HEAD_DIM :] = jnp.where(below | above, 1.0, 0.0).astype(jnp.bfloat16)

    flip_at = lax.broadcasted_iota(jnp.int32, (QB, QB), 0) + lax.broadcasted_iota(jnp.int32, (QB, QB), 1)
    flip = jnp.where(flip_at == QB - 1, 1.0, 0.0).astype(jnp.bfloat16)
    dqs = []
    for half in range(2):
        rows = slice(half * HEAD_DIM, (half + 1) * HEAD_DIM)
        mine = (lane < HEAD_DIM) if half == 0 else (lane >= HEAD_DIM)
        q_mask = jnp.where(mine, q_ref[...], jnp.zeros_like(q_ref))
        g_mask = jnp.where(mine, g_ref[...], jnp.zeros_like(g_ref))
        fill_scores(first_block, q_mask, k_ref, span_ref, s_ref, edge_ref)
        d_ref[...] = lax.dot_general(g_mask, v_ref[...], NT, preferred_element_type=jnp.float32)
        delta = jnp.sum(g_mask.astype(jnp.float32) * o_ref[...].astype(jnp.float32), axis=1, keepdims=True)
        lse = lse_ref[:, half * HEAD_DIM : half * HEAD_DIM + 1]
        edge_ref[...] = edge_ref[...] - lse[None]
        delta = jnp.broadcast_to(delta, (QB, QB))
        for block in range(blocks):
            here = slice(block * QB, (block + 1) * QB)
            there = slice((block + 1) * QB, (block + 2) * QB)
            p = jnp.exp(s_ref[:, there] + edge_ref[edge_of(block, first_block)])
            p_ref[:, here] = p.astype(jnp.bfloat16)
            z_ref[:, there] = (p * (d_ref[:, here] - delta)).astype(jnp.bfloat16)
        z_all = z_ref[:, QB : QB + keys]
        dv_acc[rows] += jnp.dot(gt_ref[rows], p_ref[...], preferred_element_type=jnp.float32)
        dk_acc[rows] += jnp.dot(qt_ref[rows], z_all, preferred_element_type=jnp.float32)
        dq = jnp.dot(z_all, wide_ref[...], preferred_element_type=jnp.float32)
        at = pl.ds(pl.multiple_of(first_block * QB, QB), BAND)
        band = jnp.dot(flip, z_ref[:, at], preferred_element_type=jnp.float32)
        band = jnp.concatenate([band, jnp.zeros((QB, SPAN - BAND), jnp.float32)], axis=1)
        spread = pltpu.roll(band, 0, 1, stride=1, stride_axis=0).astype(jnp.bfloat16)
        spread = jnp.dot(flip, spread, preferred_element_type=jnp.float32).astype(jnp.bfloat16)
        dq_rel = jnp.dot(spread, span_ref[...], preferred_element_type=jnp.float32)
        below_sum = dq[:, 2 * HEAD_DIM : 2 * HEAD_DIM + 1]
        above_sum = dq[:, 2 * HEAD_DIM + 1 : 2 * HEAD_DIM + 2]
        span_low = span_ref[:1, :].astype(jnp.float32)
        span_high = span_ref[SPAN - 1 :, :].astype(jnp.float32)
        dqs.append(dq[:, : 2 * HEAD_DIM] + dq_rel + below_sum * span_low + above_sum * span_high)
        bins_ref[...] += jnp.dot(qt_ref[rows], spread, preferred_element_type=jnp.float32)
        q_wide = q_mask.astype(jnp.float32)
        ends_ref[0:1, :] += jnp.sum(q_wide * below_sum, axis=0, keepdims=True)
        ends_ref[1:2, :] += jnp.sum(q_wide * above_sum, axis=0, keepdims=True)
    scale = 1.0 / 8.0
    dq_ref[...] = (jnp.where(lane < HEAD_DIM, dqs[0], dqs[1]) * scale).astype(dq_ref.dtype)

    @pl.when(step == pl.num_programs(1) - 1)
    def _():
        dkt_ref[...] = dk_acc[...].astype(dkt_ref.dtype)
        dvt_ref[...] = dv_acc[...].astype(dvt_ref.dtype)


def attention_backward(position, q, q_t, g, g_t, o, lse, k, v, span):
    rows, width = q.shape
    keys = k.shape[0]
    pairs = width // (2 * HEAD_DIM)
    two = 2 * HEAD_DIM
    row_spec = pl.BlockSpec((QB, two), lambda p, b, pos: (b, p))
    col_spec = pl.BlockSpec((two, QB), lambda p, b, pos: (p, b))
    key_spec = pl.BlockSpec((keys, two), lambda p, b, pos: (0, p))
    keyt_spec = pl.BlockSpec((two, keys), lambda p, b, pos: (p, 0))
    fixed = lambda shape: pl.BlockSpec(shape, lambda p, b, pos: (0, 0))
    dq, dkt, dvt, bins, ends = pl.pallas_call(
        backward_kernel,
        out_shape=(
            jax.ShapeDtypeStruct((rows, width), jnp.bfloat16),
            jax.ShapeDtypeStruct((width, keys), jnp.bfloat16),
            jax.ShapeDtypeStruct((width, keys), jnp.bfloat16),
            jax.ShapeDtypeStruct((HEAD_DIM, SPAN), jnp.float32),
            jax.ShapeDtypeStruct((8, two), jnp.float32),
        ),
        grid_spec=pltpu.PrefetchScalarGridSpec(
            num_scalar_prefetch=1,
            grid=(pairs, rows // QB),
            in_specs=[row_spec, col_spec, row_spec, col_spec, row_spec, row_spec, key_spec, key_spec, fixed((SPAN, two))],
            out_specs=(row_spec, keyt_spec, keyt_spec, fixed((HEAD_DIM, SPAN)), fixed((8, two))),
            scratch_shapes=[
                pltpu.VMEM((QB, keys + 2 * QB), jnp.float32),
                pltpu.VMEM((3, QB, QB), jnp.float32),
                pltpu.VMEM((QB, keys), jnp.float32),
                pltpu.VMEM((QB, keys), jnp.bfloat16),
                pltpu.VMEM((QB, keys + 2 * QB), jnp.bfloat16),
                pltpu.VMEM((keys, 2 * two), jnp.bfloat16),
                pltpu.VMEM((two, keys), jnp.float32),
                pltpu.VMEM((two, keys), jnp.float32),
            ],
        ),
        compiler_params=pltpu.CompilerParams(vmem_limit_bytes=40 << 20),
        cost_estimate=pl.CostEstimate(flops=20 * rows * keys * width, bytes_accessed=8 * (keys + rows) * width, transcendentals=0),
        name="attention_backward",
    )(position.reshape(1), q, q_t, g, g_t, o, lse, k, v, span)
    at = 2 * QB - 1 - LEFT
    ends = ends[:2, :HEAD_DIM] + ends[:2, HEAD_DIM:]
    spread = bins.T
    inner = spread[at + 1 : at + LEFT + RIGHT]
    low = jnp.sum(spread[: at + 1], axis=0) + ends[0]
    high = jnp.sum(spread[at + LEFT + RIGHT :], axis=0) + ends[1]
    table = jnp.concatenate([low[None], inner, high[None]], axis=0)
    return dq, dkt, dvt, table


def attend_forward(rows_in, gain_vec, weight_in, weight_out, relative, position):
    normed = layer_norm(rows_in, gain_vec).astype(jnp.bfloat16)
    projected = jnp.einsum(
        "td,kde->kte", normed, weight_in, preferred_element_type=jnp.float32
    ).astype(jnp.bfloat16)
    key_rows, value_rows = (
        lax.all_gather(projected[1], "context", axis=0, tiled=True),
        lax.all_gather(projected[2], "context", axis=0, tiled=True),
    )
    queries = projected[0] * jnp.bfloat16(1.0 / math.sqrt(HEAD_DIM))
    span = span_table(relative)
    mixed, log_total = attention_forward(position, queries, key_rows, value_rows, span)
    return (
        branch_total(dot_rows(mixed, weight_out)),
        (normed, queries, key_rows, value_rows, log_total, mixed, span),
    )


def attend_backward(weight_in, weight_out, relative, position, saved, upstream):
    normed, queries, key_rows, value_rows, log_total, mixed, span = saved
    branch_grad = upstream.astype(jnp.bfloat16)
    grad_out = dot_inner(mixed, branch_grad)
    mixed_grad = dot_outer(branch_grad, weight_out).astype(jnp.bfloat16)
    query_grad, key_grad, value_grad, table_grad = attention_backward(
        position, queries, queries.T, mixed_grad, mixed_grad.T, mixed, log_total, key_rows, value_rows, span
    )
    key_grad = lax.psum_scatter(key_grad, "context", scatter_dimension=1, tiled=True)
    value_grad = lax.psum_scatter(value_grad, "context", scatter_dimension=1, tiled=True)
    stacked = jnp.stack([query_grad, key_grad.T, value_grad.T])
    grad_in = jnp.einsum("td,kte->kde", normed, stacked, preferred_element_type=jnp.float32)
    partial_sum = jnp.einsum("kte,kde->td", stacked, weight_in, preferred_element_type=jnp.float32)
    return (partial_sum, table_grad, grad_in, grad_out)


def conv_forward(rows_in, gain_vec, weight_in, weight_out, depthwise, gain_middle):
    normed = layer_norm(rows_in, gain_vec).astype(jnp.bfloat16)
    projected = jnp.einsum("td,kde->kte", normed, weight_in, preferred_element_type=jnp.float32)
    gated = gate_unit(projected[0], projected[1])
    rows_here = gated.shape[0]
    reach_rows = depthwise.shape[0] - 1
    edge_rows = shifted_2(gated[rows_here - reach_rows :], "context", 1)
    padded = jnp.concatenate([edge_rows, gated], axis=0)
    mixed = depthwise[0] * padded[0:rows_here]
    for offset in range(1, reach_rows + 1):
        mixed = mixed + depthwise[offset] * padded[offset : offset + rows_here]
    row_sums, row_squares = lax.psum(
        (jnp.sum(mixed, axis=1), jnp.sum(mixed * mixed, axis=1)), "tensor"
    )
    row_mean = row_sums / D
    inverse = lax.rsqrt(row_squares / D - row_mean * row_mean + epsilon)
    scaled = (mixed - row_mean[:, None]) * inverse[:, None]
    shaped = scaled * gain_middle
    active = jax.nn.silu(shaped).astype(jnp.bfloat16)
    return (
        branch_total(dot_rows(active, weight_out)),
        (normed, projected, padded, scaled, inverse, shaped, active),
    )


def conv_backward(weight_in, weight_out, depthwise, gain_middle, saved, upstream):
    normed, projected, padded, scaled, inverse, shaped, active = saved
    rows_here, channels = scaled.shape
    reach_rows = depthwise.shape[0] - 1
    branch_grad = upstream.astype(jnp.bfloat16)
    grad_out = dot_inner(active, branch_grad)
    unused, pullback = jax.vjp(jax.nn.silu, shaped)
    shaped_grad = pullback(dot_outer(branch_grad, weight_out))[0]
    middle_grad = jnp.sum(shaped_grad * scaled, axis=0)
    scaled_grad = shaped_grad * gain_middle
    first_sum, second_sum = lax.psum(
        (jnp.sum(scaled_grad, axis=1), jnp.sum(scaled_grad * scaled, axis=1)), "tensor"
    )
    mixed_grad = inverse[:, None] * (
        scaled_grad - first_sum[:, None] / D - scaled * (second_sum[:, None] / D)
    )
    padded_grad = jnp.zeros((rows_here + reach_rows, channels), jnp.float32)
    for offset in range(reach_rows + 1):
        padded_grad = padded_grad.at[offset : offset + rows_here].add(
            depthwise[offset] * mixed_grad
        )
    depth_grad = jnp.stack(
        [
            jnp.sum(padded[offset : offset + rows_here] * mixed_grad, axis=0)
            for offset in range(reach_rows + 1)
        ]
    )
    back_rows = shifted_2(padded_grad[:reach_rows], "context", -1)
    gated_grad = padded_grad[reach_rows:] + jnp.pad(
        back_rows, ((rows_here - reach_rows, 0), (0, 0))
    )
    unused, pullback = jax.vjp(gate_unit, projected[0], projected[1])
    unit_grad, gate_grad = pullback(gated_grad)
    stacked = jnp.stack([unit_grad, gate_grad]).astype(jnp.bfloat16)
    grad_in = jnp.einsum("td,kte->kde", normed, stacked, preferred_element_type=jnp.float32)
    partial_sum = jnp.einsum("kte,kde->td", stacked, weight_in, preferred_element_type=jnp.float32)
    return (partial_sum, grad_in, grad_out, middle_grad, depth_grad)


def local(
    inputs,
    gain_first,
    first_in,
    first_out,
    gain_attend,
    attend_in,
    attend_out,
    relative,
    gain_convolve,
    convolve_in,
    depthwise,
    gain_middle,
    convolve_out,
    gain_second,
    second_in,
    second_out,
    gain_final,
    cotangent,
):
    position = lax.axis_index("context")
    start_rows = inputs[0].astype(jnp.float32)
    first_pair = fetch(first_in[None], first_out)
    branch_out, first_saved = ffn_forward(start_rows, gain_first, first_pair[0][0], first_pair[1])
    after_first = start_rows + 0.5 * branch_out
    attend_pair = fetch(attend_in, attend_out)
    branch_out, attend_saved = attend_forward(
        after_first, gain_attend, attend_pair[0], attend_pair[1], relative, position
    )
    after_attend = after_first + branch_out
    convolve_pair = fetch(convolve_in, convolve_out)
    branch_out, convolve_saved = conv_forward(
        after_attend, gain_convolve, convolve_pair[0], convolve_pair[1], depthwise, gain_middle
    )
    after_convolve = after_attend + branch_out
    second_pair = fetch(second_in[None], second_out)
    branch_out, second_saved = ffn_forward(
        after_convolve, gain_second, second_pair[0][0], second_pair[1]
    )
    after_second = after_convolve + 0.5 * branch_out
    final_out, pullback = jax.vjp(layer_norm, after_second, gain_final)
    upstream, grad_final = pullback(cotangent[0].astype(jnp.float32))
    second_pair = weights_back(second_in[None], second_out)
    upstream, grad_gain_second, grad_in, grad_out = ffn_backward(
        after_convolve, gain_second, second_pair[0][0], second_pair[1], second_saved, upstream
    )
    second_grads = send_grads(grad_in[None], grad_out)
    convolve_pair = weights_back(convolve_in, convolve_out)
    partial_sum, grad_in, grad_out, grad_middle, grad_depth = conv_backward(
        convolve_pair[0], convolve_pair[1], depthwise, gain_middle, convolve_saved, upstream
    )
    rows_grad, grad_gain_convolve = norm_back(after_attend, gain_convolve, input_total(partial_sum))
    upstream = upstream + rows_grad
    convolve_grads = send_grads(grad_in, grad_out)
    attend_pair = weights_back(attend_in, attend_out)
    partial_sum, table_grad, grad_in, grad_out = attend_backward(
        attend_pair[0], attend_pair[1], relative, position, attend_saved, upstream
    )
    normed_grad, table_grad = (
        lax.psum(partial_sum.astype(jnp.bfloat16), "tensor").astype(jnp.float32),
        lax.psum(table_grad.astype(jnp.bfloat16), "tensor").astype(jnp.float32),
    )
    rows_grad, grad_gain_attend = norm_back(after_first, gain_attend, normed_grad)
    upstream = upstream + rows_grad
    attend_grads = send_grads(grad_in, grad_out)
    first_pair = weights_back(first_in[None], first_out)
    upstream, grad_gain_first, grad_in, grad_out = ffn_backward(
        start_rows, gain_first, first_pair[0][0], first_pair[1], first_saved, upstream
    )
    first_grads = send_grads(grad_in[None], grad_out)
    smalls = lax.psum(
        (
            grad_gain_first,
            grad_gain_attend,
            table_grad,
            grad_gain_convolve,
            grad_depth,
            grad_middle,
            grad_gain_second,
            grad_final,
        ),
        ("clips", "context"),
    )
    return (
        final_out.astype(jnp.bfloat16)[None],
        upstream[None],
        smalls[0],
        first_grads[0][0],
        first_grads[1],
        smalls[1],
        attend_grads[0],
        attend_grads[1],
        smalls[2],
        smalls[3],
        convolve_grads[0],
        smalls[4],
        smalls[5],
        convolve_grads[1],
        smalls[6],
        second_grads[0][0],
        second_grads[1],
        smalls[7],
    )


def solution(mesh):
    placed = (
        P("clips", "context", None),
        P(),
        P(("clips", "context"), "tensor"),
        P("tensor", ("clips", "context")),
        P(),
        P(None, ("clips", "context"), "tensor"),
        P("tensor", ("clips", "context")),
        P(),
        P(),
        P(None, ("clips", "context"), "tensor"),
        P(None, "tensor"),
        P("tensor"),
        P("tensor", ("clips", "context")),
        P(),
        P(("clips", "context"), "tensor"),
        P("tensor", ("clips", "context")),
        P(),
        P("clips", "context", None),
    )
    return jax.shard_map(
        local,
        mesh=mesh,
        in_specs=placed,
        out_specs=(
            P("clips", "context", None),
            P("clips", "context", None),
            P(),
            P(("clips", "context"), "tensor"),
            P("tensor", ("clips", "context")),
            P(),
            P(None, ("clips", "context"), "tensor"),
            P("tensor", ("clips", "context")),
            P(),
            P(),
            P(None, ("clips", "context"), "tensor"),
            P(None, "tensor"),
            P("tensor"),
            P("tensor", ("clips", "context")),
            P(),
            P(("clips", "context"), "tensor"),
            P("tensor", ("clips", "context")),
            P(),
        ),
        check_vma=False,
    )
```

```python
import math

import jax
import jax.numpy as jnp
from jax import lax
from jax.experimental import pallas as pl
from jax.experimental.pallas import tpu as pltpu
from jax.sharding import PartitionSpec as P

D = 1024
HEAD_DIM = 64
LEFT = 64
RIGHT = 8

epsilon = 1e-05


def shifted_2(value, axis, steps):
    count = lax.axis_size(axis)
    initial, last = (max(0, -steps), min(count, count - steps))
    return lax.ppermute(value, axis, [(source, source + steps) for source in range(initial, last)])


def dot_rows(former, latter):
    return jnp.dot(former, latter, preferred_element_type=jnp.float32)


def dot_inner(former, latter):
    return lax.dot_general(
        former, latter, (((0,), (0,)), ((), ())), preferred_element_type=jnp.float32
    )


def dot_outer(former, latter):
    return lax.dot_general(
        former, latter, (((1,), (1,)), ((), ())), preferred_element_type=jnp.float32
    )


def layer_norm(rows_in, gain_vec):
    row_mean = jnp.mean(rows_in, axis=-1, keepdims=True)
    centred = rows_in - row_mean
    variance = jnp.mean(centred * centred, axis=-1, keepdims=True)
    return centred * lax.rsqrt(variance + epsilon) * gain_vec


def gate_unit(unit_half, gate_half):
    return unit_half * jax.nn.sigmoid(gate_half)


def fetch(weight_in, weight_out):
    return (
        lax.all_gather(weight_in.astype(jnp.bfloat16), ("clips", "context"), axis=1, tiled=True),
        lax.all_gather(weight_out.astype(jnp.bfloat16), ("clips", "context"), axis=1, tiled=True),
    )


def scatter_sum(grad, axis):
    summed = lax.psum_scatter(
        grad.astype(jnp.bfloat16), ("clips", "context"), scatter_dimension=axis, tiled=True
    )
    return summed.astype(jnp.float32)


def send_grads(grad_in, grad_out):
    return (scatter_sum(grad_in, 1), scatter_sum(grad_out, 1))


MESH_ID = pl.DeviceIdType.MESH
CHUNKS = 32
LAG = 5


def line_sum(axis, partial_ref, acc_ref, from_end, from_mid, total_ref, send_sem, recv_sem, finish):
    at = lax.axis_index(axis)
    low = at < 2
    end = jnp.where(low, 0, 3)
    mid = jnp.where(low, 1, 2)
    other = jnp.where(low, 2, 1)
    is_mid = at == mid
    size = partial_ref.shape[0] // CHUNKS

    def rows(chunk):
        return pl.ds(pl.multiple_of(chunk * size, size), size)

    def hop(stage, chunk, source, target, device):
        return pltpu.make_async_remote_copy(
            src_ref=source.at[rows(chunk)],
            dst_ref=target.at[rows(chunk)],
            send_sem=send_sem.at[stage, chunk],
            recv_sem=recv_sem.at[stage, chunk],
            device_id={axis: device},
            device_id_type=MESH_ID,
        )

    inward = lambda chunk: hop(0, chunk, partial_ref, from_end, mid)
    across = lambda chunk: hop(1, chunk, acc_ref, from_mid, other)
    outward = lambda chunk: hop(2, chunk, total_ref, total_ref, end)
    barrier = pltpu.get_barrier_semaphore()

    def loop(low, high, body):
        def step(chunk, carry):
            body(chunk)
            return carry
        lax.fori_loop(low, high, step, 0)

    @pl.when(is_mid)
    def _():
        pl.semaphore_signal(barrier, inc=1, device_id={axis: end}, device_id_type=MESH_ID)
        pl.semaphore_signal(barrier, inc=1, device_id={axis: other}, device_id_type=MESH_ID)
        pl.semaphore_wait(barrier, 2)

        def first(chunk):
            inward(chunk).wait_recv()
            here = rows(chunk)
            acc_ref[here] = (partial_ref[here].astype(jnp.float32) + from_end[here].astype(jnp.float32)).astype(acc_ref.dtype)
            across(chunk).start()

        def second(chunk):
            across(chunk).wait_recv()
            here = rows(chunk)
            total_ref[here] = (acc_ref[here].astype(jnp.float32) + from_mid[here].astype(jnp.float32)).astype(total_ref.dtype)
            outward(chunk).start()
            finish(here)

        def both(chunk):
            first(chunk)
            second(chunk - LAG)

        loop(0, LAG, first)
        loop(LAG, CHUNKS, both)
        loop(CHUNKS - LAG, CHUNKS, second)

        def drain(chunk):
            across(chunk).wait_send()
            outward(chunk).wait_send()

        loop(0, CHUNKS, drain)

    @pl.when(jnp.logical_not(is_mid))
    def _():
        pl.semaphore_signal(barrier, inc=1, device_id={axis: mid}, device_id_type=MESH_ID)
        pl.semaphore_wait(barrier, 1)
        loop(0, CHUNKS, lambda chunk: inward(chunk).start())

        def receive(chunk):
            outward(chunk).wait_recv()
            finish(rows(chunk))

        loop(0, CHUNKS, receive)
        loop(0, CHUNKS, lambda chunk: inward(chunk).wait_send())


def unit_rows(rows_in):
    mean = jnp.mean(rows_in, axis=-1, keepdims=True)
    centred = rows_in - mean
    variance = jnp.mean(centred * centred, axis=-1, keepdims=True)
    inverse = lax.rsqrt(variance + epsilon)
    return centred * inverse, inverse


def rows_back(unit, inverse, scaled):
    return inverse * (
        scaled
        - jnp.mean(scaled, axis=-1, keepdims=True)
        - unit * jnp.mean(scaled * unit, axis=-1, keepdims=True)
    )


def gather_eight(value):
    total = value[:8]
    for at in range(8, value.shape[0], 8):
        total = total + value[at : at + 8]
    return total


def sum_call(body, name, cid, partial, operands, outs):
    rows, width = partial.shape
    chunk_shape = pltpu.VMEM((rows, width), jnp.bfloat16)
    vmem = pl.BlockSpec(memory_space=pltpu.VMEM)

    def kernel(partial_ref, *refs):
        ins, results = refs[: len(operands)], refs[len(operands) : len(operands) + len(outs)]
        acc, from_end, from_mid, total, send_sem, recv_sem = refs[len(operands) + len(outs) :]
        start, finish = body(total, ins, results)
        start()
        line_sum("tensor", partial_ref, acc, from_end, from_mid, total, send_sem, recv_sem, finish)

    return pl.pallas_call(
        kernel,
        out_shape=tuple(jax.ShapeDtypeStruct(shape, kind) for shape, kind in outs),
        in_specs=[vmem] * (1 + len(operands)),
        out_specs=(vmem,) * len(outs),
        scratch_shapes=[chunk_shape] * 4
        + [pltpu.SemaphoreType.DMA((3, CHUNKS)), pltpu.SemaphoreType.DMA((3, CHUNKS))],
        compiler_params=pltpu.CompilerParams(collective_id=cid, has_side_effects=True, vmem_limit_bytes=40 << 20),
        cost_estimate=pl.CostEstimate(flops=60_000_000_000, bytes_accessed=100_000_000, transcendentals=0),
        name=name,
    )(partial, *operands)


def forward_sum(cid, partial, rows_in, gain, scale):
    def body(total, ins, results):
        x_ref, gain_ref = ins
        x_out, a_out = results

        def finish(here):
            x = x_ref[here].astype(jnp.float32) + scale * total[here].astype(jnp.float32)
            x_out[here] = x
            a_out[here] = (unit_rows(x)[0] * gain_ref[...]).astype(a_out.dtype)

        return lambda: None, finish

    shape = partial.shape
    return sum_call(body, f"forward_sum_{cid}", cid, partial, (rows_in, gain.reshape(1, -1)), ((shape, jnp.float32), (shape, jnp.bfloat16)))


def turn_sum(cid, partial, rows_in, gain, cotangent):
    def body(total, ins, results):
        x_ref, gain_ref, cot_ref = ins
        out_ref, d_ref, half_ref, gain_grad_ref = results

        def start():
            gain_grad_ref[...] = jnp.zeros_like(gain_grad_ref)

        def finish(here):
            x = x_ref[here] + 0.5 * total[here].astype(jnp.float32)
            unit, inverse = unit_rows(x)
            out_ref[here] = (unit * gain_ref[...]).astype(out_ref.dtype)
            upstream = cot_ref[here].astype(jnp.float32)
            d = rows_back(unit, inverse, upstream * gain_ref[...])
            d_ref[here] = d
            half_ref[here] = (0.5 * d).astype(half_ref.dtype)
            gain_grad_ref[...] += gather_eight(upstream * unit)

        return start, finish

    shape = partial.shape
    out, d, half, gain_grad = sum_call(
        body, f"turn_sum_{cid}", cid, partial, (rows_in, gain.reshape(1, -1), cotangent),
        ((shape, jnp.bfloat16), (shape, jnp.float32), (shape, jnp.bfloat16), ((8, shape[1]), jnp.float32)),
    )
    return out, d, half, jnp.sum(gain_grad, axis=0)


def backward_sum(cid, partial, rows_in, gain, upstream, scale):
    def body(total, ins, results):
        x_ref, gain_ref, up_ref = ins
        d_ref, half_ref, gain_grad_ref = results

        def start():
            gain_grad_ref[...] = jnp.zeros_like(gain_grad_ref)

        def finish(here):
            unit, inverse = unit_rows(x_ref[here].astype(jnp.float32))
            normed_grad = total[here].astype(jnp.float32)
            d = up_ref[here] + rows_back(unit, inverse, normed_grad * gain_ref[...])
            d_ref[here] = d
            half_ref[here] = (scale * d).astype(half_ref.dtype)
            gain_grad_ref[...] += gather_eight(normed_grad * unit)

        return start, finish

    shape = partial.shape
    d, half, gain_grad = sum_call(
        body, f"backward_sum_{cid}", cid, partial, (rows_in, gain.reshape(1, -1), upstream),
        ((shape, jnp.float32), (shape, jnp.bfloat16), ((8, shape[1]), jnp.float32)),
    )
    return d, half, jnp.sum(gain_grad, axis=0)


def feed(normed, weight_in, weight_out):
    hidden = dot_rows(normed, weight_in)
    active = jax.nn.silu(hidden).astype(jnp.bfloat16)
    return dot_rows(active, weight_out).astype(jnp.bfloat16), (normed, hidden, active)


def feed_back(weight_in, weight_out, saved, branch_grad):
    normed, hidden, active = saved
    grad_out = dot_inner(active, branch_grad)
    unused, pullback = jax.vjp(jax.nn.silu, hidden)
    hidden_grad = pullback(dot_outer(branch_grad, weight_out))[0].astype(jnp.bfloat16)
    grad_in = dot_inner(normed, hidden_grad)
    return dot_outer(hidden_grad, weight_in).astype(jnp.bfloat16), grad_in, grad_out


QB = 128
BAND = 3 * QB
SPAN = 4 * QB
NT = (((1,), (1,)), ((), ()))


def span_table(relative):
    table = relative.astype(jnp.bfloat16)
    low = jnp.broadcast_to(table[:1], (2 * QB - 1 - LEFT, table.shape[1]))
    high = jnp.broadcast_to(table[-1:], (SPAN - (2 * QB - 1 - LEFT) - table.shape[0], table.shape[1]))
    spread = jnp.concatenate([low, table, high], axis=0)
    return jnp.concatenate([spread, spread], axis=1)


def fill_scores(first_block, q_mask, k_ref, span_ref, s_ref, edge_ref):
    keys = k_ref.shape[0]
    s_ref[:, QB : QB + keys] = lax.dot_general(q_mask, k_ref[...], NT, preferred_element_type=jnp.float32)
    spread = lax.dot_general(q_mask, span_ref[...], NT, preferred_element_type=jnp.float32)
    edge_ref[0] = jnp.broadcast_to(spread[:, :1], (QB, QB))
    edge_ref[1] = jnp.zeros((QB, QB), jnp.float32)
    edge_ref[2] = jnp.broadcast_to(spread[:, SPAN - 1 :], (QB, QB))
    skewed = pltpu.roll(spread, SPAN - (QB - 1), 1, stride=1, stride_axis=0)
    at = pl.ds(pl.multiple_of(first_block * QB, QB), BAND)
    s_ref[:, at] = s_ref[:, at] + skewed[:, :BAND]


def edge_of(block, first_block):
    return jnp.where(block < first_block - 1, 0, jnp.where(block > first_block + 1, 2, 1))


def forward_kernel(pos_ref, q_ref, k_ref, v_ref, span_ref, o_ref, lse_ref, s_ref, edge_ref, p_ref):
    keys = k_ref.shape[0]
    blocks = keys // QB
    first_block = pos_ref[0] * pl.num_programs(1) + pl.program_id(1)
    lane = lax.broadcasted_iota(jnp.int32, (QB, 2 * HEAD_DIM), 1)
    outs, lses = [], []
    for half in range(2):
        mine = (lane < HEAD_DIM) if half == 0 else (lane >= HEAD_DIM)
        q_mask = jnp.where(mine, q_ref[...], jnp.zeros_like(q_ref))
        fill_scores(first_block, q_mask, k_ref, span_ref, s_ref, edge_ref)
        top = None
        for block in range(blocks):
            z = s_ref[:, (block + 1) * QB : (block + 2) * QB] + edge_ref[edge_of(block, first_block)]
            top = z if top is None else jnp.maximum(top, z)
        top = jnp.max(top, axis=1, keepdims=True)
        edge_ref[...] = edge_ref[...] - top[None]
        total = None
        for block in range(blocks):
            z = s_ref[:, (block + 1) * QB : (block + 2) * QB] + edge_ref[edge_of(block, first_block)]
            p = jnp.exp(z)
            total = p if total is None else total + p
            p_ref[:, block * QB : (block + 1) * QB] = p.astype(jnp.bfloat16)
        total = jnp.sum(total, axis=1, keepdims=True)
        out = jnp.dot(p_ref[...], v_ref[...], preferred_element_type=jnp.float32) / total
        outs.append(out)
        lses.append(jnp.broadcast_to(top + jnp.log(total), (QB, 2 * HEAD_DIM)))
    low = lane < HEAD_DIM
    o_ref[...] = jnp.where(low, outs[0], outs[1]).astype(o_ref.dtype)
    lse_ref[...] = jnp.where(low, lses[0], lses[1])


def attention_forward(position, q, k, v, span):
    rows, width = q.shape
    keys = k.shape[0]
    pairs = width // (2 * HEAD_DIM)
    two = 2 * HEAD_DIM
    row_spec = pl.BlockSpec((QB, two), lambda p, b, pos: (b, p))
    key_spec = pl.BlockSpec((keys, two), lambda p, b, pos: (0, p))
    return pl.pallas_call(
        forward_kernel,
        out_shape=(
            jax.ShapeDtypeStruct((rows, width), jnp.bfloat16),
            jax.ShapeDtypeStruct((rows, width), jnp.float32),
        ),
        grid_spec=pltpu.PrefetchScalarGridSpec(
            num_scalar_prefetch=1,
            grid=(pairs, rows // QB),
            in_specs=[row_spec, key_spec, key_spec, pl.BlockSpec((SPAN, two), lambda p, b, pos: (0, 0))],
            out_specs=(row_spec, row_spec),
            scratch_shapes=[
                pltpu.VMEM((QB, keys + 2 * QB), jnp.float32),
                pltpu.VMEM((3, QB, QB), jnp.float32),
                pltpu.VMEM((QB, keys), jnp.bfloat16),
            ],
        ),
        compiler_params=pltpu.CompilerParams(vmem_limit_bytes=40 << 20),
        cost_estimate=pl.CostEstimate(flops=8 * rows * keys * width, bytes_accessed=4 * (keys + rows) * width, transcendentals=0),
        name="attention_forward",
    )(position.reshape(1), q, k, v, span)


def backward_kernel(pos_ref, q_ref, qt_ref, g_ref, gt_ref, o_ref, lse_ref, k_ref, v_ref, span_ref,
                    dq_ref, dkt_ref, dvt_ref, bins_ref, ends_ref,
                    s_ref, edge_ref, d_ref, p_ref, z_ref, wide_ref, dk_acc, dv_acc):
    keys = k_ref.shape[0]
    blocks = keys // QB
    step = pl.program_id(1)
    first_block = pos_ref[0] * pl.num_programs(1) + step
    lane = lax.broadcasted_iota(jnp.int32, (QB, 2 * HEAD_DIM), 1)

    @pl.when((pl.program_id(0) == 0) & (step == 0))
    def _():
        bins_ref[...] = jnp.zeros_like(bins_ref)
        ends_ref[...] = jnp.zeros_like(ends_ref)

    @pl.when(step == 0)
    def _():
        dk_acc[...] = jnp.zeros_like(dk_acc)
        dv_acc[...] = jnp.zeros_like(dv_acc)
        wide_ref[:, : 2 * HEAD_DIM] = k_ref[...]

    @pl.when((pl.program_id(0) == 0) & (step == 0))
    def _():
        z_ref[:, :QB] = jnp.zeros((QB, QB), jnp.bfloat16)
        z_ref[:, QB + keys :] = jnp.zeros((QB, QB), jnp.bfloat16)

    row_at = lax.broadcasted_iota(jnp.int32, (keys, QB), 0)
    col_at = lax.broadcasted_iota(jnp.int32, (keys, QB), 1)
    below = (row_at < (first_block - 1) * QB) & (col_at == 0)
    above = (row_at >= (first_block + 2) * QB) & (col_at == 1)
    wide_ref[:, 2 * HEAD_DIM :] = jnp.where(below | above, 1.0, 0.0).astype(jnp.bfloat16)

    flip_at = lax.broadcasted_iota(jnp.int32, (QB, QB), 0) + lax.broadcasted_iota(jnp.int32, (QB, QB), 1)
    flip = jnp.where(flip_at == QB - 1, 1.0, 0.0).astype(jnp.bfloat16)
    dqs = []
    for half in range(2):
        rows = slice(half * HEAD_DIM, (half + 1) * HEAD_DIM)
        mine = (lane < HEAD_DIM) if half == 0 else (lane >= HEAD_DIM)
        q_mask = jnp.where(mine, q_ref[...], jnp.zeros_like(q_ref))
        g_mask = jnp.where(mine, g_ref[...], jnp.zeros_like(g_ref))
        fill_scores(first_block, q_mask, k_ref, span_ref, s_ref, edge_ref)
        d_ref[...] = lax.dot_general(g_mask, v_ref[...], NT, preferred_element_type=jnp.float32)
        delta = jnp.sum(g_mask.astype(jnp.float32) * o_ref[...].astype(jnp.float32), axis=1, keepdims=True)
        lse = lse_ref[:, half * HEAD_DIM : half * HEAD_DIM + 1]
        edge_ref[...] = edge_ref[...] - lse[None]
        delta = jnp.broadcast_to(delta, (QB, QB))
        for block in range(blocks):
            here = slice(block * QB, (block + 1) * QB)
            there = slice((block + 1) * QB, (block + 2) * QB)
            p = jnp.exp(s_ref[:, there] + edge_ref[edge_of(block, first_block)])
            p_ref[:, here] = p.astype(jnp.bfloat16)
            z_ref[:, there] = (p * (d_ref[:, here] - delta)).astype(jnp.bfloat16)
        z_all = z_ref[:, QB : QB + keys]
        dv_acc[rows] += jnp.dot(gt_ref[rows], p_ref[...], preferred_element_type=jnp.float32)
        dk_acc[rows] += jnp.dot(qt_ref[rows], z_all, preferred_element_type=jnp.float32)
        dq = jnp.dot(z_all, wide_ref[...], preferred_element_type=jnp.float32)
        at = pl.ds(pl.multiple_of(first_block * QB, QB), BAND)
        band = jnp.dot(flip, z_ref[:, at], preferred_element_type=jnp.float32)
        band = jnp.concatenate([band, jnp.zeros((QB, SPAN - BAND), jnp.float32)], axis=1)
        spread = pltpu.roll(band, 0, 1, stride=1, stride_axis=0).astype(jnp.bfloat16)
        spread = jnp.dot(flip, spread, preferred_element_type=jnp.float32).astype(jnp.bfloat16)
        dq_rel = jnp.dot(spread, span_ref[...], preferred_element_type=jnp.float32)
        below_sum = dq[:, 2 * HEAD_DIM : 2 * HEAD_DIM + 1]
        above_sum = dq[:, 2 * HEAD_DIM + 1 : 2 * HEAD_DIM + 2]
        span_low = span_ref[:1, :].astype(jnp.float32)
        span_high = span_ref[SPAN - 1 :, :].astype(jnp.float32)
        dqs.append(dq[:, : 2 * HEAD_DIM] + dq_rel + below_sum * span_low + above_sum * span_high)
        bins_ref[...] += jnp.dot(qt_ref[rows], spread, preferred_element_type=jnp.float32)
        q_wide = q_mask.astype(jnp.float32)
        ends_ref[0:1, :] += jnp.sum(q_wide * below_sum, axis=0, keepdims=True)
        ends_ref[1:2, :] += jnp.sum(q_wide * above_sum, axis=0, keepdims=True)
    scale = 1.0 / 8.0
    dq_ref[...] = (jnp.where(lane < HEAD_DIM, dqs[0], dqs[1]) * scale).astype(dq_ref.dtype)

    @pl.when(step == pl.num_programs(1) - 1)
    def _():
        dkt_ref[...] = dk_acc[...].astype(dkt_ref.dtype)
        dvt_ref[...] = dv_acc[...].astype(dvt_ref.dtype)


def attention_backward(position, q, q_t, g, g_t, o, lse, k, v, span):
    rows, width = q.shape
    keys = k.shape[0]
    pairs = width // (2 * HEAD_DIM)
    two = 2 * HEAD_DIM
    row_spec = pl.BlockSpec((QB, two), lambda p, b, pos: (b, p))
    col_spec = pl.BlockSpec((two, QB), lambda p, b, pos: (p, b))
    key_spec = pl.BlockSpec((keys, two), lambda p, b, pos: (0, p))
    keyt_spec = pl.BlockSpec((two, keys), lambda p, b, pos: (p, 0))
    fixed = lambda shape: pl.BlockSpec(shape, lambda p, b, pos: (0, 0))
    dq, dkt, dvt, bins, ends = pl.pallas_call(
        backward_kernel,
        out_shape=(
            jax.ShapeDtypeStruct((rows, width), jnp.bfloat16),
            jax.ShapeDtypeStruct((width, keys), jnp.bfloat16),
            jax.ShapeDtypeStruct((width, keys), jnp.bfloat16),
            jax.ShapeDtypeStruct((HEAD_DIM, SPAN), jnp.float32),
            jax.ShapeDtypeStruct((8, two), jnp.float32),
        ),
        grid_spec=pltpu.PrefetchScalarGridSpec(
            num_scalar_prefetch=1,
            grid=(pairs, rows // QB),
            in_specs=[row_spec, col_spec, row_spec, col_spec, row_spec, row_spec, key_spec, key_spec, fixed((SPAN, two))],
            out_specs=(row_spec, keyt_spec, keyt_spec, fixed((HEAD_DIM, SPAN)), fixed((8, two))),
            scratch_shapes=[
                pltpu.VMEM((QB, keys + 2 * QB), jnp.float32),
                pltpu.VMEM((3, QB, QB), jnp.float32),
                pltpu.VMEM((QB, keys), jnp.float32),
                pltpu.VMEM((QB, keys), jnp.bfloat16),
                pltpu.VMEM((QB, keys + 2 * QB), jnp.bfloat16),
                pltpu.VMEM((keys, 2 * two), jnp.bfloat16),
                pltpu.VMEM((two, keys), jnp.float32),
                pltpu.VMEM((two, keys), jnp.float32),
            ],
        ),
        compiler_params=pltpu.CompilerParams(vmem_limit_bytes=40 << 20),
        cost_estimate=pl.CostEstimate(flops=20 * rows * keys * width, bytes_accessed=8 * (keys + rows) * width, transcendentals=0),
        name="attention_backward",
    )(position.reshape(1), q, q_t, g, g_t, o, lse, k, v, span)
    at = 2 * QB - 1 - LEFT
    ends = ends[:2, :HEAD_DIM] + ends[:2, HEAD_DIM:]
    spread = bins.T
    inner = spread[at + 1 : at + LEFT + RIGHT]
    low = jnp.sum(spread[: at + 1], axis=0) + ends[0]
    high = jnp.sum(spread[at + LEFT + RIGHT :], axis=0) + ends[1]
    table = jnp.concatenate([low[None], inner, high[None]], axis=0)
    return dq, dkt, dvt, table


def attend_forward(normed, weight_in, weight_out, relative, position):
    projected = jnp.einsum(
        "td,kde->kte", normed, weight_in, preferred_element_type=jnp.float32
    ).astype(jnp.bfloat16)
    key_rows, value_rows = (
        lax.all_gather(projected[1], "context", axis=0, tiled=True),
        lax.all_gather(projected[2], "context", axis=0, tiled=True),
    )
    queries = projected[0] * jnp.bfloat16(1.0 / math.sqrt(HEAD_DIM))
    span = span_table(relative)
    mixed, log_total = attention_forward(position, queries, key_rows, value_rows, span)
    return (
        dot_rows(mixed, weight_out).astype(jnp.bfloat16),
        (normed, queries, key_rows, value_rows, log_total, mixed, span),
    )


def attend_backward(weight_in, weight_out, position, saved, branch_grad):
    normed, queries, key_rows, value_rows, log_total, mixed, span = saved
    grad_out = dot_inner(mixed, branch_grad)
    mixed_grad = dot_outer(branch_grad, weight_out).astype(jnp.bfloat16)
    query_grad, key_grad, value_grad, table_grad = attention_backward(
        position, queries, queries.T, mixed_grad, mixed_grad.T, mixed, log_total, key_rows, value_rows, span
    )
    key_grad = lax.psum_scatter(key_grad, "context", scatter_dimension=1, tiled=True)
    value_grad = lax.psum_scatter(value_grad, "context", scatter_dimension=1, tiled=True)
    stacked = jnp.stack([query_grad, key_grad.T, value_grad.T])
    grad_in = jnp.einsum("td,kte->kde", normed, stacked, preferred_element_type=jnp.float32)
    partial_sum = jnp.einsum("kte,kde->td", stacked, weight_in, preferred_element_type=jnp.float32)
    return (partial_sum.astype(jnp.bfloat16), table_grad, grad_in, grad_out)


def conv_forward(normed, weight_in, weight_out, depthwise, gain_middle):
    projected = jnp.einsum("td,kde->kte", normed, weight_in, preferred_element_type=jnp.float32)
    gated = gate_unit(projected[0], projected[1])
    rows_here = gated.shape[0]
    reach_rows = depthwise.shape[0] - 1
    edge_rows = shifted_2(gated[rows_here - reach_rows :], "context", 1)
    padded = jnp.concatenate([edge_rows, gated], axis=0)
    mixed = depthwise[0] * padded[0:rows_here]
    for offset in range(1, reach_rows + 1):
        mixed = mixed + depthwise[offset] * padded[offset : offset + rows_here]
    row_sums, row_squares = lax.psum(
        (jnp.sum(mixed, axis=1), jnp.sum(mixed * mixed, axis=1)), "tensor"
    )
    row_mean = row_sums / D
    inverse = lax.rsqrt(row_squares / D - row_mean * row_mean + epsilon)
    scaled = (mixed - row_mean[:, None]) * inverse[:, None]
    shaped = scaled * gain_middle
    active = jax.nn.silu(shaped).astype(jnp.bfloat16)
    return (
        dot_rows(active, weight_out).astype(jnp.bfloat16),
        (normed, projected, padded, scaled, inverse, shaped, active),
    )


def conv_backward(weight_in, weight_out, depthwise, gain_middle, saved, branch_grad):
    normed, projected, padded, scaled, inverse, shaped, active = saved
    rows_here = scaled.shape[0]
    reach_rows = depthwise.shape[0] - 1
    grad_out = dot_inner(active, branch_grad)
    unused, pullback = jax.vjp(jax.nn.silu, shaped)
    shaped_grad = pullback(dot_outer(branch_grad, weight_out))[0]
    middle_grad = jnp.sum(shaped_grad * scaled, axis=0)
    scaled_grad = shaped_grad * gain_middle
    first_sum, second_sum = lax.psum(
        (jnp.sum(scaled_grad, axis=1), jnp.sum(scaled_grad * scaled, axis=1)), "tensor"
    )
    mixed_grad = inverse[:, None] * (
        scaled_grad - first_sum[:, None] / D - scaled * (second_sum[:, None] / D)
    )
    next_rows = shifted_2(mixed_grad[:reach_rows], "context", -1)
    padded_grad = jnp.concatenate([mixed_grad, next_rows], axis=0)
    gated_grad = depthwise[reach_rows] * padded_grad[0:rows_here]
    for offset in range(1, reach_rows + 1):
        gated_grad = gated_grad + depthwise[reach_rows - offset] * padded_grad[offset : offset + rows_here]
    depth_grad = jnp.stack(
        [
            jnp.sum(padded[offset : offset + rows_here] * mixed_grad, axis=0)
            for offset in range(reach_rows + 1)
        ]
    )
    unused, pullback = jax.vjp(gate_unit, projected[0], projected[1])
    unit_grad, gate_grad = pullback(gated_grad)
    stacked = jnp.stack([unit_grad, gate_grad]).astype(jnp.bfloat16)
    grad_in = jnp.einsum("td,kte->kde", normed, stacked, preferred_element_type=jnp.float32)
    partial_sum = jnp.einsum("kte,kde->td", stacked, weight_in, preferred_element_type=jnp.float32)
    return (partial_sum.astype(jnp.bfloat16), grad_in, grad_out, middle_grad, depth_grad)


def local(
    inputs,
    gain_first,
    first_in,
    first_out,
    gain_attend,
    attend_in,
    attend_out,
    relative,
    gain_convolve,
    convolve_in,
    depthwise,
    gain_middle,
    convolve_out,
    gain_second,
    second_in,
    second_out,
    gain_final,
    cotangent,
):
    position = lax.axis_index("context")
    start_rows = inputs[0]
    first_in, first_out = fetch(first_in[None], first_out)
    attend_in, attend_out = fetch(attend_in, attend_out)
    convolve_in, convolve_out = fetch(convolve_in, convolve_out)
    second_in, second_out = fetch(second_in[None], second_out)
    first_in, second_in = first_in[0], second_in[0]
    normed = layer_norm(start_rows.astype(jnp.float32), gain_first).astype(jnp.bfloat16)
    branch, first_saved = feed(normed, first_in, first_out)
    after_first, normed = forward_sum(1, branch, start_rows, gain_attend, 0.5)
    branch, attend_saved = attend_forward(normed, attend_in, attend_out, relative, position)
    after_attend, normed = forward_sum(2, branch, after_first, gain_convolve, 1.0)
    branch, convolve_saved = conv_forward(normed, convolve_in, convolve_out, depthwise, gain_middle)
    after_convolve, normed = forward_sum(3, branch, after_attend, gain_second, 1.0)
    branch, second_saved = feed(normed, second_in, second_out)
    final_out, upstream, branch_grad, grad_final = turn_sum(4, branch, after_convolve, gain_final, cotangent[0])
    branch, grad_in, grad_out = feed_back(second_in, second_out, second_saved, branch_grad)
    second_grads = send_grads(grad_in[None], grad_out)
    upstream, branch_grad, grad_gain_second = backward_sum(5, branch, after_convolve, gain_second, upstream, 1.0)
    branch, grad_in, grad_out, grad_middle, grad_depth = conv_backward(
        convolve_in, convolve_out, depthwise, gain_middle, convolve_saved, branch_grad
    )
    convolve_grads = send_grads(grad_in, grad_out)
    upstream, branch_grad, grad_gain_convolve = backward_sum(6, branch, after_attend, gain_convolve, upstream, 1.0)
    branch, table_grad, grad_in, grad_out = attend_backward(attend_in, attend_out, position, attend_saved, branch_grad)
    attend_grads = send_grads(grad_in, grad_out)
    upstream, branch_grad, grad_gain_attend = backward_sum(7, branch, after_first, gain_attend, upstream, 0.5)
    branch, grad_in, grad_out = feed_back(first_in, first_out, first_saved, branch_grad)
    first_grads = send_grads(grad_in[None], grad_out)
    upstream, branch_grad, grad_gain_first = backward_sum(8, branch, start_rows, gain_first, upstream, 1.0)
    table_grad = lax.psum(table_grad, "tensor")
    smalls = lax.psum(
        (
            grad_gain_first,
            grad_gain_attend,
            table_grad,
            grad_gain_convolve,
            grad_depth,
            grad_middle,
            grad_gain_second,
            grad_final,
        ),
        ("clips", "context"),
    )
    return (
        final_out[None],
        upstream[None],
        smalls[0],
        first_grads[0][0],
        first_grads[1],
        smalls[1],
        attend_grads[0],
        attend_grads[1],
        smalls[2],
        smalls[3],
        convolve_grads[0],
        smalls[4],
        smalls[5],
        convolve_grads[1],
        smalls[6],
        second_grads[0][0],
        second_grads[1],
        smalls[7],
    )


def solution(mesh):
    placed = (
        P("clips", "context", None),
        P(),
        P(("clips", "context"), "tensor"),
        P("tensor", ("clips", "context")),
        P(),
        P(None, ("clips", "context"), "tensor"),
        P("tensor", ("clips", "context")),
        P(),
        P(),
        P(None, ("clips", "context"), "tensor"),
        P(None, "tensor"),
        P("tensor"),
        P("tensor", ("clips", "context")),
        P(),
        P(("clips", "context"), "tensor"),
        P("tensor", ("clips", "context")),
        P(),
        P("clips", "context", None),
    )
    return jax.shard_map(
        local,
        mesh=mesh,
        in_specs=placed,
        out_specs=(
            P("clips", "context", None),
            P("clips", "context", None),
            P(),
            P(("clips", "context"), "tensor"),
            P("tensor", ("clips", "context")),
            P(),
            P(None, ("clips", "context"), "tensor"),
            P("tensor", ("clips", "context")),
            P(),
            P(),
            P(None, ("clips", "context"), "tensor"),
            P(None, "tensor"),
            P("tensor"),
            P("tensor", ("clips", "context")),
            P(),
            P(("clips", "context"), "tensor"),
            P("tensor", ("clips", "context")),
            P(),
        ),
        check_vma=False,
    )
```

```python
import math

import jax
import jax.numpy as jnp
from jax import lax
from jax.experimental import pallas as pl
from jax.experimental.pallas import tpu as pltpu
from jax.sharding import PartitionSpec as P

CLIPS, CONTEXT, TENSOR = "clips", "context", "tensor"
D = 1024
HEAD_DIM = 64
LEFT = 64
RIGHT = 8

epsilon = 1e-05


def shifted_2(value, axis, steps):
    count = lax.axis_size(axis)
    initial, last = (max(0, -steps), min(count, count - steps))
    return lax.ppermute(value, axis, [(source, source + steps) for source in range(initial, last)])


def dot_rows(former, latter):
    return jnp.dot(former, latter, preferred_element_type=jnp.float32)


def dot_inner(former, latter):
    return lax.dot_general(
        former, latter, (((0,), (0,)), ((), ())), preferred_element_type=jnp.float32
    )


def dot_outer(former, latter):
    return lax.dot_general(
        former, latter, (((1,), (1,)), ((), ())), preferred_element_type=jnp.float32
    )


def layer_norm(rows_in, gain_vec):
    row_mean = jnp.mean(rows_in, axis=-1, keepdims=True)
    centred = rows_in - row_mean
    variance = jnp.mean(centred * centred, axis=-1, keepdims=True)
    return centred * lax.rsqrt(variance + epsilon) * gain_vec


def gate_unit(unit_half, gate_half):
    return unit_half * jax.nn.sigmoid(gate_half)


def fetch(weight_in, weight_out):
    return (
        lax.all_gather(weight_in.astype(jnp.bfloat16), (CLIPS, CONTEXT), axis=weight_in.ndim - 2, tiled=True),
        lax.all_gather(weight_out.astype(jnp.bfloat16), (CLIPS, CONTEXT), axis=1, tiled=True),
    )


def scatter_sum(grad, axis):
    summed = lax.psum_scatter(
        grad.astype(jnp.bfloat16), (CLIPS, CONTEXT), scatter_dimension=axis, tiled=True
    )
    return summed.astype(jnp.float32)


def send_grads(grad_in, grad_out):
    return (scatter_sum(grad_in, grad_in.ndim - 2), scatter_sum(grad_out, 1))


MESH_ID = pl.DeviceIdType.MESH
CHUNKS = 16
LAG = 3
FULL, TOP, BOTTOM = 0, 1, 2
FIRST, ATTEND, CONVOLVE, SECOND = range(4)


def near():
    across_clips = lax.axis_index(CLIPS)
    along = lax.axis_index(CONTEXT)
    deep, core = along // 2, along % 2
    devices = (
        {CLIPS: 1 - across_clips},
        {CONTEXT: (1 - deep) * 2 + core},
        {CONTEXT: deep * 2 + 1 - core},
    )
    return (across_clips, deep, core), devices


def greet(devices):
    barrier = pltpu.get_barrier_semaphore()
    for device in devices:
        pl.semaphore_signal(barrier, inc=1, device_id=device, device_id_type=MESH_ID)
    pl.semaphore_wait(barrier, len(devices))


def part_of(ref, wide, count, shard, part):
    if wide:
        size = ref.shape[-1] // count
        rows = ref.shape[-2]
        along = slice(None) if part == FULL else pl.ds((part - 1) * (rows // 2), rows // 2)
        return ref.at[along, pl.ds(pl.multiple_of(shard * size, 128), size)]
    size = ref.shape[-2] // count
    start, length = shard * size, size
    if part != FULL:
        length = size // 2
        start = start + (part - 1) * length
    window = pl.ds(pl.multiple_of(start, 16), length)
    return ref.at[window] if len(ref.shape) == 2 else ref.at[:, window]


def half_of(ref, part):
    length = ref.shape[-2] // 2
    window = pl.ds((part - 1) * length, length)
    return ref.at[window] if len(ref.shape) == 2 else ref.at[:, window]


class Gather:
    copies = 9
    line = False

    def __init__(self, wide, shard_shape):
        self.wide = wide
        self.shape = shard_shape[:-2] + (
            (shard_shape[-2], shard_shape[-1] * 8) if wide else (shard_shape[-2] * 8, shard_shape[-1])
        )

    def outs(self):
        return [(self.shape, jnp.bfloat16)]

    def scratch(self):
        return [pltpu.SemaphoreType.DMA((self.copies,)), pltpu.SemaphoreType.DMA((self.copies,)), pltpu.SemaphoreType.DMA]

    def bind(self, ins, outs, scratch):
        (shard_ref,), (full_ref,) = ins, outs
        send, recv, own_sem = scratch
        (x, y, core), (to_x, to_y, to_core) = near()
        shard = lambda a, b: a * 4 + b * 2 + core
        own, at_x, at_y, at_far = shard(x, y), shard(1 - x, y), shard(x, 1 - y), shard(1 - x, 1 - y)
        place = lambda which, part: part_of(full_ref, self.wide, 8, which, part)

        def copy(index, source, which, part, device):
            return pltpu.make_async_remote_copy(
                src_ref=source, dst_ref=place(which, part), send_sem=send.at[index], recv_sem=recv.at[index],
                device_id=device, device_id_type=MESH_ID,
            )

        passed = lambda index, which, part, device: copy(index, place(which, part), which, part, device)
        moves = [
            copy(0, shard_ref, own, FULL, to_x),
            copy(1, shard_ref, own, FULL, to_y),
            copy(2, shard_ref, own, FULL, to_core),
            passed(3, at_x, TOP, to_y),
            passed(4, at_x, FULL, to_core),
            passed(5, at_y, BOTTOM, to_x),
            passed(6, at_y, FULL, to_core),
            passed(7, at_far, TOP, to_core),
            passed(8, at_far, BOTTOM, to_core),
        ]
        mine = pltpu.make_async_copy(shard_ref, place(own, FULL), own_sem)

        def begin():
            for index in (0, 1, 2):
                moves[index].start()
            mine.start()

        def second():
            moves[0].wait_recv()
            moves[3].start()
            moves[4].start()
            moves[1].wait_recv()
            moves[5].start()
            moves[6].start()

        def third():
            moves[3].wait_recv()
            moves[7].start()
            moves[5].wait_recv()
            moves[8].start()

        def last():
            for index in (2, 4, 6, 7, 8):
                moves[index].wait_recv()
            mine.wait()
            for move in moves:
                move.wait_send()

        return begin, [second, third], last


class Scatter:
    copies = 8
    line = False

    def __init__(self, wide, full_shape):
        self.wide = wide
        self.shape = full_shape[:-2] + (
            (full_shape[-2], full_shape[-1] // 8) if wide else (full_shape[-2] // 8, full_shape[-1])
        )

    def outs(self):
        return [(self.shape, jnp.float32)]

    def scratch(self):
        half = self.shape[:-2] + (self.shape[-2] // 2, self.shape[-1])
        return [
            pltpu.VMEM((4,) + self.shape, jnp.bfloat16),
            pltpu.VMEM((4,) + self.shape, jnp.bfloat16),
            pltpu.VMEM((2,) + self.shape, jnp.bfloat16),
            pltpu.VMEM((2,) + half, jnp.bfloat16),
            pltpu.SemaphoreType.DMA((self.copies,)),
            pltpu.SemaphoreType.DMA((self.copies,)),
        ]

    def bind(self, ins, outs, scratch):
        (full_ref,), (out_ref,) = ins, outs
        from_core, pair, whole, halves, send, recv = scratch
        (x, y, core), (to_x, to_y, to_core) = near()

        def copy(index, source, target, device):
            return pltpu.make_async_remote_copy(
                src_ref=source, dst_ref=target, send_sem=send.at[index], recv_sem=recv.at[index],
                device_id=device, device_id_type=MESH_ID,
            )

        place = lambda slot, at_core: part_of(full_ref, self.wide, 8, slot * 2 + at_core, FULL)
        own, at_x, at_y, at_far = x * 2 + y, (1 - x) * 2 + y, x * 2 + 1 - y, (1 - x) * 2 + 1 - y
        moves = [copy(slot, place(slot, 1 - core), from_core.at[slot], to_core) for slot in range(4)]
        moves += [
            copy(4, half_of(pair.at[at_far], TOP), halves.at[0], to_x),
            copy(5, half_of(pair.at[at_far], BOTTOM), halves.at[1], to_y),
            copy(6, pair.at[at_x], whole.at[0], to_x),
            copy(7, pair.at[at_y], whole.at[1], to_y),
        ]
        wide = lambda ref: ref[...].astype(jnp.float32)

        def begin():
            for slot in range(4):
                moves[slot].start()

        def second():
            for slot in range(4):
                moves[slot].wait_recv()
                pair[slot] = (wide(place(slot, core)) + wide(from_core.at[slot])).astype(jnp.bfloat16)
            moves[4].start()
            moves[5].start()

        def third():
            moves[4].wait_recv()
            target = half_of(pair.at[at_y], TOP)
            target[...] = (wide(target) + wide(halves.at[0])).astype(jnp.bfloat16)
            moves[7].start()
            moves[5].wait_recv()
            target = half_of(pair.at[at_x], BOTTOM)
            target[...] = (wide(target) + wide(halves.at[1])).astype(jnp.bfloat16)
            moves[6].start()

        def last():
            moves[6].wait_recv()
            moves[7].wait_recv()
            out_ref[...] = wide(pair.at[own]) + wide(whole.at[0]) + wide(whole.at[1])
            for move in moves:
                move.wait_send()

        return begin, [second, third], last


class PlaneSum:
    line = False

    def __init__(self, shape):
        self.shape = shape

    def outs(self):
        return [(self.shape, jnp.float32)]

    def scratch(self):
        return [
            pltpu.VMEM((3,) + self.shape, jnp.float32),
            pltpu.VMEM((2,) + self.shape, jnp.float32),
            pltpu.SemaphoreType.DMA((3,)),
            pltpu.SemaphoreType.DMA((3,)),
        ]

    def bind(self, ins, outs, scratch):
        (value_ref,), (out_ref,) = ins, outs
        slots, totals, send, recv = scratch
        to_x, to_y, to_core = near()[1]
        moves = [
            pltpu.make_async_remote_copy(
                src_ref=source, dst_ref=slots.at[index], send_sem=send.at[index], recv_sem=recv.at[index],
                device_id=device, device_id_type=MESH_ID,
            )
            for index, (source, device) in enumerate(
                ((value_ref, to_core), (totals.at[0], to_y), (totals.at[1], to_x))
            )
        ]

        def begin():
            moves[0].start()

        def second():
            moves[0].wait_recv()
            totals[0] = value_ref[...] + slots[0]
            moves[1].start()

        def third():
            moves[1].wait_recv()
            totals[1] = totals[0] + slots[1]
            moves[2].start()

        def last():
            moves[2].wait_recv()
            out_ref[...] = totals[1] + slots[2]
            for move in moves:
                move.wait_send()

        return begin, [second, third], last


class LineSum:
    line = True

    def __init__(self, shape):
        self.shape = shape

    def outs(self):
        return [(self.shape, jnp.float32)]

    def scratch(self):
        return [
            pltpu.VMEM((4,) + self.shape, jnp.float32),
            pltpu.SemaphoreType.DMA((4,)),
            pltpu.SemaphoreType.DMA((4,)),
        ]

    def bind(self, ins, outs, scratch):
        (value_ref,), (out_ref,) = ins, outs
        slots, send, recv = scratch
        at = lax.axis_index(TENSOR)

        def copy(step, slot):
            return pltpu.make_async_remote_copy(
                src_ref=value_ref, dst_ref=slots.at[slot], send_sem=send.at[step], recv_sem=recv.at[slot],
                device_id={TENSOR: (at + step) % 4}, device_id_type=MESH_ID,
            )

        def begin():
            for step in range(1, 4):
                copy(step, at).start()
            slots[at] = value_ref[...]

        def last():
            for step in range(1, 4):
                copy(step, (at + step) % 4).wait_recv()
            out_ref[...] = slots[0] + slots[1] + slots[2] + slots[3]
            for step in range(1, 4):
                copy(step, at).wait_send()

        return begin, [lambda: None, lambda: None], last


def bind_all(tasks, ins, outs, scratch):
    begins, middles, lasts = [], [], []
    for task, task_in, task_out in zip(tasks, ins, outs):
        count = len(task.scratch())
        begin, steps, last = task.bind((task_in,), (task_out,), scratch[:count])
        scratch = scratch[count:]
        begins.append(begin)
        middles.append(steps)
        lasts.append(last)
    return begins, [step for turn in zip(*middles) for step in turn], lasts


def plane_call(cid, tasks, operands):
    vmem = pl.BlockSpec(memory_space=pltpu.VMEM)
    outs = [out for task in tasks for out in task.outs()]

    def kernel(*refs):
        n = len(tasks)
        greet(near()[1])
        begins, steps, lasts = bind_all(tasks, refs[:n], refs[n : 2 * n], refs[2 * n :])
        for step in begins + steps + lasts:
            step()

    return pl.pallas_call(
        kernel,
        out_shape=tuple(jax.ShapeDtypeStruct(shape, kind) for shape, kind in outs),
        in_specs=[vmem] * len(operands),
        out_specs=(vmem,) * len(outs),
        scratch_shapes=[piece for task in tasks for piece in task.scratch()],
        compiler_params=pltpu.CompilerParams(collective_id=cid, has_side_effects=True, vmem_limit_bytes=12 << 20),
        cost_estimate=pl.CostEstimate(flops=30_000_000_000, bytes_accessed=50_000_000, transcendentals=0),
        name=f"call_{cid}",
    )(*operands)


def line_sum(axis, partial_ref, acc_ref, from_end, from_mid, total_ref, send_sem, recv_sem, finish, others, whole_line, begins, steps, lasts):
    at = lax.axis_index(axis)
    low = at < 2
    end = jnp.where(low, 0, 3)
    mid = jnp.where(low, 1, 2)
    other = jnp.where(low, 2, 1)
    is_mid = at == mid
    rest = [{axis: (at + step) % 4} for step in range(1, 4)]
    size = partial_ref.shape[0] // CHUNKS
    gap = (CHUNKS - LAG) // (len(steps) + 1)

    def rows(chunk):
        return pl.ds(pl.multiple_of(chunk * size, size), size)

    def hop(stage, chunk, source, target, device):
        return pltpu.make_async_remote_copy(
            src_ref=source.at[rows(chunk)],
            dst_ref=target.at[rows(chunk)],
            send_sem=send_sem.at[stage, chunk],
            recv_sem=recv_sem.at[stage, chunk],
            device_id={axis: device},
            device_id_type=MESH_ID,
        )

    inward = lambda chunk: hop(0, chunk, partial_ref, from_end, mid)
    across = lambda chunk: hop(1, chunk, acc_ref, from_mid, other)
    outward = lambda chunk: hop(2, chunk, total_ref, total_ref, end)

    def loop(low, high, body):
        def step(chunk, carry):
            body(chunk)
            return carry

        lax.fori_loop(low, high, step, 0)

    def beside(chunk):
        for index, step in enumerate(steps):
            pl.when(chunk == LAG + (index + 1) * gap)(step)

    @pl.when(is_mid)
    def _():
        greet((rest if whole_line else [{axis: end}, {axis: other}]) + others)
        for begin in begins:
            begin()

        def first(chunk):
            inward(chunk).wait_recv()
            here = rows(chunk)
            acc_ref[here] = (partial_ref[here].astype(jnp.float32) + from_end[here].astype(jnp.float32)).astype(acc_ref.dtype)
            across(chunk).start()

        def second(chunk):
            across(chunk).wait_recv()
            here = rows(chunk)
            total_ref[here] = (acc_ref[here].astype(jnp.float32) + from_mid[here].astype(jnp.float32)).astype(total_ref.dtype)
            outward(chunk).start()
            finish(here)

        def both(chunk):
            first(chunk)
            second(chunk - LAG)
            beside(chunk)

        loop(0, LAG, first)
        loop(LAG, CHUNKS, both)
        loop(CHUNKS - LAG, CHUNKS, second)

        def drain(chunk):
            across(chunk).wait_send()
            outward(chunk).wait_send()

        loop(0, CHUNKS, drain)

    @pl.when(jnp.logical_not(is_mid))
    def _():
        greet((rest if whole_line else [{axis: mid}]) + others)
        loop(0, CHUNKS, lambda chunk: inward(chunk).start())
        for begin in begins:
            begin()

        def receive(chunk):
            beside(chunk + LAG)
            outward(chunk).wait_recv()
            finish(rows(chunk))

        loop(0, CHUNKS, receive)
        loop(0, CHUNKS, lambda chunk: inward(chunk).wait_send())

    for last in lasts:
        last()


def unit_rows(rows_in):
    mean = jnp.mean(rows_in, axis=-1, keepdims=True)
    centred = rows_in - mean
    variance = jnp.mean(centred * centred, axis=-1, keepdims=True)
    inverse = lax.rsqrt(variance + epsilon)
    return centred * inverse, inverse


def rows_back(unit, inverse, scaled):
    return inverse * (
        scaled
        - jnp.mean(scaled, axis=-1, keepdims=True)
        - unit * jnp.mean(scaled * unit, axis=-1, keepdims=True)
    )


def gather_eight(value):
    total = value[:8]
    for at in range(8, value.shape[0], 8):
        total = total + value[at : at + 8]
    return total


def sum_call(body, cid, partial, operands, outs, tasks, task_operands):
    rows, width = partial.shape
    chunk_shape = pltpu.VMEM((rows, width), jnp.bfloat16)
    vmem = pl.BlockSpec(memory_space=pltpu.VMEM)
    task_outs = [out for task in tasks for out in task.outs()]
    grant = (30 if any(isinstance(task, Scatter) for task in tasks) else 22) << 20
    pieces = [piece for task in tasks for piece in task.scratch()]

    def kernel(partial_ref, *refs):
        def take(count):
            nonlocal refs
            taken, refs = refs[:count], refs[count:]
            return taken

        ins, task_ins = take(len(operands)), take(len(tasks))
        results, task_results = take(len(outs)), take(len(tasks))
        acc, from_end, from_mid, total, send_sem, recv_sem = take(6)
        begins, steps, lasts, others = [], [], [], []
        if tasks:
            others = list(near()[1])
            begins, steps, lasts = bind_all(tasks, task_ins, task_results, refs)
        start, finish = body(total, ins, results)
        start()
        line_sum(
            TENSOR, partial_ref, acc, from_end, from_mid, total, send_sem, recv_sem, finish, others,
            any(task.line for task in tasks), begins, steps, lasts,
        )

    got = pl.pallas_call(
        kernel,
        out_shape=tuple(jax.ShapeDtypeStruct(shape, kind) for shape, kind in list(outs) + task_outs),
        in_specs=[vmem] * (1 + len(operands) + len(tasks)),
        out_specs=(vmem,) * (len(outs) + len(tasks)),
        scratch_shapes=[chunk_shape] * 4
        + [pltpu.SemaphoreType.DMA((3, CHUNKS)), pltpu.SemaphoreType.DMA((3, CHUNKS))]
        + pieces,
        compiler_params=pltpu.CompilerParams(collective_id=cid, has_side_effects=True, vmem_limit_bytes=grant),
        cost_estimate=pl.CostEstimate(flops=60_000_000_000, bytes_accessed=100_000_000, transcendentals=0),
        name=f"call_{cid}",
    )(partial, *operands, *task_operands)
    return got[: len(outs)], got[len(outs) :]


def forward_sum(cid, partial, rows_in, gain, scale, tasks=(), task_operands=()):
    def body(total, ins, results):
        x_ref, gain_ref = ins
        x_out, a_out = results

        def finish(here):
            x = x_ref[here].astype(jnp.float32) + scale * total[here].astype(jnp.float32)
            x_out[here] = x
            a_out[here] = (unit_rows(x)[0] * gain_ref[...]).astype(a_out.dtype)

        return lambda: None, finish

    shape = partial.shape
    return sum_call(
        body, cid, partial, (rows_in, gain.reshape(1, -1)),
        ((shape, jnp.float32), (shape, jnp.bfloat16)), tasks, task_operands,
    )


def turn_sum(cid, partial, rows_in, gain, cotangent):
    def body(total, ins, results):
        x_ref, gain_ref, cot_ref = ins
        out_ref, d_ref, half_ref, gain_grad_ref = results

        def start():
            gain_grad_ref[...] = jnp.zeros_like(gain_grad_ref)

        def finish(here):
            x = x_ref[here] + 0.5 * total[here].astype(jnp.float32)
            unit, inverse = unit_rows(x)
            out_ref[here] = (unit * gain_ref[...]).astype(out_ref.dtype)
            upstream = cot_ref[here].astype(jnp.float32)
            d = rows_back(unit, inverse, upstream * gain_ref[...])
            d_ref[here] = d
            half_ref[here] = (0.5 * d).astype(half_ref.dtype)
            gain_grad_ref[...] += gather_eight(upstream * unit)

        return start, finish

    shape = partial.shape
    (out, d, half, gain_grad), _ = sum_call(
        body, cid, partial, (rows_in, gain.reshape(1, -1), cotangent),
        ((shape, jnp.bfloat16), (shape, jnp.float32), (shape, jnp.bfloat16), ((8, shape[1]), jnp.float32)), (), (),
    )
    return out, d, half, gain_grad


def backward_sum(cid, partial, rows_in, gain, upstream, scale, tasks=(), task_operands=()):
    def body(total, ins, results):
        x_ref, gain_ref, up_ref = ins
        d_ref, half_ref, gain_grad_ref = results

        def start():
            gain_grad_ref[...] = jnp.zeros_like(gain_grad_ref)

        def finish(here):
            unit, inverse = unit_rows(x_ref[here].astype(jnp.float32))
            normed_grad = total[here].astype(jnp.float32)
            d = up_ref[here] + rows_back(unit, inverse, normed_grad * gain_ref[...])
            d_ref[here] = d
            half_ref[here] = (scale * d).astype(half_ref.dtype)
            gain_grad_ref[...] += gather_eight(normed_grad * unit)

        return start, finish

    shape = partial.shape
    return sum_call(
        body, cid, partial, (rows_in, gain.reshape(1, -1), upstream),
        ((shape, jnp.float32), (shape, jnp.bfloat16), ((8, shape[1]), jnp.float32)), tasks, task_operands,
    )


def context_places():
    along = lax.axis_index(CONTEXT)
    deep, core = along // 2, along % 2
    return deep, core, {CONTEXT: (1 - deep) * 2 + core}, {CONTEXT: deep * 2 + 1 - core}


def context_call(kernel, cid, operands, outs, scratch, ready=20_000_000_000):
    vmem = pl.BlockSpec(memory_space=pltpu.VMEM)
    return pl.pallas_call(
        kernel,
        out_shape=tuple(jax.ShapeDtypeStruct(shape, kind) for shape, kind in outs),
        in_specs=[vmem] * len(operands),
        out_specs=(vmem,) * len(outs),
        scratch_shapes=scratch,
        compiler_params=pltpu.CompilerParams(collective_id=cid, has_side_effects=True, vmem_limit_bytes=12 << 20),
        cost_estimate=pl.CostEstimate(flops=ready, bytes_accessed=30_000_000, transcendentals=0),
        name=f"call_{cid}",
    )(*operands)


def gather_context(cid, first, second):
    rows, width = first.shape

    def kernel(first_ref, second_ref, first_out, second_out, send, recv, own_sem):
        deep, core, to_y, to_core = context_places()
        greet([to_y, to_core])

        def block(ref, which):
            return ref.at[pl.ds(pl.multiple_of(which * rows, rows), rows)]

        def copy(index, source, target, device):
            return pltpu.make_async_remote_copy(
                src_ref=source, dst_ref=target, send_sem=send.at[index], recv_sem=recv.at[index],
                device_id=device, device_id_type=MESH_ID,
            )

        own, beyond = deep * 2 + core, (1 - deep) * 2 + core
        pairs = ((first_ref, first_out), (second_ref, second_out))
        out_y = [copy(i, source, block(full, own), to_y) for i, (source, full) in enumerate(pairs)]
        out_core = [copy(2 + i, source, block(full, own), to_core) for i, (source, full) in enumerate(pairs)]
        passed = [copy(4 + i, block(full, beyond), block(full, beyond), to_core) for i, (source, full) in enumerate(pairs)]
        mine = [pltpu.make_async_copy(source, block(full, own), own_sem.at[i]) for i, (source, full) in enumerate(pairs)]
        for move in out_y + out_core + mine:
            move.start()
        for arrived, onward in zip(out_y, passed):
            arrived.wait_recv()
            onward.start()
        for move in out_core + passed:
            move.wait_recv()
        for move in mine:
            move.wait()
        for move in out_y + out_core + passed:
            move.wait_send()

    full = ((4 * rows, width), first.dtype)
    return context_call(
        kernel, cid, (first, second), (full, full),
        [pltpu.SemaphoreType.DMA((6,)), pltpu.SemaphoreType.DMA((6,)), pltpu.SemaphoreType.DMA((2,))],
    )


def scatter_context(cid, first, second):
    rows, width = first.shape
    part = width // 4

    def kernel(first_ref, second_ref, first_out, second_out, from_core, pair, from_y, send, recv):
        deep, core, to_y, to_core = context_places()
        greet([to_y, to_core])

        def block(ref, which):
            return ref.at[:, pl.ds(pl.multiple_of(which * part, 128), part)]

        def copy(index, source, target, device):
            return pltpu.make_async_remote_copy(
                src_ref=source, dst_ref=target, send_sem=send.at[index], recv_sem=recv.at[index],
                device_id=device, device_id_type=MESH_ID,
            )

        wide = lambda ref: ref[...].astype(jnp.float32)
        sources, targets = (first_ref, second_ref), (first_out, second_out)
        far, close = 1 - deep, deep
        inner, outer = [], []
        for i, source in enumerate(sources):
            for j, at in enumerate((far, close)):
                inner.append(copy(2 * i + j, block(source, at * 2 + 1 - core), from_core.at[2 * i + j], to_core))
            outer.append(copy(4 + i, pair.at[2 * i], from_y.at[i], to_y))
        for at in (0, 2, 1, 3):
            inner[at].start()
        for i, source in enumerate(sources):
            inner[2 * i].wait_recv()
            pair[2 * i] = (wide(block(source, far * 2 + core)) + wide(from_core.at[2 * i])).astype(jnp.bfloat16)
            outer[i].start()
        for i, source in enumerate(sources):
            inner[2 * i + 1].wait_recv()
            pair[2 * i + 1] = (wide(block(source, close * 2 + core)) + wide(from_core.at[2 * i + 1])).astype(jnp.bfloat16)
        for i, target in enumerate(targets):
            outer[i].wait_recv()
            target[...] = (wide(pair.at[2 * i + 1]) + wide(from_y.at[i])).astype(target.dtype)
        for move in inner + outer:
            move.wait_send()

    out = ((rows, part), jnp.bfloat16)
    piece = (rows, part)
    return context_call(
        kernel, cid, (first, second), (out, out),
        [
            pltpu.VMEM((4,) + piece, jnp.bfloat16),
            pltpu.VMEM((4,) + piece, jnp.bfloat16),
            pltpu.VMEM((2,) + piece, jnp.bfloat16),
            pltpu.SemaphoreType.DMA((6,)),
            pltpu.SemaphoreType.DMA((6,)),
        ],
    )


def line_total(cid, value):
    count = lax.axis_size(TENSOR)

    def kernel(value_ref, out_ref, slots, send, recv):
        at = lax.axis_index(TENSOR)
        others = [{TENSOR: (at + step) % count} for step in range(1, count)]
        greet(others)
        moves = [
            pltpu.make_async_remote_copy(
                src_ref=value_ref, dst_ref=slots.at[step], send_sem=send.at[step], recv_sem=recv.at[step],
                device_id=device, device_id_type=MESH_ID,
            )
            for step, device in enumerate(others)
        ]
        for move in moves:
            move.start()
        for move in moves:
            move.wait_recv()
        total = value_ref[...]
        for step in range(count - 1):
            total = total + slots[step]
        out_ref[...] = total
        for move in moves:
            move.wait_send()

    (total,) = context_call(
        kernel, cid, (value,), ((value.shape, jnp.float32),),
        [
            pltpu.VMEM((count - 1,) + value.shape, jnp.float32),
            pltpu.SemaphoreType.DMA((count - 1,)),
            pltpu.SemaphoreType.DMA((count - 1,)),
        ],
        5_000_000_000,
    )
    return total


def feed(normed, weight_in, weight_out):
    hidden = dot_rows(normed, weight_in)
    active = jax.nn.silu(hidden).astype(jnp.bfloat16)
    return dot_rows(active, weight_out).astype(jnp.bfloat16), (normed, hidden, active)


def feed_back(weight_in, weight_out, saved, branch_grad):
    normed, hidden, active = saved
    grad_out = dot_inner(active, branch_grad)
    unused, pullback = jax.vjp(jax.nn.silu, hidden)
    hidden_grad = pullback(dot_outer(branch_grad, weight_out))[0].astype(jnp.bfloat16)
    grad_in = dot_inner(normed, hidden_grad)
    return dot_outer(hidden_grad, weight_in).astype(jnp.bfloat16), grad_in, grad_out


QB = 128
BAND = 3 * QB
SPAN = 4 * QB
NT = (((1,), (1,)), ((), ()))


def span_table(relative):
    table = relative.astype(jnp.bfloat16)
    low = jnp.broadcast_to(table[:1], (2 * QB - 1 - LEFT, table.shape[1]))
    high = jnp.broadcast_to(table[-1:], (SPAN - (2 * QB - 1 - LEFT) - table.shape[0], table.shape[1]))
    spread = jnp.concatenate([low, table, high], axis=0)
    return jnp.concatenate([spread, spread], axis=1)


def fill_scores(first_block, q_mask, k_ref, span_ref, s_ref, edge_ref):
    keys = k_ref.shape[0]
    s_ref[:, QB : QB + keys] = lax.dot_general(q_mask, k_ref[...], NT, preferred_element_type=jnp.float32)
    spread = lax.dot_general(q_mask, span_ref[...], NT, preferred_element_type=jnp.float32)
    edge_ref[0] = jnp.broadcast_to(spread[:, :1], (QB, QB))
    edge_ref[1] = jnp.zeros((QB, QB), jnp.float32)
    edge_ref[2] = jnp.broadcast_to(spread[:, SPAN - 1 :], (QB, QB))
    skewed = pltpu.roll(spread, SPAN - (QB - 1), 1, stride=1, stride_axis=0)
    at = pl.ds(pl.multiple_of(first_block * QB, QB), BAND)
    s_ref[:, at] = s_ref[:, at] + skewed[:, :BAND]


def edge_of(block, first_block):
    return jnp.where(block < first_block - 1, 0, jnp.where(block > first_block + 1, 2, 1))


def forward_kernel(pos_ref, q_ref, k_ref, v_ref, span_ref, o_ref, lse_ref, s_ref, edge_ref, p_ref):
    keys = k_ref.shape[0]
    blocks = keys // QB
    first_block = pos_ref[0] * pl.num_programs(1) + pl.program_id(1)
    lane = lax.broadcasted_iota(jnp.int32, (QB, 2 * HEAD_DIM), 1)
    outs, lses = [], []
    for half in range(2):
        mine = (lane < HEAD_DIM) if half == 0 else (lane >= HEAD_DIM)
        q_mask = jnp.where(mine, q_ref[...], jnp.zeros_like(q_ref))
        fill_scores(first_block, q_mask, k_ref, span_ref, s_ref, edge_ref)
        top = None
        for block in range(blocks):
            z = s_ref[:, (block + 1) * QB : (block + 2) * QB] + edge_ref[edge_of(block, first_block)]
            top = z if top is None else jnp.maximum(top, z)
        top = jnp.max(top, axis=1, keepdims=True)
        edge_ref[...] = edge_ref[...] - top[None]
        total = None
        for block in range(blocks):
            z = s_ref[:, (block + 1) * QB : (block + 2) * QB] + edge_ref[edge_of(block, first_block)]
            p = jnp.exp(z)
            total = p if total is None else total + p
            p_ref[:, block * QB : (block + 1) * QB] = p.astype(jnp.bfloat16)
        total = jnp.sum(total, axis=1, keepdims=True)
        out = jnp.dot(p_ref[...], v_ref[...], preferred_element_type=jnp.float32) / total
        outs.append(out)
        lses.append(jnp.broadcast_to(top + jnp.log(total), (QB, 2 * HEAD_DIM)))
    low = lane < HEAD_DIM
    o_ref[...] = jnp.where(low, outs[0], outs[1]).astype(o_ref.dtype)
    lse_ref[...] = jnp.where(low, lses[0], lses[1])


def attention_forward(position, q, k, v, span):
    rows, width = q.shape
    keys = k.shape[0]
    pairs = width // (2 * HEAD_DIM)
    two = 2 * HEAD_DIM
    row_spec = pl.BlockSpec((QB, two), lambda p, b, pos: (b, p))
    key_spec = pl.BlockSpec((keys, two), lambda p, b, pos: (0, p))
    return pl.pallas_call(
        forward_kernel,
        out_shape=(
            jax.ShapeDtypeStruct((rows, width), jnp.bfloat16),
            jax.ShapeDtypeStruct((rows, width), jnp.float32),
        ),
        grid_spec=pltpu.PrefetchScalarGridSpec(
            num_scalar_prefetch=1,
            grid=(pairs, rows // QB),
            in_specs=[row_spec, key_spec, key_spec, pl.BlockSpec((SPAN, two), lambda p, b, pos: (0, 0))],
            out_specs=(row_spec, row_spec),
            scratch_shapes=[
                pltpu.VMEM((QB, keys + 2 * QB), jnp.float32),
                pltpu.VMEM((3, QB, QB), jnp.float32),
                pltpu.VMEM((QB, keys), jnp.bfloat16),
            ],
        ),
        compiler_params=pltpu.CompilerParams(vmem_limit_bytes=20 << 20),
        cost_estimate=pl.CostEstimate(flops=8 * rows * keys * width, bytes_accessed=4 * (keys + rows) * width, transcendentals=0),
        name="attention_forward",
    )(position.reshape(1), q, k, v, span)


def backward_kernel(pos_ref, q_ref, qt_ref, g_ref, gt_ref, o_ref, lse_ref, k_ref, v_ref, span_ref,
                    dq_ref, dkt_ref, dvt_ref, bins_ref, ends_ref,
                    s_ref, edge_ref, d_ref, p_ref, z_ref, wide_ref, dk_acc, dv_acc):
    keys = k_ref.shape[0]
    blocks = keys // QB
    step = pl.program_id(1)
    first_block = pos_ref[0] * pl.num_programs(1) + step
    lane = lax.broadcasted_iota(jnp.int32, (QB, 2 * HEAD_DIM), 1)

    @pl.when((pl.program_id(0) == 0) & (step == 0))
    def _():
        bins_ref[...] = jnp.zeros_like(bins_ref)
        ends_ref[...] = jnp.zeros_like(ends_ref)

    @pl.when(step == 0)
    def _():
        dk_acc[...] = jnp.zeros_like(dk_acc)
        dv_acc[...] = jnp.zeros_like(dv_acc)
        wide_ref[:, : 2 * HEAD_DIM] = k_ref[...]

    @pl.when((pl.program_id(0) == 0) & (step == 0))
    def _():
        z_ref[:, :QB] = jnp.zeros((QB, QB), jnp.bfloat16)
        z_ref[:, QB + keys :] = jnp.zeros((QB, QB), jnp.bfloat16)

    row_at = lax.broadcasted_iota(jnp.int32, (keys, QB), 0)
    col_at = lax.broadcasted_iota(jnp.int32, (keys, QB), 1)
    below = (row_at < (first_block - 1) * QB) & (col_at == 0)
    above = (row_at >= (first_block + 2) * QB) & (col_at == 1)
    wide_ref[:, 2 * HEAD_DIM :] = jnp.where(below | above, 1.0, 0.0).astype(jnp.bfloat16)

    flip_at = lax.broadcasted_iota(jnp.int32, (QB, QB), 0) + lax.broadcasted_iota(jnp.int32, (QB, QB), 1)
    flip = jnp.where(flip_at == QB - 1, 1.0, 0.0).astype(jnp.bfloat16)
    dqs = []
    for half in range(2):
        rows = slice(half * HEAD_DIM, (half + 1) * HEAD_DIM)
        mine = (lane < HEAD_DIM) if half == 0 else (lane >= HEAD_DIM)
        q_mask = jnp.where(mine, q_ref[...], jnp.zeros_like(q_ref))
        g_mask = jnp.where(mine, g_ref[...], jnp.zeros_like(g_ref))
        fill_scores(first_block, q_mask, k_ref, span_ref, s_ref, edge_ref)
        d_ref[...] = lax.dot_general(g_mask, v_ref[...], NT, preferred_element_type=jnp.float32)
        delta = jnp.sum(g_mask.astype(jnp.float32) * o_ref[...].astype(jnp.float32), axis=1, keepdims=True)
        lse = lse_ref[:, half * HEAD_DIM : half * HEAD_DIM + 1]
        edge_ref[...] = edge_ref[...] - lse[None]
        delta = jnp.broadcast_to(delta, (QB, QB))
        for block in range(blocks):
            here = slice(block * QB, (block + 1) * QB)
            there = slice((block + 1) * QB, (block + 2) * QB)
            p = jnp.exp(s_ref[:, there] + edge_ref[edge_of(block, first_block)])
            p_ref[:, here] = p.astype(jnp.bfloat16)
            z_ref[:, there] = (p * (d_ref[:, here] - delta)).astype(jnp.bfloat16)
        z_all = z_ref[:, QB : QB + keys]
        dv_acc[rows] += jnp.dot(gt_ref[rows], p_ref[...], preferred_element_type=jnp.float32)
        dk_acc[rows] += jnp.dot(qt_ref[rows], z_all, preferred_element_type=jnp.float32)
        dq = jnp.dot(z_all, wide_ref[...], preferred_element_type=jnp.float32)
        at = pl.ds(pl.multiple_of(first_block * QB, QB), BAND)
        band = jnp.dot(flip, z_ref[:, at], preferred_element_type=jnp.float32)
        band = jnp.concatenate([band, jnp.zeros((QB, SPAN - BAND), jnp.float32)], axis=1)
        spread = pltpu.roll(band, 0, 1, stride=1, stride_axis=0).astype(jnp.bfloat16)
        spread = jnp.dot(flip, spread, preferred_element_type=jnp.float32).astype(jnp.bfloat16)
        dq_rel = jnp.dot(spread, span_ref[...], preferred_element_type=jnp.float32)
        below_sum = dq[:, 2 * HEAD_DIM : 2 * HEAD_DIM + 1]
        above_sum = dq[:, 2 * HEAD_DIM + 1 : 2 * HEAD_DIM + 2]
        span_low = span_ref[:1, :].astype(jnp.float32)
        span_high = span_ref[SPAN - 1 :, :].astype(jnp.float32)
        dqs.append(dq[:, : 2 * HEAD_DIM] + dq_rel + below_sum * span_low + above_sum * span_high)
        bins_ref[...] += jnp.dot(qt_ref[rows], spread, preferred_element_type=jnp.float32)
        q_wide = q_mask.astype(jnp.float32)
        ends_ref[0:1, :] += jnp.sum(q_wide * below_sum, axis=0, keepdims=True)
        ends_ref[1:2, :] += jnp.sum(q_wide * above_sum, axis=0, keepdims=True)
    scale = 1.0 / 8.0
    dq_ref[...] = (jnp.where(lane < HEAD_DIM, dqs[0], dqs[1]) * scale).astype(dq_ref.dtype)

    @pl.when(step == pl.num_programs(1) - 1)
    def _():
        dkt_ref[...] = dk_acc[...].astype(dkt_ref.dtype)
        dvt_ref[...] = dv_acc[...].astype(dvt_ref.dtype)


def attention_backward(position, q, q_t, g, g_t, o, lse, k, v, span):
    rows, width = q.shape
    keys = k.shape[0]
    pairs = width // (2 * HEAD_DIM)
    two = 2 * HEAD_DIM
    row_spec = pl.BlockSpec((QB, two), lambda p, b, pos: (b, p))
    col_spec = pl.BlockSpec((two, QB), lambda p, b, pos: (p, b))
    key_spec = pl.BlockSpec((keys, two), lambda p, b, pos: (0, p))
    keyt_spec = pl.BlockSpec((two, keys), lambda p, b, pos: (p, 0))
    fixed = lambda shape: pl.BlockSpec(shape, lambda p, b, pos: (0, 0))
    dq, dkt, dvt, bins, ends = pl.pallas_call(
        backward_kernel,
        out_shape=(
            jax.ShapeDtypeStruct((rows, width), jnp.bfloat16),
            jax.ShapeDtypeStruct((width, keys), jnp.bfloat16),
            jax.ShapeDtypeStruct((width, keys), jnp.bfloat16),
            jax.ShapeDtypeStruct((HEAD_DIM, SPAN), jnp.float32),
            jax.ShapeDtypeStruct((8, two), jnp.float32),
        ),
        grid_spec=pltpu.PrefetchScalarGridSpec(
            num_scalar_prefetch=1,
            grid=(pairs, rows // QB),
            in_specs=[row_spec, col_spec, row_spec, col_spec, row_spec, row_spec, key_spec, key_spec, fixed((SPAN, two))],
            out_specs=(row_spec, keyt_spec, keyt_spec, fixed((HEAD_DIM, SPAN)), fixed((8, two))),
            scratch_shapes=[
                pltpu.VMEM((QB, keys + 2 * QB), jnp.float32),
                pltpu.VMEM((3, QB, QB), jnp.float32),
                pltpu.VMEM((QB, keys), jnp.float32),
                pltpu.VMEM((QB, keys), jnp.bfloat16),
                pltpu.VMEM((QB, keys + 2 * QB), jnp.bfloat16),
                pltpu.VMEM((keys, 2 * two), jnp.bfloat16),
                pltpu.VMEM((two, keys), jnp.float32),
                pltpu.VMEM((two, keys), jnp.float32),
            ],
        ),
        compiler_params=pltpu.CompilerParams(vmem_limit_bytes=20 << 20),
        cost_estimate=pl.CostEstimate(flops=20 * rows * keys * width, bytes_accessed=8 * (keys + rows) * width, transcendentals=0),
        name="attention_backward",
    )(position.reshape(1), q, q_t, g, g_t, o, lse, k, v, span)
    at = 2 * QB - 1 - LEFT
    ends = ends[:2, :HEAD_DIM] + ends[:2, HEAD_DIM:]
    spread = bins.T
    inner = spread[at + 1 : at + LEFT + RIGHT]
    low = jnp.sum(spread[: at + 1], axis=0) + ends[0]
    high = jnp.sum(spread[at + LEFT + RIGHT :], axis=0) + ends[1]
    table = jnp.concatenate([low[None], inner, high[None]], axis=0)
    return dq, dkt, dvt, table


def attend_forward(normed, weight_in, weight_out, relative, position):
    projected = jnp.einsum(
        "td,kde->kte", normed, weight_in, preferred_element_type=jnp.float32
    ).astype(jnp.bfloat16)
    key_rows, value_rows = gather_context(10, projected[1], projected[2])
    queries = projected[0] * jnp.bfloat16(1.0 / math.sqrt(HEAD_DIM))
    span = span_table(relative)
    mixed, log_total = attention_forward(position, queries, key_rows, value_rows, span)
    return (
        dot_rows(mixed, weight_out).astype(jnp.bfloat16),
        (normed, queries, key_rows, value_rows, log_total, mixed, span),
    )


def attend_backward(weight_in, weight_out, position, saved, branch_grad):
    normed, queries, key_rows, value_rows, log_total, mixed, span = saved
    grad_out = dot_inner(mixed, branch_grad)
    mixed_grad = dot_outer(branch_grad, weight_out).astype(jnp.bfloat16)
    query_grad, key_grad, value_grad, table_grad = attention_backward(
        position, queries, queries.T, mixed_grad, mixed_grad.T, mixed, log_total, key_rows, value_rows, span
    )
    key_grad, value_grad = scatter_context(11, key_grad, value_grad)
    stacked = jnp.stack([query_grad, key_grad.T, value_grad.T])
    grad_in = jnp.einsum("td,kte->kde", normed, stacked, preferred_element_type=jnp.float32)
    partial_sum = jnp.einsum("kte,kde->td", stacked, weight_in, preferred_element_type=jnp.float32)
    return (partial_sum.astype(jnp.bfloat16), table_grad, grad_in, grad_out)


def channel_sums(cid, first, second):
    total = line_total(cid, jnp.concatenate([first, second]).reshape(-1, 128)).reshape(2, -1)
    return total[0], total[1]


def conv_forward(normed, weight_in, weight_out, depthwise, gain_middle):
    projected = jnp.einsum("td,kde->kte", normed, weight_in, preferred_element_type=jnp.float32)
    gated = gate_unit(projected[0], projected[1])
    rows_here = gated.shape[0]
    reach_rows = depthwise.shape[0] - 1
    edge_rows = shifted_2(gated[rows_here - reach_rows :], CONTEXT, 1)
    padded = jnp.concatenate([edge_rows, gated], axis=0)
    mixed = depthwise[0] * padded[0:rows_here]
    for offset in range(1, reach_rows + 1):
        mixed = mixed + depthwise[offset] * padded[offset : offset + rows_here]
    row_sums, row_squares = channel_sums(12, jnp.sum(mixed, axis=1), jnp.sum(mixed * mixed, axis=1))
    row_mean = row_sums / D
    inverse = lax.rsqrt(row_squares / D - row_mean * row_mean + epsilon)
    scaled = (mixed - row_mean[:, None]) * inverse[:, None]
    shaped = scaled * gain_middle
    active = jax.nn.silu(shaped).astype(jnp.bfloat16)
    return (
        dot_rows(active, weight_out).astype(jnp.bfloat16),
        (normed, projected, padded, scaled, inverse, shaped, active),
    )


def conv_backward(weight_in, weight_out, depthwise, gain_middle, saved, branch_grad):
    normed, projected, padded, scaled, inverse, shaped, active = saved
    rows_here = scaled.shape[0]
    reach_rows = depthwise.shape[0] - 1
    grad_out = dot_inner(active, branch_grad)
    unused, pullback = jax.vjp(jax.nn.silu, shaped)
    shaped_grad = pullback(dot_outer(branch_grad, weight_out))[0]
    middle_grad = jnp.sum(shaped_grad * scaled, axis=0)
    scaled_grad = shaped_grad * gain_middle
    first_sum, second_sum = channel_sums(13, jnp.sum(scaled_grad, axis=1), jnp.sum(scaled_grad * scaled, axis=1))
    mixed_grad = inverse[:, None] * (
        scaled_grad - first_sum[:, None] / D - scaled * (second_sum[:, None] / D)
    )
    next_rows = shifted_2(mixed_grad[:reach_rows], CONTEXT, -1)
    padded_grad = jnp.concatenate([mixed_grad, next_rows], axis=0)
    gated_grad = depthwise[reach_rows] * padded_grad[0:rows_here]
    for offset in range(1, reach_rows + 1):
        gated_grad = gated_grad + depthwise[reach_rows - offset] * padded_grad[offset : offset + rows_here]
    depth_grad = jnp.stack(
        [
            jnp.sum(padded[offset : offset + rows_here] * mixed_grad, axis=0)
            for offset in range(reach_rows + 1)
        ]
    )
    unused, pullback = jax.vjp(gate_unit, projected[0], projected[1])
    unit_grad, gate_grad = pullback(gated_grad)
    stacked = jnp.stack([unit_grad, gate_grad]).astype(jnp.bfloat16)
    grad_in = jnp.einsum("td,kte->kde", normed, stacked, preferred_element_type=jnp.float32)
    partial_sum = jnp.einsum("kte,kde->td", stacked, weight_in, preferred_element_type=jnp.float32)
    return (partial_sum.astype(jnp.bfloat16), grad_in, grad_out, middle_grad, depth_grad)


def local(
    inputs,
    gain_first,
    first_in,
    first_out,
    gain_attend,
    attend_in,
    attend_out,
    relative,
    gain_convolve,
    convolve_in,
    depthwise,
    gain_middle,
    convolve_out,
    gain_second,
    second_in,
    second_out,
    gain_final,
    cotangent,
):
    position = lax.axis_index(CONTEXT)
    start_rows = inputs[0]
    small_plane = lax.axis_size(CLIPS) == 2
    weights = {
        FIRST: (first_in, first_out),
        ATTEND: (attend_in, attend_out),
        CONVOLVE: (convolve_in, convolve_out),
        SECOND: (second_in, second_out),
    }
    held, grads = {}, {}

    def collecting(name):
        if not small_plane:
            return (), ()
        pair = tuple(weight.astype(jnp.bfloat16) for weight in weights[name])
        return tuple(Gather(wide, weight.shape) for wide, weight in zip((False, True), pair)), pair

    def collect(name, gathered):
        held[name] = gathered if small_plane else fetch(*weights[name])

    def spreading(grad_in, grad_out):
        if not small_plane:
            return (), ()
        pair = (grad_in.astype(jnp.bfloat16), grad_out.astype(jnp.bfloat16))
        return tuple(Scatter(wide, grad.shape) for wide, grad in zip((False, True), pair)), pair

    def with_small(rest, kind, value):
        if not small_plane:
            return rest
        return rest[0] + (kind(value.shape),), rest[1] + (value,)

    def spread(name, scattered, grad_in, grad_out):
        grads[name] = scattered if small_plane else send_grads(grad_in, grad_out)

    tasks, pair = collecting(FIRST)
    collect(FIRST, plane_call(9, tasks, pair) if small_plane else None)
    normed = layer_norm(start_rows.astype(jnp.float32), gain_first).astype(jnp.bfloat16)
    branch, first_saved = feed(normed, *held[FIRST])
    (after_first, normed), got = forward_sum(1, branch, start_rows, gain_attend, 0.5, *collecting(ATTEND))
    collect(ATTEND, got)
    branch, attend_saved = attend_forward(normed, *held[ATTEND], relative, position)
    (after_attend, normed), got = forward_sum(2, branch, after_first, gain_convolve, 1.0, *collecting(CONVOLVE))
    collect(CONVOLVE, got)
    branch, convolve_saved = conv_forward(normed, *held[CONVOLVE], depthwise, gain_middle)
    (after_convolve, normed), got = forward_sum(3, branch, after_attend, gain_second, 1.0, *collecting(SECOND))
    collect(SECOND, got)
    branch, second_saved = feed(normed, *held[SECOND])
    final_out, upstream, branch_grad, grad_final = turn_sum(4, branch, after_convolve, gain_final, cotangent[0])
    branch, *pair = feed_back(*held[SECOND], second_saved, branch_grad)
    (upstream, branch_grad, grad_gain_second), got = backward_sum(
        5, branch, after_convolve, gain_second, upstream, 1.0, *spreading(*pair)
    )
    spread(SECOND, got, *pair)
    branch, *pair, grad_middle, grad_depth = conv_backward(
        *held[CONVOLVE], depthwise, gain_middle, convolve_saved, branch_grad
    )
    (upstream, branch_grad, grad_gain_convolve), got = backward_sum(
        6, branch, after_attend, gain_convolve, upstream, 1.0, *spreading(*pair)
    )
    spread(CONVOLVE, got, *pair)
    branch, table_grad, *pair = attend_backward(*held[ATTEND], position, attend_saved, branch_grad)
    shared = jnp.pad(table_grad.reshape(-1), (0, -table_grad.size % 1024)).reshape(-1, 128)
    (upstream, branch_grad, grad_gain_attend), got = backward_sum(
        7, branch, after_first, gain_attend, upstream, 0.5, *with_small(spreading(*pair), LineSum, shared)
    )
    spread(ATTEND, got[:2], *pair)
    branch, *pair = feed_back(*held[FIRST], first_saved, branch_grad)
    gains = [
        jnp.sum(part, axis=0) for part in (grad_gain_attend, grad_gain_convolve, grad_gain_second, grad_final)
    ]
    smalls = [*gains, grad_middle, grad_depth.reshape(-1)]
    sizes = [part.shape[0] for part in smalls]
    packed = jnp.concatenate(smalls).reshape(-1, 128)
    if small_plane:
        packed = jnp.concatenate([packed, got[2]], axis=0)
    (upstream, branch_grad, grad_gain_first), got = backward_sum(
        8, branch, start_rows, gain_first, upstream, 1.0, *with_small(spreading(*pair), PlaneSum, packed)
    )
    spread(FIRST, got[:2], *pair)
    grad_gain_first = jnp.sum(grad_gain_first, axis=0)
    if small_plane:
        packed = got[2].reshape(-1)
        (grad_gain_first,) = plane_call(14, (PlaneSum((8, 128)),), (grad_gain_first.reshape(8, 128),))
        grad_gain_first = grad_gain_first.reshape(-1)
        table_grad = packed[sum(sizes) : sum(sizes) + table_grad.size].reshape(table_grad.shape)
    else:
        table_grad = lax.psum(table_grad, (CLIPS, CONTEXT, TENSOR))
        packed, grad_gain_first = lax.psum((packed.reshape(-1), grad_gain_first), (CLIPS, CONTEXT))
    smalls, at = [], 0
    for size in sizes:
        smalls.append(packed[at : at + size])
        at += size
    grad_depth = smalls[5].reshape(depthwise.shape)
    return (
        final_out[None],
        upstream[None],
        grad_gain_first,
        grads[FIRST][0],
        grads[FIRST][1],
        smalls[0],
        grads[ATTEND][0],
        grads[ATTEND][1],
        table_grad,
        smalls[1],
        grads[CONVOLVE][0],
        grad_depth,
        smalls[4],
        grads[CONVOLVE][1],
        smalls[2],
        grads[SECOND][0],
        grads[SECOND][1],
        smalls[3],
    )


def solution(mesh):
    placed = (
        P(CLIPS, CONTEXT, None),
        P(),
        P((CLIPS, CONTEXT), TENSOR),
        P(TENSOR, (CLIPS, CONTEXT)),
        P(),
        P(None, (CLIPS, CONTEXT), TENSOR),
        P(TENSOR, (CLIPS, CONTEXT)),
        P(),
        P(),
        P(None, (CLIPS, CONTEXT), TENSOR),
        P(None, TENSOR),
        P(TENSOR),
        P(TENSOR, (CLIPS, CONTEXT)),
        P(),
        P((CLIPS, CONTEXT), TENSOR),
        P(TENSOR, (CLIPS, CONTEXT)),
        P(),
        P(CLIPS, CONTEXT, None),
    )
    return jax.shard_map(
        local,
        mesh=mesh,
        in_specs=placed,
        out_specs=(
            P(CLIPS, CONTEXT, None),
            P(CLIPS, CONTEXT, None),
            P(),
            P((CLIPS, CONTEXT), TENSOR),
            P(TENSOR, (CLIPS, CONTEXT)),
            P(),
            P(None, (CLIPS, CONTEXT), TENSOR),
            P(TENSOR, (CLIPS, CONTEXT)),
            P(),
            P(),
            P(None, (CLIPS, CONTEXT), TENSOR),
            P(None, TENSOR),
            P(TENSOR),
            P(TENSOR, (CLIPS, CONTEXT)),
            P(),
            P((CLIPS, CONTEXT), TENSOR),
            P(TENSOR, (CLIPS, CONTEXT)),
            P(),
        ),
        check_vma=False,
    )
```

```python
import math

import jax
import jax.numpy as jnp
from jax import lax
from jax.experimental import pallas as pl
from jax.experimental.pallas import tpu as pltpu
from jax.sharding import PartitionSpec as P

CLIPS, CONTEXT, TENSOR = "clips", "context", "tensor"
D = 1024
HEAD_DIM = 64
LEFT = 64
RIGHT = 8

epsilon = 1e-05


def shifted_2(value, axis, steps):
    count = lax.axis_size(axis)
    initial, last = (max(0, -steps), min(count, count - steps))
    return lax.ppermute(value, axis, [(source, source + steps) for source in range(initial, last)])


def dot_rows(former, latter):
    return jnp.dot(former, latter, preferred_element_type=jnp.float32)


def dot_inner(former, latter):
    return lax.dot_general(
        former, latter, (((0,), (0,)), ((), ())), preferred_element_type=jnp.float32
    )


def dot_outer(former, latter):
    return lax.dot_general(
        former, latter, (((1,), (1,)), ((), ())), preferred_element_type=jnp.float32
    )


def layer_norm(rows_in, gain_vec):
    row_mean = jnp.mean(rows_in, axis=-1, keepdims=True)
    centred = rows_in - row_mean
    variance = jnp.mean(centred * centred, axis=-1, keepdims=True)
    return centred * lax.rsqrt(variance + epsilon) * gain_vec


def gate_unit(unit_half, gate_half):
    return unit_half * jax.nn.sigmoid(gate_half)


def fetch(weight_in, weight_out):
    return (
        lax.all_gather(weight_in.astype(jnp.bfloat16), (CLIPS, CONTEXT), axis=weight_in.ndim - 2, tiled=True),
        lax.all_gather(weight_out.astype(jnp.bfloat16), (CLIPS, CONTEXT), axis=1, tiled=True),
    )


def scatter_sum(grad, axis):
    summed = lax.psum_scatter(
        grad.astype(jnp.bfloat16), (CLIPS, CONTEXT), scatter_dimension=axis, tiled=True
    )
    return summed.astype(jnp.float32)


def send_grads(grad_in, grad_out):
    return (scatter_sum(grad_in, grad_in.ndim - 2), scatter_sum(grad_out, 1))


MESH_ID = pl.DeviceIdType.MESH
CHUNKS = 16
LAG = 3
FULL, TOP, BOTTOM = 0, 1, 2
FIRST, ATTEND, CONVOLVE, SECOND = range(4)


def near():
    across_clips = lax.axis_index(CLIPS)
    along = lax.axis_index(CONTEXT)
    deep, core = along // 2, along % 2
    devices = (
        {CLIPS: 1 - across_clips},
        {CONTEXT: (1 - deep) * 2 + core},
        {CONTEXT: deep * 2 + 1 - core},
    )
    return (across_clips, deep, core), devices


def greet(devices):
    barrier = pltpu.get_barrier_semaphore()
    for device in devices:
        pl.semaphore_signal(barrier, inc=1, device_id=device, device_id_type=MESH_ID)
    pl.semaphore_wait(barrier, len(devices))


def part_of(ref, wide, count, shard, part):
    if wide:
        size = ref.shape[-1] // count
        rows = ref.shape[-2]
        along = slice(None) if part == FULL else pl.ds((part - 1) * (rows // 2), rows // 2)
        return ref.at[along, pl.ds(pl.multiple_of(shard * size, 128), size)]
    size = ref.shape[-2] // count
    start, length = shard * size, size
    if part != FULL:
        length = size // 2
        start = start + (part - 1) * length
    window = pl.ds(pl.multiple_of(start, 16), length)
    return ref.at[window] if len(ref.shape) == 2 else ref.at[:, window]


def half_of(ref, part):
    length = ref.shape[-2] // 2
    window = pl.ds((part - 1) * length, length)
    return ref.at[window] if len(ref.shape) == 2 else ref.at[:, window]


class Gather:
    copies = 9
    line = False

    def __init__(self, wide, shard_shape):
        self.wide = wide
        self.shape = shard_shape[:-2] + (
            (shard_shape[-2], shard_shape[-1] * 8) if wide else (shard_shape[-2] * 8, shard_shape[-1])
        )

    def outs(self):
        return [(self.shape, jnp.bfloat16)]

    def scratch(self):
        return [pltpu.SemaphoreType.DMA((self.copies,)), pltpu.SemaphoreType.DMA((self.copies,)), pltpu.SemaphoreType.DMA]

    def bind(self, ins, outs, scratch):
        (shard_ref,), (full_ref,) = ins, outs
        send, recv, own_sem = scratch
        (x, y, core), (to_x, to_y, to_core) = near()
        shard = lambda a, b: a * 4 + b * 2 + core
        own, at_x, at_y, at_far = shard(x, y), shard(1 - x, y), shard(x, 1 - y), shard(1 - x, 1 - y)
        place = lambda which, part: part_of(full_ref, self.wide, 8, which, part)

        def copy(index, source, which, part, device):
            return pltpu.make_async_remote_copy(
                src_ref=source, dst_ref=place(which, part), send_sem=send.at[index], recv_sem=recv.at[index],
                device_id=device, device_id_type=MESH_ID,
            )

        passed = lambda index, which, part, device: copy(index, place(which, part), which, part, device)
        moves = [
            copy(0, shard_ref, own, FULL, to_x),
            copy(1, shard_ref, own, FULL, to_y),
            copy(2, shard_ref, own, FULL, to_core),
            passed(3, at_x, TOP, to_y),
            passed(4, at_x, FULL, to_core),
            passed(5, at_y, BOTTOM, to_x),
            passed(6, at_y, FULL, to_core),
            passed(7, at_far, TOP, to_core),
            passed(8, at_far, BOTTOM, to_core),
        ]
        mine = pltpu.make_async_copy(shard_ref, place(own, FULL), own_sem)

        def begin():
            for index in (0, 1, 2):
                moves[index].start()
            mine.start()

        def second():
            moves[0].wait_recv()
            moves[3].start()
            moves[4].start()
            moves[1].wait_recv()
            moves[5].start()
            moves[6].start()

        def third():
            moves[3].wait_recv()
            moves[7].start()
            moves[5].wait_recv()
            moves[8].start()

        def last():
            for index in (2, 4, 6, 7, 8):
                moves[index].wait_recv()
            mine.wait()
            for move in moves:
                move.wait_send()

        return begin, [second, third], last


class Scatter:
    copies = 8
    line = False

    def __init__(self, wide, full_shape):
        self.wide = wide
        self.shape = full_shape[:-2] + (
            (full_shape[-2], full_shape[-1] // 8) if wide else (full_shape[-2] // 8, full_shape[-1])
        )

    def outs(self):
        return [(self.shape, jnp.float32)]

    def scratch(self):
        half = self.shape[:-2] + (self.shape[-2] // 2, self.shape[-1])
        return [
            pltpu.VMEM((4,) + self.shape, jnp.bfloat16),
            pltpu.VMEM((4,) + self.shape, jnp.bfloat16),
            pltpu.VMEM((2,) + self.shape, jnp.bfloat16),
            pltpu.VMEM((2,) + half, jnp.bfloat16),
            pltpu.SemaphoreType.DMA((self.copies,)),
            pltpu.SemaphoreType.DMA((self.copies,)),
        ]

    def bind(self, ins, outs, scratch):
        (full_ref,), (out_ref,) = ins, outs
        from_core, pair, whole, halves, send, recv = scratch
        (x, y, core), (to_x, to_y, to_core) = near()

        def copy(index, source, target, device):
            return pltpu.make_async_remote_copy(
                src_ref=source, dst_ref=target, send_sem=send.at[index], recv_sem=recv.at[index],
                device_id=device, device_id_type=MESH_ID,
            )

        place = lambda slot, at_core: part_of(full_ref, self.wide, 8, slot * 2 + at_core, FULL)
        own, at_x, at_y, at_far = x * 2 + y, (1 - x) * 2 + y, x * 2 + 1 - y, (1 - x) * 2 + 1 - y
        moves = [copy(slot, place(slot, 1 - core), from_core.at[slot], to_core) for slot in range(4)]
        moves += [
            copy(4, half_of(pair.at[at_far], TOP), halves.at[0], to_x),
            copy(5, half_of(pair.at[at_far], BOTTOM), halves.at[1], to_y),
            copy(6, pair.at[at_x], whole.at[0], to_x),
            copy(7, pair.at[at_y], whole.at[1], to_y),
        ]
        wide = lambda ref: ref[...].astype(jnp.float32)

        def begin():
            for slot in range(4):
                moves[slot].start()

        def second():
            for slot in range(4):
                moves[slot].wait_recv()
                pair[slot] = (wide(place(slot, core)) + wide(from_core.at[slot])).astype(jnp.bfloat16)
            moves[4].start()
            moves[5].start()

        def third():
            moves[4].wait_recv()
            target = half_of(pair.at[at_y], TOP)
            target[...] = (wide(target) + wide(halves.at[0])).astype(jnp.bfloat16)
            moves[7].start()
            moves[5].wait_recv()
            target = half_of(pair.at[at_x], BOTTOM)
            target[...] = (wide(target) + wide(halves.at[1])).astype(jnp.bfloat16)
            moves[6].start()

        def last():
            moves[6].wait_recv()
            moves[7].wait_recv()
            out_ref[...] = wide(pair.at[own]) + wide(whole.at[0]) + wide(whole.at[1])
            for move in moves:
                move.wait_send()

        return begin, [second, third], last


class PlaneSum:
    line = False

    def __init__(self, shape):
        self.shape = shape

    def outs(self):
        return [(self.shape, jnp.float32)]

    def scratch(self):
        return [
            pltpu.VMEM((3,) + self.shape, jnp.float32),
            pltpu.VMEM((2,) + self.shape, jnp.float32),
            pltpu.SemaphoreType.DMA((3,)),
            pltpu.SemaphoreType.DMA((3,)),
        ]

    def bind(self, ins, outs, scratch):
        (value_ref,), (out_ref,) = ins, outs
        slots, totals, send, recv = scratch
        to_x, to_y, to_core = near()[1]
        moves = [
            pltpu.make_async_remote_copy(
                src_ref=source, dst_ref=slots.at[index], send_sem=send.at[index], recv_sem=recv.at[index],
                device_id=device, device_id_type=MESH_ID,
            )
            for index, (source, device) in enumerate(
                ((value_ref, to_core), (totals.at[0], to_y), (totals.at[1], to_x))
            )
        ]

        def begin():
            moves[0].start()

        def second():
            moves[0].wait_recv()
            totals[0] = value_ref[...] + slots[0]
            moves[1].start()

        def third():
            moves[1].wait_recv()
            totals[1] = totals[0] + slots[1]
            moves[2].start()

        def last():
            moves[2].wait_recv()
            out_ref[...] = totals[1] + slots[2]
            for move in moves:
                move.wait_send()

        return begin, [second, third], last


class LineSum:
    line = True

    def __init__(self, shape):
        self.shape = shape

    def outs(self):
        return [(self.shape, jnp.float32)]

    def scratch(self):
        return [
            pltpu.VMEM((4,) + self.shape, jnp.float32),
            pltpu.SemaphoreType.DMA((4,)),
            pltpu.SemaphoreType.DMA((4,)),
        ]

    def bind(self, ins, outs, scratch):
        (value_ref,), (out_ref,) = ins, outs
        slots, send, recv = scratch
        at = lax.axis_index(TENSOR)

        def copy(step, slot):
            return pltpu.make_async_remote_copy(
                src_ref=value_ref, dst_ref=slots.at[slot], send_sem=send.at[step], recv_sem=recv.at[slot],
                device_id={TENSOR: (at + step) % 4}, device_id_type=MESH_ID,
            )

        def begin():
            for step in range(1, 4):
                copy(step, at).start()
            slots[at] = value_ref[...]

        def last():
            for step in range(1, 4):
                copy(step, (at + step) % 4).wait_recv()
            out_ref[...] = slots[0] + slots[1] + slots[2] + slots[3]
            for step in range(1, 4):
                copy(step, at).wait_send()

        return begin, [lambda: None, lambda: None], last


def bind_all(tasks, ins, outs, scratch):
    begins, middles, lasts = [], [], []
    for task, task_in, task_out in zip(tasks, ins, outs):
        count = len(task.scratch())
        begin, steps, last = task.bind((task_in,), (task_out,), scratch[:count])
        scratch = scratch[count:]
        begins.append(begin)
        middles.append(steps)
        lasts.append(last)
    return begins, [step for turn in zip(*middles) for step in turn], lasts


def plane_call(cid, tasks, operands):
    vmem = pl.BlockSpec(memory_space=pltpu.VMEM)
    outs = [out for task in tasks for out in task.outs()]

    def kernel(*refs):
        n = len(tasks)
        greet(near()[1])
        begins, steps, lasts = bind_all(tasks, refs[:n], refs[n : 2 * n], refs[2 * n :])
        for step in begins + steps + lasts:
            step()

    return pl.pallas_call(
        kernel,
        out_shape=tuple(jax.ShapeDtypeStruct(shape, kind) for shape, kind in outs),
        in_specs=[vmem] * len(operands),
        out_specs=(vmem,) * len(outs),
        scratch_shapes=[piece for task in tasks for piece in task.scratch()],
        compiler_params=pltpu.CompilerParams(collective_id=cid, has_side_effects=True, vmem_limit_bytes=12 << 20),
        cost_estimate=pl.CostEstimate(flops=30_000_000_000, bytes_accessed=50_000_000, transcendentals=0),
        name=f"call_{cid}",
    )(*operands)


def line_sum(axis, partial_ref, acc_ref, from_end, from_mid, total_ref, send_sem, recv_sem, finish, others, whole_line, begins, steps, lasts):
    at = lax.axis_index(axis)
    low = at < 2
    end = jnp.where(low, 0, 3)
    mid = jnp.where(low, 1, 2)
    other = jnp.where(low, 2, 1)
    is_mid = at == mid
    rest = [{axis: (at + step) % 4} for step in range(1, 4)]
    size = partial_ref.shape[0] // CHUNKS

    gap = max((CHUNKS - LAG) // (len(steps) + 1), 1)

    def rows(chunk):
        return pl.ds(pl.multiple_of(chunk * size, size), size)

    def hop(stage, chunk, source, target, device):
        return pltpu.make_async_remote_copy(
            src_ref=source.at[rows(chunk)],
            dst_ref=target.at[rows(chunk)],
            send_sem=send_sem.at[stage, chunk],
            recv_sem=recv_sem.at[stage, chunk],
            device_id={axis: device},
            device_id_type=MESH_ID,
        )

    inward = lambda chunk: hop(0, chunk, partial_ref, from_end, mid)
    across = lambda chunk: hop(1, chunk, acc_ref, from_mid, other)
    outward = lambda chunk: hop(2, chunk, total_ref, total_ref, end)

    def loop(low, high, body):
        def step(chunk, carry):
            body(chunk)
            return carry

        lax.fori_loop(low, high, step, 0)

    def beside(chunk):
        for index, step in enumerate(steps):
            pl.when(chunk == LAG + gap * (1 + index))(step)

    @pl.when(is_mid)
    def _():
        greet((rest if whole_line else [{axis: end}, {axis: other}]) + others)
        for begin in begins:
            begin()

        def first(chunk):
            inward(chunk).wait_recv()
            here = rows(chunk)
            acc_ref[here] = (partial_ref[here].astype(jnp.float32) + from_end[here].astype(jnp.float32)).astype(acc_ref.dtype)
            across(chunk).start()

        def second(chunk):
            across(chunk).wait_recv()
            here = rows(chunk)
            total_ref[here] = (acc_ref[here].astype(jnp.float32) + from_mid[here].astype(jnp.float32)).astype(total_ref.dtype)
            outward(chunk).start()
            finish(here)

        def both(chunk):
            first(chunk)
            second(chunk - LAG)
            beside(chunk)

        loop(0, LAG, first)
        loop(LAG, CHUNKS, both)
        loop(CHUNKS - LAG, CHUNKS, second)

        def drain(chunk):
            across(chunk).wait_send()
            outward(chunk).wait_send()

        loop(0, CHUNKS, drain)

    @pl.when(jnp.logical_not(is_mid))
    def _():
        greet((rest if whole_line else [{axis: mid}]) + others)
        loop(0, CHUNKS, lambda chunk: inward(chunk).start())
        for begin in begins:
            begin()

        def receive(chunk):
            beside(chunk + LAG)
            outward(chunk).wait_recv()
            finish(rows(chunk))

        loop(0, CHUNKS, receive)
        loop(0, CHUNKS, lambda chunk: inward(chunk).wait_send())

    for last in lasts:
        last()


def unit_rows(rows_in):
    mean = jnp.mean(rows_in, axis=-1, keepdims=True)
    centred = rows_in - mean
    variance = jnp.mean(centred * centred, axis=-1, keepdims=True)
    inverse = lax.rsqrt(variance + epsilon)
    return centred * inverse, inverse


def rows_back(unit, inverse, scaled):
    return inverse * (
        scaled
        - jnp.mean(scaled, axis=-1, keepdims=True)
        - unit * jnp.mean(scaled * unit, axis=-1, keepdims=True)
    )


def gather_eight(value):
    total = value[:8]
    for at in range(8, value.shape[0], 8):
        total = total + value[at : at + 8]
    return total


def sum_call(body, cid, partial, operands, outs, tasks, task_operands):
    rows, width = partial.shape
    chunk_shape = pltpu.VMEM((rows, width), jnp.bfloat16)
    vmem = pl.BlockSpec(memory_space=pltpu.VMEM)
    far = [at for at, operand in enumerate(operands) if operand.shape[0] == rows]
    kinds = [pl.BlockSpec(memory_space=pltpu.HBM) if at in far else vmem for at in range(len(operands))]
    task_outs = [out for task in tasks for out in task.outs()]
    grant = (30 if any(isinstance(task, Scatter) for task in tasks) else 22) << 20
    pieces = [piece for task in tasks for piece in task.scratch()]

    def kernel(partial_ref, *refs):
        def take(count):
            nonlocal refs
            taken, refs = refs[:count], refs[count:]
            return taken

        ins, task_ins = take(len(operands)), take(len(tasks))
        results, task_results = take(len(outs)), take(len(tasks))
        acc, from_end, from_mid, total, send_sem, recv_sem = take(6)
        copies, fetch_sem = take(len(far)), take(1)[0]
        fetches = [
            pltpu.make_async_copy(ins[at], held, fetch_sem.at[index]) for index, (at, held) in enumerate(zip(far, copies))
        ]
        for fetched in fetches:
            fetched.start()
        ins = [copies[far.index(at)] if at in far else ref for at, ref in enumerate(ins)]
        begins, steps, lasts, others = [], [], [], []
        if tasks:
            others = list(near()[1])
            begins, steps, lasts = bind_all(tasks, task_ins, task_results, refs)
        start, finish = body(total, ins, results)
        start()

        def arrive():
            for fetched in fetches:
                fetched.wait()

        begins.append(arrive)
        line_sum(
            TENSOR, partial_ref, acc, from_end, from_mid, total, send_sem, recv_sem, finish, others,
            any(task.line for task in tasks), begins, steps, lasts,
        )

    got = pl.pallas_call(
        kernel,
        out_shape=tuple(jax.ShapeDtypeStruct(shape, kind) for shape, kind in list(outs) + task_outs),
        in_specs=[vmem] + kinds + [vmem] * len(tasks),
        out_specs=(vmem,) * (len(outs) + len(tasks)),
        scratch_shapes=[chunk_shape] * 4
        + [pltpu.SemaphoreType.DMA((3, CHUNKS)), pltpu.SemaphoreType.DMA((3, CHUNKS))]
        + [pltpu.VMEM(operands[at].shape, operands[at].dtype) for at in far]
        + [pltpu.SemaphoreType.DMA((len(far),))]
        + pieces,
        compiler_params=pltpu.CompilerParams(collective_id=cid, has_side_effects=True, vmem_limit_bytes=grant),
        cost_estimate=pl.CostEstimate(flops=60_000_000_000, bytes_accessed=100_000_000, transcendentals=0),
        name=f"call_{cid}",
    )(partial, *operands, *task_operands)
    return got[: len(outs)], got[len(outs) :]


def forward_sum(cid, partial, rows_in, gain, scale, tasks=(), task_operands=()):
    def body(total, ins, results):
        x_ref, gain_ref = ins
        x_out, a_out = results

        def finish(here):
            x = x_ref[here].astype(jnp.float32) + scale * total[here].astype(jnp.float32)
            x_out[here] = x
            a_out[here] = (unit_rows(x)[0] * gain_ref[...]).astype(a_out.dtype)

        return lambda: None, finish

    shape = partial.shape
    return sum_call(
        body, cid, partial, (rows_in, gain.reshape(1, -1)),
        ((shape, jnp.float32), (shape, jnp.bfloat16)), tasks, task_operands,
    )


def turn_sum(cid, partial, rows_in, gain, cotangent):
    def body(total, ins, results):
        x_ref, gain_ref, cot_ref = ins
        out_ref, d_ref, half_ref, gain_grad_ref = results

        def start():
            gain_grad_ref[...] = jnp.zeros_like(gain_grad_ref)

        def finish(here):
            x = x_ref[here] + 0.5 * total[here].astype(jnp.float32)
            unit, inverse = unit_rows(x)
            out_ref[here] = (unit * gain_ref[...]).astype(out_ref.dtype)
            upstream = cot_ref[here].astype(jnp.float32)
            d = rows_back(unit, inverse, upstream * gain_ref[...])
            d_ref[here] = d
            half_ref[here] = (0.5 * d).astype(half_ref.dtype)
            gain_grad_ref[...] += gather_eight(upstream * unit)

        return start, finish

    shape = partial.shape
    (out, d, half, gain_grad), _ = sum_call(
        body, cid, partial, (rows_in, gain.reshape(1, -1), cotangent),
        ((shape, jnp.bfloat16), (shape, jnp.float32), (shape, jnp.bfloat16), ((8, shape[1]), jnp.float32)), (), (),
    )
    return out, d, half, gain_grad


def backward_sum(cid, partial, rows_in, gain, upstream, scale, tasks=(), task_operands=()):
    def body(total, ins, results):
        x_ref, gain_ref, up_ref = ins
        d_ref, half_ref, gain_grad_ref = results

        def start():
            gain_grad_ref[...] = jnp.zeros_like(gain_grad_ref)

        def finish(here):
            unit, inverse = unit_rows(x_ref[here].astype(jnp.float32))
            normed_grad = total[here].astype(jnp.float32)
            d = up_ref[here] + rows_back(unit, inverse, normed_grad * gain_ref[...])
            d_ref[here] = d
            half_ref[here] = (scale * d).astype(half_ref.dtype)
            gain_grad_ref[...] += gather_eight(normed_grad * unit)

        return start, finish

    shape = partial.shape
    return sum_call(
        body, cid, partial, (rows_in, gain.reshape(1, -1), upstream),
        ((shape, jnp.float32), (shape, jnp.bfloat16), ((8, shape[1]), jnp.float32)), tasks, task_operands,
    )


def context_places():
    along = lax.axis_index(CONTEXT)
    deep, core = along // 2, along % 2
    return deep, core, {CONTEXT: (1 - deep) * 2 + core}, {CONTEXT: deep * 2 + 1 - core}


def context_call(kernel, cid, operands, outs, scratch, ready=20_000_000_000, place=pltpu.VMEM):
    vmem = pl.BlockSpec(memory_space=pltpu.VMEM)
    return pl.pallas_call(
        kernel,
        out_shape=tuple(jax.ShapeDtypeStruct(shape, kind) for shape, kind in outs),
        in_specs=[pl.BlockSpec(memory_space=place)] * len(operands),
        out_specs=(vmem,) * len(outs),
        scratch_shapes=scratch,
        compiler_params=pltpu.CompilerParams(collective_id=cid, has_side_effects=True, vmem_limit_bytes=12 << 20),
        cost_estimate=pl.CostEstimate(flops=ready, bytes_accessed=30_000_000, transcendentals=0),
        name=f"call_{cid}",
    )(*operands)


def gather_context(cid, first, second):
    rows, width = first.shape

    def kernel(first_ref, second_ref, first_out, second_out, send, recv, own_sem):
        deep, core, to_y, to_core = context_places()
        greet([to_y, to_core])

        def block(ref, which):
            return ref.at[pl.ds(pl.multiple_of(which * rows, rows), rows)]

        def copy(index, source, target, device):
            return pltpu.make_async_remote_copy(
                src_ref=source, dst_ref=target, send_sem=send.at[index], recv_sem=recv.at[index],
                device_id=device, device_id_type=MESH_ID,
            )

        own, beyond = deep * 2 + core, (1 - deep) * 2 + core
        pairs = ((first_ref, first_out), (second_ref, second_out))
        out_y = [copy(i, source, block(full, own), to_y) for i, (source, full) in enumerate(pairs)]
        out_core = [copy(2 + i, source, block(full, own), to_core) for i, (source, full) in enumerate(pairs)]
        passed = [copy(4 + i, block(full, beyond), block(full, beyond), to_core) for i, (source, full) in enumerate(pairs)]
        mine = [pltpu.make_async_copy(source, block(full, own), own_sem.at[i]) for i, (source, full) in enumerate(pairs)]
        for move in out_y + out_core + mine:
            move.start()
        for arrived, onward in zip(out_y, passed):
            arrived.wait_recv()
            onward.start()
        for move in out_core + passed:
            move.wait_recv()
        for move in mine:
            move.wait()
        for move in out_y + out_core + passed:
            move.wait_send()

    full = ((4 * rows, width), first.dtype)
    return context_call(
        kernel, cid, (first, second), (full, full),
        [pltpu.SemaphoreType.DMA((6,)), pltpu.SemaphoreType.DMA((6,)), pltpu.SemaphoreType.DMA((2,))],
    )


def scatter_context(cid, first, second):
    rows, width = first.shape
    part = width // 4

    def kernel(first_ref, second_ref, first_out, second_out, from_core, pair, from_y, local, send, recv, local_sem):
        deep, core, to_y, to_core = context_places()
        greet([to_y, to_core])

        def block(ref, which):
            return ref.at[:, pl.ds(pl.multiple_of(which * part, 128), part)]

        def copy(index, source, target, device):
            return pltpu.make_async_remote_copy(
                src_ref=source, dst_ref=target, send_sem=send.at[index], recv_sem=recv.at[index],
                device_id=device, device_id_type=MESH_ID,
            )

        wide = lambda ref: ref[...].astype(jnp.float32)
        sources, targets = (first_ref, second_ref), (first_out, second_out)
        far, close = 1 - deep, deep
        inner, outer = [], []
        for i, source in enumerate(sources):
            for j, at in enumerate((far, close)):
                inner.append(copy(2 * i + j, block(source, at * 2 + 1 - core), from_core.at[2 * i + j], to_core))
            outer.append(copy(4 + i, pair.at[2 * i], from_y.at[i], to_y))
        mine = [
            pltpu.make_async_copy(block(source, at * 2 + core), local.at[2 * i + j], local_sem.at[2 * i + j])
            for i, source in enumerate(sources)
            for j, at in enumerate((far, close))
        ]
        for at in (0, 2, 1, 3):
            inner[at].start()
            mine[at].start()
        for i, source in enumerate(sources):
            inner[2 * i].wait_recv()
            mine[2 * i].wait()
            pair[2 * i] = (wide(local.at[2 * i]) + wide(from_core.at[2 * i])).astype(jnp.bfloat16)
            outer[i].start()
        for i, source in enumerate(sources):
            inner[2 * i + 1].wait_recv()
            mine[2 * i + 1].wait()
            pair[2 * i + 1] = (wide(local.at[2 * i + 1]) + wide(from_core.at[2 * i + 1])).astype(jnp.bfloat16)
        for i, target in enumerate(targets):
            outer[i].wait_recv()
            target[...] = (wide(pair.at[2 * i + 1]) + wide(from_y.at[i])).astype(target.dtype)
        for move in inner + outer:
            move.wait_send()

    out = ((rows, part), jnp.bfloat16)
    piece = (rows, part)
    return context_call(
        kernel, cid, (first, second), (out, out),
        [
            pltpu.VMEM((4,) + piece, jnp.bfloat16),
            pltpu.VMEM((4,) + piece, jnp.bfloat16),
            pltpu.VMEM((2,) + piece, jnp.bfloat16),
            pltpu.VMEM((4,) + piece, jnp.bfloat16),
            pltpu.SemaphoreType.DMA((6,)),
            pltpu.SemaphoreType.DMA((6,)),
            pltpu.SemaphoreType.DMA((4,)),
        ],
        place=pltpu.HBM,
    )


def line_total(cid, value):
    count = lax.axis_size(TENSOR)

    def kernel(value_ref, out_ref, slots, send, recv):
        at = lax.axis_index(TENSOR)
        others = [{TENSOR: (at + step) % count} for step in range(1, count)]
        greet(others)
        moves = [
            pltpu.make_async_remote_copy(
                src_ref=value_ref, dst_ref=slots.at[step], send_sem=send.at[step], recv_sem=recv.at[step],
                device_id=device, device_id_type=MESH_ID,
            )
            for step, device in enumerate(others)
        ]
        for move in moves:
            move.start()
        for move in moves:
            move.wait_recv()
        total = value_ref[...]
        for step in range(count - 1):
            total = total + slots[step]
        out_ref[...] = total
        for move in moves:
            move.wait_send()

    (total,) = context_call(
        kernel, cid, (value,), ((value.shape, jnp.float32),),
        [
            pltpu.VMEM((count - 1,) + value.shape, jnp.float32),
            pltpu.SemaphoreType.DMA((count - 1,)),
            pltpu.SemaphoreType.DMA((count - 1,)),
        ],
        5_000_000_000,
    )
    return total


def feed(normed, weight_in, weight_out):
    hidden = dot_rows(normed, weight_in)
    active = jax.nn.silu(hidden).astype(jnp.bfloat16)
    return dot_rows(active, weight_out).astype(jnp.bfloat16), (normed, hidden, active)


def feed_back(weight_in, weight_out, saved, branch_grad):
    normed, hidden, active = saved
    grad_out = dot_inner(active, branch_grad)
    unused, pullback = jax.vjp(jax.nn.silu, hidden)
    hidden_grad = pullback(dot_outer(branch_grad, weight_out))[0].astype(jnp.bfloat16)
    grad_in = dot_inner(normed, hidden_grad)
    return dot_outer(hidden_grad, weight_in).astype(jnp.bfloat16), grad_in, grad_out


QB = 128
BAND = 3 * QB
SPAN = 4 * QB
NT = (((1,), (1,)), ((), ()))


def span_table(relative):
    table = relative.astype(jnp.bfloat16)
    low = jnp.broadcast_to(table[:1], (2 * QB - 1 - LEFT, table.shape[1]))
    high = jnp.broadcast_to(table[-1:], (SPAN - (2 * QB - 1 - LEFT) - table.shape[0], table.shape[1]))
    spread = jnp.concatenate([low, table, high], axis=0)
    return jnp.concatenate([spread, spread], axis=1)


def fill_scores(first_block, q_mask, k_ref, span_ref, s_ref, edge_ref):
    keys = k_ref.shape[0]
    s_ref[:, QB : QB + keys] = lax.dot_general(q_mask, k_ref[...], NT, preferred_element_type=jnp.float32)
    spread = lax.dot_general(q_mask, span_ref[...], NT, preferred_element_type=jnp.float32)
    edge_ref[0] = jnp.broadcast_to(spread[:, :1], (QB, QB))
    edge_ref[1] = jnp.zeros((QB, QB), jnp.float32)
    edge_ref[2] = jnp.broadcast_to(spread[:, SPAN - 1 :], (QB, QB))
    skewed = pltpu.roll(spread, SPAN - (QB - 1), 1, stride=1, stride_axis=0)
    at = pl.ds(pl.multiple_of(first_block * QB, QB), BAND)
    s_ref[:, at] = s_ref[:, at] + skewed[:, :BAND]


def edge_of(block, first_block):
    return jnp.where(block < first_block - 1, 0, jnp.where(block > first_block + 1, 2, 1))


def forward_kernel(pos_ref, q_ref, k_ref, v_ref, span_ref, o_ref, lse_ref, s_ref, edge_ref, p_ref):
    keys = k_ref.shape[0]
    blocks = keys // QB
    first_block = pos_ref[0] * pl.num_programs(1) + pl.program_id(1)
    lane = lax.broadcasted_iota(jnp.int32, (QB, 2 * HEAD_DIM), 1)
    outs, lses = [], []
    for half in range(2):
        mine = (lane < HEAD_DIM) if half == 0 else (lane >= HEAD_DIM)
        q_mask = jnp.where(mine, q_ref[...], jnp.zeros_like(q_ref))
        fill_scores(first_block, q_mask, k_ref, span_ref, s_ref, edge_ref)
        top = None
        for block in range(blocks):
            z = s_ref[:, (block + 1) * QB : (block + 2) * QB] + edge_ref[edge_of(block, first_block)]
            top = z if top is None else jnp.maximum(top, z)
        top = jnp.max(top, axis=1, keepdims=True)
        edge_ref[...] = edge_ref[...] - top[None]
        total = None
        for block in range(blocks):
            z = s_ref[:, (block + 1) * QB : (block + 2) * QB] + edge_ref[edge_of(block, first_block)]
            p = jnp.exp(z)
            total = p if total is None else total + p
            p_ref[:, block * QB : (block + 1) * QB] = p.astype(jnp.bfloat16)
        total = jnp.sum(total, axis=1, keepdims=True)
        out = jnp.dot(p_ref[...], v_ref[...], preferred_element_type=jnp.float32) / total
        outs.append(out)
        lses.append(jnp.broadcast_to(top + jnp.log(total), (QB, 2 * HEAD_DIM)))
    low = lane < HEAD_DIM
    o_ref[...] = jnp.where(low, outs[0], outs[1]).astype(o_ref.dtype)
    lse_ref[...] = jnp.where(low, lses[0], lses[1])


def attention_forward(position, q, k, v, span):
    rows, width = q.shape
    keys = k.shape[0]
    pairs = width // (2 * HEAD_DIM)
    two = 2 * HEAD_DIM
    row_spec = pl.BlockSpec((QB, two), lambda p, b, pos: (b, p))
    key_spec = pl.BlockSpec((keys, two), lambda p, b, pos: (0, p))
    return pl.pallas_call(
        forward_kernel,
        out_shape=(
            jax.ShapeDtypeStruct((rows, width), jnp.bfloat16),
            jax.ShapeDtypeStruct((rows, width), jnp.float32),
        ),
        grid_spec=pltpu.PrefetchScalarGridSpec(
            num_scalar_prefetch=1,
            grid=(pairs, rows // QB),
            in_specs=[row_spec, key_spec, key_spec, pl.BlockSpec((SPAN, two), lambda p, b, pos: (0, 0))],
            out_specs=(row_spec, row_spec),
            scratch_shapes=[
                pltpu.VMEM((QB, keys + 2 * QB), jnp.float32),
                pltpu.VMEM((3, QB, QB), jnp.float32),
                pltpu.VMEM((QB, keys), jnp.bfloat16),
            ],
        ),
        compiler_params=pltpu.CompilerParams(vmem_limit_bytes=20 << 20),
        cost_estimate=pl.CostEstimate(flops=8 * rows * keys * width, bytes_accessed=4 * (keys + rows) * width, transcendentals=0),
        name="attention_forward",
    )(position.reshape(1), q, k, v, span)


def backward_kernel(pos_ref, q_ref, qt_ref, g_ref, gt_ref, o_ref, lse_ref, k_ref, v_ref, span_ref,
                    dq_ref, dkt_ref, dvt_ref, bins_ref, ends_ref,
                    s_ref, edge_ref, d_ref, p_ref, z_ref, wide_ref, dk_acc, dv_acc):
    keys = k_ref.shape[0]
    blocks = keys // QB
    step = pl.program_id(1)
    first_block = pos_ref[0] * pl.num_programs(1) + step
    lane = lax.broadcasted_iota(jnp.int32, (QB, 2 * HEAD_DIM), 1)

    @pl.when((pl.program_id(0) == 0) & (step == 0))
    def _():
        bins_ref[...] = jnp.zeros_like(bins_ref)
        ends_ref[...] = jnp.zeros_like(ends_ref)

    @pl.when(step == 0)
    def _():
        dk_acc[...] = jnp.zeros_like(dk_acc)
        dv_acc[...] = jnp.zeros_like(dv_acc)
        wide_ref[:, : 2 * HEAD_DIM] = k_ref[...]

    @pl.when((pl.program_id(0) == 0) & (step == 0))
    def _():
        z_ref[:, :QB] = jnp.zeros((QB, QB), jnp.bfloat16)
        z_ref[:, QB + keys :] = jnp.zeros((QB, QB), jnp.bfloat16)

    row_at = lax.broadcasted_iota(jnp.int32, (keys, QB), 0)
    col_at = lax.broadcasted_iota(jnp.int32, (keys, QB), 1)
    below = (row_at < (first_block - 1) * QB) & (col_at == 0)
    above = (row_at >= (first_block + 2) * QB) & (col_at == 1)
    wide_ref[:, 2 * HEAD_DIM :] = jnp.where(below | above, 1.0, 0.0).astype(jnp.bfloat16)

    flip_at = lax.broadcasted_iota(jnp.int32, (QB, QB), 0) + lax.broadcasted_iota(jnp.int32, (QB, QB), 1)
    flip = jnp.where(flip_at == QB - 1, 1.0, 0.0).astype(jnp.bfloat16)
    dqs = []
    for half in range(2):
        rows = slice(half * HEAD_DIM, (half + 1) * HEAD_DIM)
        mine = (lane < HEAD_DIM) if half == 0 else (lane >= HEAD_DIM)
        q_mask = jnp.where(mine, q_ref[...], jnp.zeros_like(q_ref))
        g_mask = jnp.where(mine, g_ref[...], jnp.zeros_like(g_ref))
        fill_scores(first_block, q_mask, k_ref, span_ref, s_ref, edge_ref)
        d_ref[...] = lax.dot_general(g_mask, v_ref[...], NT, preferred_element_type=jnp.float32)
        delta = jnp.sum(g_mask.astype(jnp.float32) * o_ref[...].astype(jnp.float32), axis=1, keepdims=True)
        lse = lse_ref[:, half * HEAD_DIM : half * HEAD_DIM + 1]
        edge_ref[...] = edge_ref[...] - lse[None]
        delta = jnp.broadcast_to(delta, (QB, QB))
        for block in range(blocks):
            here = slice(block * QB, (block + 1) * QB)
            there = slice((block + 1) * QB, (block + 2) * QB)
            p = jnp.exp(s_ref[:, there] + edge_ref[edge_of(block, first_block)])
            p_ref[:, here] = p.astype(jnp.bfloat16)
            z_ref[:, there] = (p * (d_ref[:, here] - delta)).astype(jnp.bfloat16)
        z_all = z_ref[:, QB : QB + keys]
        dv_acc[rows] += jnp.dot(gt_ref[rows], p_ref[...], preferred_element_type=jnp.float32)
        dk_acc[rows] += jnp.dot(qt_ref[rows], z_all, preferred_element_type=jnp.float32)
        dq = jnp.dot(z_all, wide_ref[...], preferred_element_type=jnp.float32)
        at = pl.ds(pl.multiple_of(first_block * QB, QB), BAND)
        band = jnp.dot(flip, z_ref[:, at], preferred_element_type=jnp.float32)
        band = jnp.concatenate([band, jnp.zeros((QB, SPAN - BAND), jnp.float32)], axis=1)
        spread = pltpu.roll(band, 0, 1, stride=1, stride_axis=0).astype(jnp.bfloat16)
        spread = jnp.dot(flip, spread, preferred_element_type=jnp.float32).astype(jnp.bfloat16)
        dq_rel = jnp.dot(spread, span_ref[...], preferred_element_type=jnp.float32)
        below_sum = dq[:, 2 * HEAD_DIM : 2 * HEAD_DIM + 1]
        above_sum = dq[:, 2 * HEAD_DIM + 1 : 2 * HEAD_DIM + 2]
        span_low = span_ref[:1, :].astype(jnp.float32)
        span_high = span_ref[SPAN - 1 :, :].astype(jnp.float32)
        dqs.append(dq[:, : 2 * HEAD_DIM] + dq_rel + below_sum * span_low + above_sum * span_high)
        bins_ref[...] += jnp.dot(qt_ref[rows], spread, preferred_element_type=jnp.float32)
        q_wide = q_mask.astype(jnp.float32)
        ends_ref[0:1, :] += jnp.sum(q_wide * below_sum, axis=0, keepdims=True)
        ends_ref[1:2, :] += jnp.sum(q_wide * above_sum, axis=0, keepdims=True)
    scale = 1.0 / 8.0
    dq_ref[...] = (jnp.where(lane < HEAD_DIM, dqs[0], dqs[1]) * scale).astype(dq_ref.dtype)

    @pl.when(step == pl.num_programs(1) - 1)
    def _():
        dkt_ref[...] = dk_acc[...].astype(dkt_ref.dtype)
        dvt_ref[...] = dv_acc[...].astype(dvt_ref.dtype)


def attention_backward(position, q, q_t, g, g_t, o, lse, k, v, span):
    rows, width = q.shape
    keys = k.shape[0]
    pairs = width // (2 * HEAD_DIM)
    two = 2 * HEAD_DIM
    row_spec = pl.BlockSpec((QB, two), lambda p, b, pos: (b, p))
    col_spec = pl.BlockSpec((two, QB), lambda p, b, pos: (p, b))
    key_spec = pl.BlockSpec((keys, two), lambda p, b, pos: (0, p))
    keyt_spec = pl.BlockSpec((two, keys), lambda p, b, pos: (p, 0))
    fixed = lambda shape: pl.BlockSpec(shape, lambda p, b, pos: (0, 0))
    dq, dkt, dvt, bins, ends = pl.pallas_call(
        backward_kernel,
        out_shape=(
            jax.ShapeDtypeStruct((rows, width), jnp.bfloat16),
            jax.ShapeDtypeStruct((width, keys), jnp.bfloat16),
            jax.ShapeDtypeStruct((width, keys), jnp.bfloat16),
            jax.ShapeDtypeStruct((HEAD_DIM, SPAN), jnp.float32),
            jax.ShapeDtypeStruct((8, two), jnp.float32),
        ),
        grid_spec=pltpu.PrefetchScalarGridSpec(
            num_scalar_prefetch=1,
            grid=(pairs, rows // QB),
            in_specs=[row_spec, col_spec, row_spec, col_spec, row_spec, row_spec, key_spec, key_spec, fixed((SPAN, two))],
            out_specs=(row_spec, keyt_spec, keyt_spec, fixed((HEAD_DIM, SPAN)), fixed((8, two))),
            scratch_shapes=[
                pltpu.VMEM((QB, keys + 2 * QB), jnp.float32),
                pltpu.VMEM((3, QB, QB), jnp.float32),
                pltpu.VMEM((QB, keys), jnp.float32),
                pltpu.VMEM((QB, keys), jnp.bfloat16),
                pltpu.VMEM((QB, keys + 2 * QB), jnp.bfloat16),
                pltpu.VMEM((keys, 2 * two), jnp.bfloat16),
                pltpu.VMEM((two, keys), jnp.float32),
                pltpu.VMEM((two, keys), jnp.float32),
            ],
        ),
        compiler_params=pltpu.CompilerParams(vmem_limit_bytes=20 << 20),
        cost_estimate=pl.CostEstimate(flops=20 * rows * keys * width, bytes_accessed=8 * (keys + rows) * width, transcendentals=0),
        name="attention_backward",
    )(position.reshape(1), q, q_t, g, g_t, o, lse, k, v, span)
    at = 2 * QB - 1 - LEFT
    ends = ends[:2, :HEAD_DIM] + ends[:2, HEAD_DIM:]
    spread = bins.T
    inner = spread[at + 1 : at + LEFT + RIGHT]
    low = jnp.sum(spread[: at + 1], axis=0) + ends[0]
    high = jnp.sum(spread[at + LEFT + RIGHT :], axis=0) + ends[1]
    table = jnp.concatenate([low[None], inner, high[None]], axis=0)
    return dq, dkt, dvt, table


def attend_forward(normed, weight_in, weight_out, relative, position):
    projected = jnp.einsum(
        "td,kde->kte", normed, weight_in, preferred_element_type=jnp.float32
    ).astype(jnp.bfloat16)
    key_rows, value_rows = gather_context(10, projected[1], projected[2])
    queries = projected[0] * jnp.bfloat16(1.0 / math.sqrt(HEAD_DIM))
    span = span_table(relative)
    mixed, log_total = attention_forward(position, queries, key_rows, value_rows, span)
    return (
        dot_rows(mixed, weight_out).astype(jnp.bfloat16),
        (normed, queries, key_rows, value_rows, log_total, mixed, span),
    )


def attend_backward(weight_in, weight_out, position, saved, branch_grad):
    normed, queries, key_rows, value_rows, log_total, mixed, span = saved
    grad_out = dot_inner(mixed, branch_grad)
    mixed_grad = dot_outer(branch_grad, weight_out).astype(jnp.bfloat16)
    query_grad, key_grad, value_grad, table_grad = attention_backward(
        position, queries, queries.T, mixed_grad, mixed_grad.T, mixed, log_total, key_rows, value_rows, span
    )
    key_grad, value_grad = scatter_context(11, key_grad, value_grad)
    stacked = jnp.stack([query_grad, key_grad.T, value_grad.T])
    grad_in = jnp.einsum("td,kte->kde", normed, stacked, preferred_element_type=jnp.float32)
    partial_sum = jnp.einsum("kte,kde->td", stacked, weight_in, preferred_element_type=jnp.float32)
    return (partial_sum.astype(jnp.bfloat16), table_grad, grad_in, grad_out)


TILE = 64


def sliding(ext_ref, tile, lanes):
    window = ext_ref[pl.ds(pl.multiple_of(tile * TILE, TILE), TILE + 32), lanes]
    for low in range(8):
        moved = window[low : low + TILE + 24]
        for high in range(0, 31 - low, 8):
            yield high + low, moved[high : high + TILE]


def tile_loop(rows, width, body):
    def step(tile, carry):
        for at in range(0, width, 128):
            body(tile, slice(at, at + 128))
        return carry

    lax.fori_loop(0, rows // TILE, step, 0)


def extended(before, rows, after):
    pad = -(before.shape[0] + after.shape[0]) % 32
    return jnp.concatenate([before, rows, after, jnp.zeros((pad, rows.shape[1]), rows.dtype)], axis=0)


def depth_forward(ext, depthwise):
    rows, width = ext.shape[0] - 32, ext.shape[1]

    def kernel(ext_ref, depth_ref, out_ref):
        def body(tile, lanes):
            total = None
            for distance, part in sliding(ext_ref, tile, lanes):
                term = depth_ref[distance : distance + 1, lanes] * part
                total = term if total is None else total + term
            out_ref[pl.ds(pl.multiple_of(tile * TILE, TILE), TILE), lanes] = total

        tile_loop(rows, width, body)

    vmem = pl.BlockSpec(memory_space=pltpu.VMEM)
    return pl.pallas_call(
        kernel,
        out_shape=jax.ShapeDtypeStruct((rows, width), jnp.float32),
        in_specs=[vmem] * 2,
        out_specs=vmem,
        compiler_params=pltpu.CompilerParams(vmem_limit_bytes=6 << 20),
        cost_estimate=pl.CostEstimate(flops=1_000_000_000, bytes_accessed=2_000_000, transcendentals=0),
    )(ext, depthwise)


def depth_backward(grad_ext, ext, depthwise):
    rows, width = ext.shape[0] - 32, ext.shape[1]
    reach = depthwise.shape[0] - 1

    def kernel(grad_ref, ext_ref, depth_ref, out_ref, depth_out, sums):
        sums[...] = jnp.zeros_like(sums)

        def body(tile, lanes):
            here = pl.ds(pl.multiple_of(tile * TILE, TILE), TILE)
            total = None
            for distance, part in sliding(grad_ref, tile, lanes):
                term = depth_ref[reach - distance : reach - distance + 1, lanes] * part
                total = term if total is None else total + term
            out_ref[here, lanes] = total
            grad = grad_ref[here, lanes]
            for distance, part in sliding(ext_ref, tile, lanes):
                sums[distance, :, lanes] += gather_eight(grad * part)

        tile_loop(rows, width, body)
        for distance in range(reach + 1):
            depth_out[distance : distance + 1] = jnp.sum(sums[distance], axis=0, keepdims=True)

    vmem = pl.BlockSpec(memory_space=pltpu.VMEM)
    return pl.pallas_call(
        kernel,
        out_shape=(
            jax.ShapeDtypeStruct((rows, width), jnp.float32),
            jax.ShapeDtypeStruct(depthwise.shape, jnp.float32),
        ),
        in_specs=[vmem] * 3,
        out_specs=(vmem, vmem),
        scratch_shapes=[pltpu.VMEM((reach + 1, 8, width), jnp.float32)],
        compiler_params=pltpu.CompilerParams(vmem_limit_bytes=8 << 20),
        cost_estimate=pl.CostEstimate(flops=2_000_000_000, bytes_accessed=4_000_000, transcendentals=0),
    )(grad_ext, ext, depthwise)


def channel_sums(cid, first, second):
    total = line_total(cid, jnp.concatenate([first, second]).reshape(-1, 128)).reshape(2, -1)
    return total[0], total[1]


def conv_forward(normed, weight_in, weight_out, depthwise, gain_middle):
    projected = jnp.einsum("td,kde->kte", normed, weight_in, preferred_element_type=jnp.float32)
    gated = gate_unit(projected[0], projected[1])
    rows_here = gated.shape[0]
    reach_rows = depthwise.shape[0] - 1
    edge_rows = shifted_2(gated[rows_here - reach_rows :], CONTEXT, 1)
    padded = extended(edge_rows, gated, gated[:0])
    mixed = depth_forward(padded, depthwise)
    row_sums, row_squares = channel_sums(12, jnp.sum(mixed, axis=1), jnp.sum(mixed * mixed, axis=1))
    row_mean = row_sums / D
    inverse = lax.rsqrt(row_squares / D - row_mean * row_mean + epsilon)
    scaled = (mixed - row_mean[:, None]) * inverse[:, None]
    shaped = scaled * gain_middle
    active = jax.nn.silu(shaped).astype(jnp.bfloat16)
    return (
        dot_rows(active, weight_out).astype(jnp.bfloat16),
        (normed, projected, padded, scaled, inverse, shaped, active),
    )


def conv_backward(weight_in, weight_out, depthwise, gain_middle, saved, branch_grad):
    normed, projected, padded, scaled, inverse, shaped, active = saved
    reach_rows = depthwise.shape[0] - 1
    grad_out = dot_inner(active, branch_grad)
    unused, pullback = jax.vjp(jax.nn.silu, shaped)
    shaped_grad = pullback(dot_outer(branch_grad, weight_out))[0]
    middle_grad = jnp.sum(shaped_grad * scaled, axis=0)
    scaled_grad = shaped_grad * gain_middle
    first_sum, second_sum = channel_sums(13, jnp.sum(scaled_grad, axis=1), jnp.sum(scaled_grad * scaled, axis=1))
    mixed_grad = inverse[:, None] * (
        scaled_grad - first_sum[:, None] / D - scaled * (second_sum[:, None] / D)
    )
    next_rows = shifted_2(mixed_grad[:reach_rows], CONTEXT, -1)
    gated_grad, depth_grad = depth_backward(extended(mixed_grad[:0], mixed_grad, next_rows), padded, depthwise)
    unused, pullback = jax.vjp(gate_unit, projected[0], projected[1])
    unit_grad, gate_grad = pullback(gated_grad)
    stacked = jnp.stack([unit_grad, gate_grad]).astype(jnp.bfloat16)
    grad_in = jnp.einsum("td,kte->kde", normed, stacked, preferred_element_type=jnp.float32)
    partial_sum = jnp.einsum("kte,kde->td", stacked, weight_in, preferred_element_type=jnp.float32)
    return (partial_sum.astype(jnp.bfloat16), grad_in, grad_out, middle_grad, depth_grad)


def local(
    inputs,
    gain_first,
    first_in,
    first_out,
    gain_attend,
    attend_in,
    attend_out,
    relative,
    gain_convolve,
    convolve_in,
    depthwise,
    gain_middle,
    convolve_out,
    gain_second,
    second_in,
    second_out,
    gain_final,
    cotangent,
):
    position = lax.axis_index(CONTEXT)
    start_rows = inputs[0]
    small_plane = lax.axis_size(CLIPS) == 2
    weights = {
        FIRST: (first_in, first_out),
        ATTEND: (attend_in, attend_out),
        CONVOLVE: (convolve_in, convolve_out),
        SECOND: (second_in, second_out),
    }
    held, grads = {}, {}

    def collecting(name):
        if not small_plane:
            return (), ()
        pair = tuple(weight.astype(jnp.bfloat16) for weight in weights[name])
        return tuple(Gather(wide, weight.shape) for wide, weight in zip((False, True), pair)), pair

    def collect(name, gathered):
        held[name] = gathered if small_plane else fetch(*weights[name])

    def spreading(*sums):
        if not small_plane:
            return (), ()
        sums = tuple(grad.astype(jnp.bfloat16) for grad in sums)
        return tuple(Scatter(at % 2 == 1, grad.shape) for at, grad in enumerate(sums)), sums

    def with_small(rest, kind, value):
        if not small_plane:
            return rest
        return rest[0] + (kind(value.shape),), rest[1] + (value,)

    def spread(name, scattered, grad_in, grad_out):
        grads[name] = scattered if small_plane else send_grads(grad_in, grad_out)

    tasks, pair = collecting(FIRST)
    collect(FIRST, plane_call(9, tasks, pair) if small_plane else None)
    normed = layer_norm(start_rows.astype(jnp.float32), gain_first).astype(jnp.bfloat16)
    branch, first_saved = feed(normed, *held[FIRST])
    (after_first, normed), got = forward_sum(1, branch, start_rows, gain_attend, 0.5, *collecting(ATTEND))
    collect(ATTEND, got)
    branch, attend_saved = attend_forward(normed, *held[ATTEND], relative, position)
    (after_attend, normed), got = forward_sum(2, branch, after_first, gain_convolve, 1.0, *collecting(CONVOLVE))
    collect(CONVOLVE, got)
    branch, convolve_saved = conv_forward(normed, *held[CONVOLVE], depthwise, gain_middle)
    (after_convolve, normed), got = forward_sum(3, branch, after_attend, gain_second, 1.0, *collecting(SECOND))
    collect(SECOND, got)
    branch, second_saved = feed(normed, *held[SECOND])
    final_out, upstream, branch_grad, grad_final = turn_sum(4, branch, after_convolve, gain_final, cotangent[0])
    branch, *second_pair = feed_back(*held[SECOND], second_saved, branch_grad)
    (upstream, branch_grad, grad_gain_second), _ = backward_sum(
        5, branch, after_convolve, gain_second, upstream, 1.0
    )
    branch, *convolve_pair, grad_middle, grad_depth = conv_backward(
        *held[CONVOLVE], depthwise, gain_middle, convolve_saved, branch_grad
    )
    (upstream, branch_grad, grad_gain_convolve), got = backward_sum(
        6, branch, after_attend, gain_convolve, upstream, 1.0, *spreading(*second_pair)
    )
    spread(SECOND, got, *second_pair)
    branch, table_grad, *pair = attend_backward(*held[ATTEND], position, attend_saved, branch_grad)
    shared = jnp.pad(table_grad.reshape(-1), (0, -table_grad.size % 1024)).reshape(-1, 128)
    (upstream, branch_grad, grad_gain_attend), got = backward_sum(
        7, branch, after_first, gain_attend, upstream, 0.5, *with_small(spreading(*convolve_pair, *pair), LineSum, shared)
    )
    spread(CONVOLVE, got[:2], *convolve_pair)
    spread(ATTEND, got[2:4], *pair)
    branch, *pair = feed_back(*held[FIRST], first_saved, branch_grad)
    gains = [
        jnp.sum(part, axis=0) for part in (grad_gain_attend, grad_gain_convolve, grad_gain_second, grad_final)
    ]
    smalls = [*gains, grad_middle, grad_depth.reshape(-1)]
    sizes = [part.shape[0] for part in smalls]
    packed = jnp.concatenate(smalls).reshape(-1, 128)
    if small_plane:
        packed = jnp.concatenate([packed, got[4]], axis=0)
    (upstream, branch_grad, grad_gain_first), got = backward_sum(
        8, branch, start_rows, gain_first, upstream, 1.0, *with_small(spreading(*pair), PlaneSum, packed)
    )
    spread(FIRST, got[:2], *pair)
    grad_gain_first = jnp.sum(grad_gain_first, axis=0)
    if small_plane:
        packed = got[2].reshape(-1)
        (grad_gain_first,) = plane_call(14, (PlaneSum((8, 128)),), (grad_gain_first.reshape(8, 128),))
        grad_gain_first = grad_gain_first.reshape(-1)
        table_grad = packed[sum(sizes) : sum(sizes) + table_grad.size].reshape(table_grad.shape)
    else:
        table_grad = lax.psum(table_grad, (CLIPS, CONTEXT, TENSOR))
        packed, grad_gain_first = lax.psum((packed.reshape(-1), grad_gain_first), (CLIPS, CONTEXT))
    smalls, at = [], 0
    for size in sizes:
        smalls.append(packed[at : at + size])
        at += size
    grad_depth = smalls[5].reshape(depthwise.shape)
    return (
        final_out[None],
        upstream[None],
        grad_gain_first,
        grads[FIRST][0],
        grads[FIRST][1],
        smalls[0],
        grads[ATTEND][0],
        grads[ATTEND][1],
        table_grad,
        smalls[1],
        grads[CONVOLVE][0],
        grad_depth,
        smalls[4],
        grads[CONVOLVE][1],
        smalls[2],
        grads[SECOND][0],
        grads[SECOND][1],
        smalls[3],
    )


def solution(mesh):
    placed = (
        P(CLIPS, CONTEXT, None),
        P(),
        P((CLIPS, CONTEXT), TENSOR),
        P(TENSOR, (CLIPS, CONTEXT)),
        P(),
        P(None, (CLIPS, CONTEXT), TENSOR),
        P(TENSOR, (CLIPS, CONTEXT)),
        P(),
        P(),
        P(None, (CLIPS, CONTEXT), TENSOR),
        P(None, TENSOR),
        P(TENSOR),
        P(TENSOR, (CLIPS, CONTEXT)),
        P(),
        P((CLIPS, CONTEXT), TENSOR),
        P(TENSOR, (CLIPS, CONTEXT)),
        P(),
        P(CLIPS, CONTEXT, None),
    )
    return jax.shard_map(
        local,
        mesh=mesh,
        in_specs=placed,
        out_specs=(
            P(CLIPS, CONTEXT, None),
            P(CLIPS, CONTEXT, None),
            P(),
            P((CLIPS, CONTEXT), TENSOR),
            P(TENSOR, (CLIPS, CONTEXT)),
            P(),
            P(None, (CLIPS, CONTEXT), TENSOR),
            P(TENSOR, (CLIPS, CONTEXT)),
            P(),
            P(),
            P(None, (CLIPS, CONTEXT), TENSOR),
            P(None, TENSOR),
            P(TENSOR),
            P(TENSOR, (CLIPS, CONTEXT)),
            P(),
            P((CLIPS, CONTEXT), TENSOR),
            P(TENSOR, (CLIPS, CONTEXT)),
            P(),
        ),
        check_vma=False,
    )
```

```python
import math

import jax
import jax.numpy as jnp
from jax import lax
from jax.experimental import pallas as pl
from jax.experimental.pallas import tpu as pltpu
from jax.sharding import PartitionSpec as P

CLIPS, CONTEXT, TENSOR = "clips", "context", "tensor"
D = 1024
HEAD_DIM = 64
LEFT = 64
RIGHT = 8

epsilon = 1e-05


def shifted_2(value, axis, steps):
    count = lax.axis_size(axis)
    initial, last = (max(0, -steps), min(count, count - steps))
    return lax.ppermute(value, axis, [(source, source + steps) for source in range(initial, last)])


def dot_rows(former, latter):
    return jnp.dot(former, latter, preferred_element_type=jnp.float32)


def dot_inner(former, latter):
    return lax.dot_general(
        former, latter, (((0,), (0,)), ((), ())), preferred_element_type=jnp.float32
    )


def dot_outer(former, latter):
    return lax.dot_general(
        former, latter, (((1,), (1,)), ((), ())), preferred_element_type=jnp.float32
    )


def layer_norm(rows_in, gain_vec):
    row_mean = jnp.mean(rows_in, axis=-1, keepdims=True)
    centred = rows_in - row_mean
    variance = jnp.mean(centred * centred, axis=-1, keepdims=True)
    return centred * lax.rsqrt(variance + epsilon) * gain_vec


def gate_unit(unit_half, gate_half):
    return unit_half * jax.nn.sigmoid(gate_half)


def fetch(weight_in, weight_out):
    return (
        lax.all_gather(weight_in.astype(jnp.bfloat16), (CLIPS, CONTEXT), axis=weight_in.ndim - 2, tiled=True),
        lax.all_gather(weight_out.astype(jnp.bfloat16), (CLIPS, CONTEXT), axis=1, tiled=True),
    )


def scatter_sum(grad, axis):
    summed = lax.psum_scatter(
        grad.astype(jnp.bfloat16), (CLIPS, CONTEXT), scatter_dimension=axis, tiled=True
    )
    return summed.astype(jnp.float32)


def send_grads(grad_in, grad_out):
    return (scatter_sum(grad_in, grad_in.ndim - 2), scatter_sum(grad_out, 1))


MESH_ID = pl.DeviceIdType.MESH
CHUNKS = 16
LAG = 3
FULL, TOP, BOTTOM = 0, 1, 2
FIRST, ATTEND, CONVOLVE, SECOND = range(4)


def near():
    across_clips = lax.axis_index(CLIPS)
    along = lax.axis_index(CONTEXT)
    deep, core = along // 2, along % 2
    devices = (
        {CLIPS: 1 - across_clips},
        {CONTEXT: (1 - deep) * 2 + core},
        {CONTEXT: deep * 2 + 1 - core},
    )
    return (across_clips, deep, core), devices


def greet(devices):
    barrier = pltpu.get_barrier_semaphore()
    for device in devices:
        pl.semaphore_signal(barrier, inc=1, device_id=device, device_id_type=MESH_ID)
    pl.semaphore_wait(barrier, len(devices))


def part_of(ref, wide, count, shard, part):
    if wide:
        size = ref.shape[-1] // count
        rows = ref.shape[-2]
        along = slice(None) if part == FULL else pl.ds((part - 1) * (rows // 2), rows // 2)
        return ref.at[along, pl.ds(pl.multiple_of(shard * size, 128), size)]
    size = ref.shape[-2] // count
    start, length = shard * size, size
    if part != FULL:
        length = size // 2
        start = start + (part - 1) * length
    window = pl.ds(pl.multiple_of(start, 16), length)
    return ref.at[window] if len(ref.shape) == 2 else ref.at[:, window]


def half_of(ref, part):
    length = ref.shape[-2] // 2
    window = pl.ds((part - 1) * length, length)
    return ref.at[window] if len(ref.shape) == 2 else ref.at[:, window]


class Gather:
    copies = 9
    line = False

    def __init__(self, wide, shard_shape):
        self.wide = wide
        self.shape = shard_shape[:-2] + (
            (shard_shape[-2], shard_shape[-1] * 8) if wide else (shard_shape[-2] * 8, shard_shape[-1])
        )

    def outs(self):
        return [(self.shape, jnp.bfloat16)]

    def scratch(self):
        return [pltpu.SemaphoreType.DMA((self.copies,)), pltpu.SemaphoreType.DMA((self.copies,)), pltpu.SemaphoreType.DMA]

    def bind(self, ins, outs, scratch):
        (shard_ref,), (full_ref,) = ins, outs
        send, recv, own_sem = scratch
        (x, y, core), (to_x, to_y, to_core) = near()
        shard = lambda a, b: a * 4 + b * 2 + core
        own, at_x, at_y, at_far = shard(x, y), shard(1 - x, y), shard(x, 1 - y), shard(1 - x, 1 - y)
        place = lambda which, part: part_of(full_ref, self.wide, 8, which, part)

        def copy(index, source, which, part, device):
            return pltpu.make_async_remote_copy(
                src_ref=source, dst_ref=place(which, part), send_sem=send.at[index], recv_sem=recv.at[index],
                device_id=device, device_id_type=MESH_ID,
            )

        passed = lambda index, which, part, device: copy(index, place(which, part), which, part, device)
        moves = [
            copy(0, shard_ref, own, FULL, to_x),
            copy(1, shard_ref, own, FULL, to_y),
            copy(2, shard_ref, own, FULL, to_core),
            passed(3, at_x, TOP, to_y),
            passed(4, at_x, FULL, to_core),
            passed(5, at_y, BOTTOM, to_x),
            passed(6, at_y, FULL, to_core),
            passed(7, at_far, TOP, to_core),
            passed(8, at_far, BOTTOM, to_core),
        ]
        mine = pltpu.make_async_copy(shard_ref, place(own, FULL), own_sem)

        def begin():
            for index in (0, 1, 2):
                moves[index].start()
            mine.start()

        def second():
            moves[0].wait_recv()
            moves[3].start()
            moves[4].start()
            moves[1].wait_recv()
            moves[5].start()
            moves[6].start()

        def third():
            moves[3].wait_recv()
            moves[7].start()
            moves[5].wait_recv()
            moves[8].start()

        def last():
            for index in (2, 4, 6, 7, 8):
                moves[index].wait_recv()
            mine.wait()
            for move in moves:
                move.wait_send()

        return begin, [second, third], last


class Scatter:
    copies = 8
    line = False

    def __init__(self, wide, full_shape):
        self.wide = wide
        self.shape = full_shape[:-2] + (
            (full_shape[-2], full_shape[-1] // 8) if wide else (full_shape[-2] // 8, full_shape[-1])
        )

    def outs(self):
        return [(self.shape, jnp.float32)]

    def scratch(self):
        half = self.shape[:-2] + (self.shape[-2] // 2, self.shape[-1])
        return [
            pltpu.VMEM((4,) + self.shape, jnp.bfloat16),
            pltpu.VMEM((4,) + self.shape, jnp.bfloat16),
            pltpu.VMEM((4,) + self.shape, jnp.bfloat16),
            pltpu.SemaphoreType.DMA((4,)),
            pltpu.VMEM((2,) + self.shape, jnp.bfloat16),
            pltpu.VMEM((2,) + half, jnp.bfloat16),
            pltpu.SemaphoreType.DMA((self.copies,)),
            pltpu.SemaphoreType.DMA((self.copies,)),
        ]

    def bind(self, ins, outs, scratch):
        (full_ref,), (out_ref,) = ins, outs
        from_core, pair, local, local_sem, whole, halves, send, recv = scratch
        (x, y, core), (to_x, to_y, to_core) = near()

        def copy(index, source, target, device):
            return pltpu.make_async_remote_copy(
                src_ref=source, dst_ref=target, send_sem=send.at[index], recv_sem=recv.at[index],
                device_id=device, device_id_type=MESH_ID,
            )

        place = lambda slot, at_core: part_of(full_ref, self.wide, 8, slot * 2 + at_core, FULL)
        own, at_x, at_y, at_far = x * 2 + y, (1 - x) * 2 + y, x * 2 + 1 - y, (1 - x) * 2 + 1 - y
        moves = [copy(slot, place(slot, 1 - core), from_core.at[slot], to_core) for slot in range(4)]
        moves += [
            copy(4, half_of(pair.at[at_far], TOP), halves.at[0], to_x),
            copy(5, half_of(pair.at[at_far], BOTTOM), halves.at[1], to_y),
            copy(6, pair.at[at_x], whole.at[0], to_x),
            copy(7, pair.at[at_y], whole.at[1], to_y),
        ]
        wide = lambda ref: ref[...].astype(jnp.float32)

        mine = [pltpu.make_async_copy(place(slot, core), local.at[slot], local_sem.at[slot]) for slot in range(4)]

        def begin():
            for slot in range(4):
                moves[slot].start()
                mine[slot].start()

        def second():
            for slot in range(4):
                moves[slot].wait_recv()
                mine[slot].wait()
                pair[slot] = (wide(local.at[slot]) + wide(from_core.at[slot])).astype(jnp.bfloat16)
            moves[4].start()
            moves[5].start()

        def third():
            moves[4].wait_recv()
            target = half_of(pair.at[at_y], TOP)
            target[...] = (wide(target) + wide(halves.at[0])).astype(jnp.bfloat16)
            moves[7].start()
            moves[5].wait_recv()
            target = half_of(pair.at[at_x], BOTTOM)
            target[...] = (wide(target) + wide(halves.at[1])).astype(jnp.bfloat16)
            moves[6].start()

        def last():
            moves[6].wait_recv()
            moves[7].wait_recv()
            out_ref[...] = wide(pair.at[own]) + wide(whole.at[0]) + wide(whole.at[1])
            for move in moves:
                move.wait_send()

        return begin, [second, third], last


class PlaneSum:
    line = False

    def __init__(self, shape):
        self.shape = shape

    def outs(self):
        return [(self.shape, jnp.float32)]

    def scratch(self):
        return [
            pltpu.VMEM((3,) + self.shape, jnp.float32),
            pltpu.VMEM((2,) + self.shape, jnp.float32),
            pltpu.SemaphoreType.DMA((3,)),
            pltpu.SemaphoreType.DMA((3,)),
        ]

    def bind(self, ins, outs, scratch):
        (value_ref,), (out_ref,) = ins, outs
        slots, totals, send, recv = scratch
        to_x, to_y, to_core = near()[1]
        moves = [
            pltpu.make_async_remote_copy(
                src_ref=source, dst_ref=slots.at[index], send_sem=send.at[index], recv_sem=recv.at[index],
                device_id=device, device_id_type=MESH_ID,
            )
            for index, (source, device) in enumerate(
                ((value_ref, to_core), (totals.at[0], to_y), (totals.at[1], to_x))
            )
        ]

        def begin():
            moves[0].start()

        def second():
            moves[0].wait_recv()
            totals[0] = value_ref[...] + slots[0]
            moves[1].start()

        def third():
            moves[1].wait_recv()
            totals[1] = totals[0] + slots[1]
            moves[2].start()

        def last():
            moves[2].wait_recv()
            out_ref[...] = totals[1] + slots[2]
            for move in moves:
                move.wait_send()

        return begin, [second, third], last


class LineSum:
    line = True

    def __init__(self, shape):
        self.shape = shape

    def outs(self):
        return [(self.shape, jnp.float32)]

    def scratch(self):
        return [
            pltpu.VMEM((4,) + self.shape, jnp.float32),
            pltpu.SemaphoreType.DMA((4,)),
            pltpu.SemaphoreType.DMA((4,)),
        ]

    def bind(self, ins, outs, scratch):
        (value_ref,), (out_ref,) = ins, outs
        slots, send, recv = scratch
        at = lax.axis_index(TENSOR)

        def copy(step, slot):
            return pltpu.make_async_remote_copy(
                src_ref=value_ref, dst_ref=slots.at[slot], send_sem=send.at[step], recv_sem=recv.at[slot],
                device_id={TENSOR: (at + step) % 4}, device_id_type=MESH_ID,
            )

        def begin():
            for step in range(1, 4):
                copy(step, at).start()
            slots[at] = value_ref[...]

        def last():
            for step in range(1, 4):
                copy(step, (at + step) % 4).wait_recv()
            out_ref[...] = slots[0] + slots[1] + slots[2] + slots[3]
            for step in range(1, 4):
                copy(step, at).wait_send()

        return begin, [lambda: None, lambda: None], last


def bind_all(tasks, ins, outs, scratch):
    begins, middles, lasts = [], [], []
    for task, task_in, task_out in zip(tasks, ins, outs):
        count = len(task.scratch())
        begin, steps, last = task.bind((task_in,), (task_out,), scratch[:count])
        scratch = scratch[count:]
        begins.append(begin)
        middles.append(steps)
        lasts.append(last)
    return begins, [step for turn in zip(*middles) for step in turn], lasts


def plane_call(cid, tasks, operands):
    vmem = pl.BlockSpec(memory_space=pltpu.VMEM)
    outs = [out for task in tasks for out in task.outs()]

    def kernel(*refs):
        n = len(tasks)
        greet(near()[1])
        begins, steps, lasts = bind_all(tasks, refs[:n], refs[n : 2 * n], refs[2 * n :])
        for step in begins + steps + lasts:
            step()

    return pl.pallas_call(
        kernel,
        out_shape=tuple(jax.ShapeDtypeStruct(shape, kind) for shape, kind in outs),
        in_specs=[vmem] * len(operands),
        out_specs=(vmem,) * len(outs),
        scratch_shapes=[piece for task in tasks for piece in task.scratch()],
        compiler_params=pltpu.CompilerParams(collective_id=cid, has_side_effects=True, vmem_limit_bytes=12 << 20),
        cost_estimate=pl.CostEstimate(flops=30_000_000_000, bytes_accessed=50_000_000, transcendentals=0),
        name=f"call_{cid}",
    )(*operands)


def line_sum(axis, partial_ref, acc_ref, from_end, from_mid, total_ref, send_sem, recv_sem, finish, others, whole_line, begins, steps, lasts):
    at = lax.axis_index(axis)
    low = at < 2
    end = jnp.where(low, 0, 3)
    mid = jnp.where(low, 1, 2)
    other = jnp.where(low, 2, 1)
    is_mid = at == mid
    rest = [{axis: (at + step) % 4} for step in range(1, 4)]
    size = partial_ref.shape[0] // CHUNKS

    gap = max((CHUNKS - LAG) // (len(steps) + 1), 1)

    def rows(chunk):
        return pl.ds(pl.multiple_of(chunk * size, size), size)

    def hop(stage, chunk, source, target, device):
        return pltpu.make_async_remote_copy(
            src_ref=source.at[rows(chunk)],
            dst_ref=target.at[rows(chunk)],
            send_sem=send_sem.at[stage, chunk],
            recv_sem=recv_sem.at[stage, chunk],
            device_id={axis: device},
            device_id_type=MESH_ID,
        )

    inward = lambda chunk: hop(0, chunk, partial_ref, from_end, mid)
    across = lambda chunk: hop(1, chunk, acc_ref, from_mid, other)
    outward = lambda chunk: hop(2, chunk, total_ref, total_ref, end)

    def loop(low, high, body):
        def step(chunk, carry):
            body(chunk)
            return carry

        lax.fori_loop(low, high, step, 0)

    def beside(chunk):
        for index, step in enumerate(steps):
            pl.when(chunk == LAG + gap * (1 + index))(step)

    @pl.when(is_mid)
    def _():
        greet((rest if whole_line else [{axis: end}, {axis: other}]) + others)
        for begin in begins:
            begin()

        def first(chunk):
            inward(chunk).wait_recv()
            here = rows(chunk)
            acc_ref[here] = (partial_ref[here].astype(jnp.float32) + from_end[here].astype(jnp.float32)).astype(acc_ref.dtype)
            across(chunk).start()

        def second(chunk):
            across(chunk).wait_recv()
            here = rows(chunk)
            total_ref[here] = (acc_ref[here].astype(jnp.float32) + from_mid[here].astype(jnp.float32)).astype(total_ref.dtype)
            outward(chunk).start()
            finish(here)

        def both(chunk):
            first(chunk)
            second(chunk - LAG)
            beside(chunk)

        loop(0, LAG, first)
        loop(LAG, CHUNKS, both)
        loop(CHUNKS - LAG, CHUNKS, second)

        def drain(chunk):
            across(chunk).wait_send()
            outward(chunk).wait_send()

        loop(0, CHUNKS, drain)

    @pl.when(jnp.logical_not(is_mid))
    def _():
        greet((rest if whole_line else [{axis: mid}]) + others)
        loop(0, CHUNKS, lambda chunk: inward(chunk).start())
        for begin in begins:
            begin()

        def receive(chunk):
            beside(chunk + LAG)
            outward(chunk).wait_recv()
            finish(rows(chunk))

        loop(0, CHUNKS, receive)
        loop(0, CHUNKS, lambda chunk: inward(chunk).wait_send())

    for last in lasts:
        last()


def unit_rows(rows_in):
    mean = jnp.mean(rows_in, axis=-1, keepdims=True)
    centred = rows_in - mean
    variance = jnp.mean(centred * centred, axis=-1, keepdims=True)
    inverse = lax.rsqrt(variance + epsilon)
    return centred * inverse, inverse


def rows_back(unit, inverse, scaled):
    return inverse * (
        scaled
        - jnp.mean(scaled, axis=-1, keepdims=True)
        - unit * jnp.mean(scaled * unit, axis=-1, keepdims=True)
    )


def gather_eight(value):
    total = value[:8]
    for at in range(8, value.shape[0], 8):
        total = total + value[at : at + 8]
    return total


def sum_call(body, cid, partial, operands, outs, tasks, task_operands):
    rows, width = partial.shape
    chunk_shape = pltpu.VMEM((rows, width), jnp.bfloat16)
    vmem = pl.BlockSpec(memory_space=pltpu.VMEM)
    far = [at for at, operand in enumerate(operands) if operand.shape[0] == rows]
    hbm = pl.BlockSpec(memory_space=pltpu.HBM)
    kinds = [hbm if at in far else vmem for at in range(len(operands))]
    task_outs = [out for task in tasks for out in task.outs()]
    grant = (56 if any(isinstance(task, Scatter) for task in tasks) else 22) << 20
    pieces = [piece for task in tasks for piece in task.scratch()]

    def kernel(partial_ref, *refs):
        def take(count):
            nonlocal refs
            taken, refs = refs[:count], refs[count:]
            return taken

        ins, task_ins = take(len(operands)), take(len(tasks))
        results, task_results = take(len(outs)), take(len(tasks))
        acc, from_end, from_mid, total, send_sem, recv_sem = take(6)
        copies, fetch_sem = take(len(far)), take(1)[0]
        fetches = [
            pltpu.make_async_copy(ins[at], held, fetch_sem.at[index]) for index, (at, held) in enumerate(zip(far, copies))
        ]
        for fetched in fetches:
            fetched.start()
        ins = [copies[far.index(at)] if at in far else ref for at, ref in enumerate(ins)]
        begins, steps, lasts, others = [], [], [], []
        if tasks:
            others = list(near()[1])
            begins, steps, lasts = bind_all(tasks, task_ins, task_results, refs)
        start, finish = body(total, ins, results)
        start()

        def arrive():
            for fetched in fetches:
                fetched.wait()

        begins.append(arrive)
        line_sum(
            TENSOR, partial_ref, acc, from_end, from_mid, total, send_sem, recv_sem, finish, others,
            any(task.line for task in tasks), begins, steps, lasts,
        )

    got = pl.pallas_call(
        kernel,
        out_shape=tuple(jax.ShapeDtypeStruct(shape, kind) for shape, kind in list(outs) + task_outs),
        in_specs=[vmem] + kinds + [hbm if isinstance(task, Scatter) else vmem for task in tasks],
        out_specs=(vmem,) * (len(outs) + len(tasks)),
        scratch_shapes=[chunk_shape] * 4
        + [pltpu.SemaphoreType.DMA((3, CHUNKS)), pltpu.SemaphoreType.DMA((3, CHUNKS))]
        + [pltpu.VMEM(operands[at].shape, operands[at].dtype) for at in far]
        + [pltpu.SemaphoreType.DMA((len(far),))]
        + pieces,
        compiler_params=pltpu.CompilerParams(collective_id=cid, has_side_effects=True, vmem_limit_bytes=grant),
        cost_estimate=pl.CostEstimate(flops=60_000_000_000, bytes_accessed=100_000_000, transcendentals=0),
        name=f"call_{cid}",
    )(partial, *operands, *task_operands)
    return got[: len(outs)], got[len(outs) :]


def forward_sum(cid, partial, rows_in, gain, scale, tasks=(), task_operands=()):
    def body(total, ins, results):
        x_ref, gain_ref = ins
        x_out, a_out = results

        def finish(here):
            x = x_ref[here].astype(jnp.float32) + scale * total[here].astype(jnp.float32)
            x_out[here] = x
            a_out[here] = (unit_rows(x)[0] * gain_ref[...]).astype(a_out.dtype)

        return lambda: None, finish

    shape = partial.shape
    return sum_call(
        body, cid, partial, (rows_in, gain.reshape(1, -1)),
        ((shape, jnp.float32), (shape, jnp.bfloat16)), tasks, task_operands,
    )


def turn_sum(cid, partial, rows_in, gain, cotangent):
    def body(total, ins, results):
        x_ref, gain_ref, cot_ref = ins
        out_ref, d_ref, half_ref, gain_grad_ref = results

        def start():
            gain_grad_ref[...] = jnp.zeros_like(gain_grad_ref)

        def finish(here):
            x = x_ref[here] + 0.5 * total[here].astype(jnp.float32)
            unit, inverse = unit_rows(x)
            out_ref[here] = (unit * gain_ref[...]).astype(out_ref.dtype)
            upstream = cot_ref[here].astype(jnp.float32)
            d = rows_back(unit, inverse, upstream * gain_ref[...])
            d_ref[here] = d
            half_ref[here] = (0.5 * d).astype(half_ref.dtype)
            gain_grad_ref[...] += gather_eight(upstream * unit)

        return start, finish

    shape = partial.shape
    (out, d, half, gain_grad), _ = sum_call(
        body, cid, partial, (rows_in, gain.reshape(1, -1), cotangent),
        ((shape, jnp.bfloat16), (shape, jnp.float32), (shape, jnp.bfloat16), ((8, shape[1]), jnp.float32)), (), (),
    )
    return out, d, half, gain_grad


def backward_sum(cid, partial, rows_in, gain, upstream, scale, tasks=(), task_operands=()):
    def body(total, ins, results):
        x_ref, gain_ref, up_ref = ins
        d_ref, half_ref, gain_grad_ref = results

        def start():
            gain_grad_ref[...] = jnp.zeros_like(gain_grad_ref)

        def finish(here):
            unit, inverse = unit_rows(x_ref[here].astype(jnp.float32))
            normed_grad = total[here].astype(jnp.float32)
            d = up_ref[here] + rows_back(unit, inverse, normed_grad * gain_ref[...])
            d_ref[here] = d
            half_ref[here] = (scale * d).astype(half_ref.dtype)
            gain_grad_ref[...] += gather_eight(normed_grad * unit)

        return start, finish

    shape = partial.shape
    return sum_call(
        body, cid, partial, (rows_in, gain.reshape(1, -1), upstream),
        ((shape, jnp.float32), (shape, jnp.bfloat16), ((8, shape[1]), jnp.float32)), tasks, task_operands,
    )


def context_places():
    along = lax.axis_index(CONTEXT)
    deep, core = along // 2, along % 2
    return deep, core, {CONTEXT: (1 - deep) * 2 + core}, {CONTEXT: deep * 2 + 1 - core}


def context_call(kernel, cid, operands, outs, scratch, ready=20_000_000_000, place=pltpu.VMEM):
    vmem = pl.BlockSpec(memory_space=pltpu.VMEM)
    return pl.pallas_call(
        kernel,
        out_shape=tuple(jax.ShapeDtypeStruct(shape, kind) for shape, kind in outs),
        in_specs=[pl.BlockSpec(memory_space=place)] * len(operands),
        out_specs=(vmem,) * len(outs),
        scratch_shapes=scratch,
        compiler_params=pltpu.CompilerParams(collective_id=cid, has_side_effects=True, vmem_limit_bytes=12 << 20),
        cost_estimate=pl.CostEstimate(flops=ready, bytes_accessed=30_000_000, transcendentals=0),
        name=f"call_{cid}",
    )(*operands)


def gather_context(cid, first, second):
    rows, width = first.shape

    def kernel(first_ref, second_ref, first_out, second_out, send, recv, own_sem):
        deep, core, to_y, to_core = context_places()
        greet([to_y, to_core])

        def block(ref, which):
            return ref.at[pl.ds(pl.multiple_of(which * rows, rows), rows)]

        def copy(index, source, target, device):
            return pltpu.make_async_remote_copy(
                src_ref=source, dst_ref=target, send_sem=send.at[index], recv_sem=recv.at[index],
                device_id=device, device_id_type=MESH_ID,
            )

        own, beyond = deep * 2 + core, (1 - deep) * 2 + core
        pairs = ((first_ref, first_out), (second_ref, second_out))
        out_y = [copy(i, source, block(full, own), to_y) for i, (source, full) in enumerate(pairs)]
        out_core = [copy(2 + i, source, block(full, own), to_core) for i, (source, full) in enumerate(pairs)]
        passed = [copy(4 + i, block(full, beyond), block(full, beyond), to_core) for i, (source, full) in enumerate(pairs)]
        mine = [pltpu.make_async_copy(source, block(full, own), own_sem.at[i]) for i, (source, full) in enumerate(pairs)]
        for move in out_y + out_core + mine:
            move.start()
        for arrived, onward in zip(out_y, passed):
            arrived.wait_recv()
            onward.start()
        for move in out_core + passed:
            move.wait_recv()
        for move in mine:
            move.wait()
        for move in out_y + out_core + passed:
            move.wait_send()

    full = ((4 * rows, width), first.dtype)
    return context_call(
        kernel, cid, (first, second), (full, full),
        [pltpu.SemaphoreType.DMA((6,)), pltpu.SemaphoreType.DMA((6,)), pltpu.SemaphoreType.DMA((2,))],
    )


def scatter_context(cid, first, second):
    rows, width = first.shape
    part = width // 4

    def kernel(first_ref, second_ref, first_out, second_out, from_core, pair, from_y, local, send, recv, local_sem):
        deep, core, to_y, to_core = context_places()
        greet([to_y, to_core])

        def block(ref, which):
            return ref.at[:, pl.ds(pl.multiple_of(which * part, 128), part)]

        def copy(index, source, target, device):
            return pltpu.make_async_remote_copy(
                src_ref=source, dst_ref=target, send_sem=send.at[index], recv_sem=recv.at[index],
                device_id=device, device_id_type=MESH_ID,
            )

        wide = lambda ref: ref[...].astype(jnp.float32)
        sources, targets = (first_ref, second_ref), (first_out, second_out)
        far, close = 1 - deep, deep
        inner, outer = [], []
        for i, source in enumerate(sources):
            for j, at in enumerate((far, close)):
                inner.append(copy(2 * i + j, block(source, at * 2 + 1 - core), from_core.at[2 * i + j], to_core))
            outer.append(copy(4 + i, pair.at[2 * i], from_y.at[i], to_y))
        mine = [
            pltpu.make_async_copy(block(source, at * 2 + core), local.at[2 * i + j], local_sem.at[2 * i + j])
            for i, source in enumerate(sources)
            for j, at in enumerate((far, close))
        ]
        for at in (0, 2, 1, 3):
            inner[at].start()
            mine[at].start()
        for i, source in enumerate(sources):
            inner[2 * i].wait_recv()
            mine[2 * i].wait()
            pair[2 * i] = (wide(local.at[2 * i]) + wide(from_core.at[2 * i])).astype(jnp.bfloat16)
            outer[i].start()
        for i, source in enumerate(sources):
            inner[2 * i + 1].wait_recv()
            mine[2 * i + 1].wait()
            pair[2 * i + 1] = (wide(local.at[2 * i + 1]) + wide(from_core.at[2 * i + 1])).astype(jnp.bfloat16)
        for i, target in enumerate(targets):
            outer[i].wait_recv()
            target[...] = (wide(pair.at[2 * i + 1]) + wide(from_y.at[i])).astype(target.dtype)
        for move in inner + outer:
            move.wait_send()

    out = ((rows, part), jnp.bfloat16)
    piece = (rows, part)
    return context_call(
        kernel, cid, (first, second), (out, out),
        [
            pltpu.VMEM((4,) + piece, jnp.bfloat16),
            pltpu.VMEM((4,) + piece, jnp.bfloat16),
            pltpu.VMEM((2,) + piece, jnp.bfloat16),
            pltpu.VMEM((4,) + piece, jnp.bfloat16),
            pltpu.SemaphoreType.DMA((6,)),
            pltpu.SemaphoreType.DMA((6,)),
            pltpu.SemaphoreType.DMA((4,)),
        ],
        place=pltpu.HBM,
    )


def line_total(cid, value):
    count = lax.axis_size(TENSOR)

    def kernel(value_ref, out_ref, slots, send, recv):
        at = lax.axis_index(TENSOR)
        others = [{TENSOR: (at + step) % count} for step in range(1, count)]
        greet(others)
        moves = [
            pltpu.make_async_remote_copy(
                src_ref=value_ref, dst_ref=slots.at[step], send_sem=send.at[step], recv_sem=recv.at[step],
                device_id=device, device_id_type=MESH_ID,
            )
            for step, device in enumerate(others)
        ]
        for move in moves:
            move.start()
        for move in moves:
            move.wait_recv()
        total = value_ref[...]
        for step in range(count - 1):
            total = total + slots[step]
        out_ref[...] = total
        for move in moves:
            move.wait_send()

    (total,) = context_call(
        kernel, cid, (value,), ((value.shape, jnp.float32),),
        [
            pltpu.VMEM((count - 1,) + value.shape, jnp.float32),
            pltpu.SemaphoreType.DMA((count - 1,)),
            pltpu.SemaphoreType.DMA((count - 1,)),
        ],
        5_000_000_000,
    )
    return total


def feed(normed, weight_in, weight_out):
    hidden = dot_rows(normed, weight_in)
    active = jax.nn.silu(hidden).astype(jnp.bfloat16)
    return dot_rows(active, weight_out).astype(jnp.bfloat16), (normed, hidden, active)


def feed_back(weight_in, weight_out, saved, branch_grad):
    normed, hidden, active = saved
    grad_out = dot_inner(active, branch_grad)
    unused, pullback = jax.vjp(jax.nn.silu, hidden)
    hidden_grad = pullback(dot_outer(branch_grad, weight_out))[0].astype(jnp.bfloat16)
    grad_in = dot_inner(normed, hidden_grad)
    return dot_outer(hidden_grad, weight_in).astype(jnp.bfloat16), grad_in, grad_out


QB = 128
BAND = 3 * QB
SPAN = 4 * QB
NT = (((1,), (1,)), ((), ()))


def span_table(relative):
    table = relative.astype(jnp.bfloat16)
    low = jnp.broadcast_to(table[:1], (2 * QB - 1 - LEFT, table.shape[1]))
    high = jnp.broadcast_to(table[-1:], (SPAN - (2 * QB - 1 - LEFT) - table.shape[0], table.shape[1]))
    spread = jnp.concatenate([low, table, high], axis=0)
    return jnp.concatenate([spread, spread], axis=1)


def fill_scores(first_block, q_mask, k_ref, span_ref, s_ref, edge_ref):
    keys = k_ref.shape[0]
    s_ref[:, QB : QB + keys] = lax.dot_general(q_mask, k_ref[...], NT, preferred_element_type=jnp.float32)
    spread = lax.dot_general(q_mask, span_ref[...], NT, preferred_element_type=jnp.float32)
    edge_ref[0] = jnp.broadcast_to(spread[:, :1], (QB, QB))
    edge_ref[1] = jnp.zeros((QB, QB), jnp.float32)
    edge_ref[2] = jnp.broadcast_to(spread[:, SPAN - 1 :], (QB, QB))
    skewed = pltpu.roll(spread, SPAN - (QB - 1), 1, stride=1, stride_axis=0)
    at = pl.ds(pl.multiple_of(first_block * QB, QB), BAND)
    s_ref[:, at] = s_ref[:, at] + skewed[:, :BAND]


def edge_of(block, first_block):
    return jnp.where(block < first_block - 1, 0, jnp.where(block > first_block + 1, 2, 1))


def forward_kernel(pos_ref, q_ref, k_ref, v_ref, span_ref, o_ref, lse_ref, s_ref, edge_ref, p_ref):
    keys = k_ref.shape[0]
    blocks = keys // QB
    first_block = pos_ref[0] * pl.num_programs(1) + pl.program_id(1)
    lane = lax.broadcasted_iota(jnp.int32, (QB, 2 * HEAD_DIM), 1)
    outs, lses = [], []
    for half in range(2):
        mine = (lane < HEAD_DIM) if half == 0 else (lane >= HEAD_DIM)
        q_mask = jnp.where(mine, q_ref[...], jnp.zeros_like(q_ref))
        fill_scores(first_block, q_mask, k_ref, span_ref, s_ref, edge_ref)
        top = None
        for block in range(blocks):
            z = s_ref[:, (block + 1) * QB : (block + 2) * QB] + edge_ref[edge_of(block, first_block)]
            top = z if top is None else jnp.maximum(top, z)
        top = jnp.max(top, axis=1, keepdims=True)
        edge_ref[...] = edge_ref[...] - top[None]
        total = None
        for block in range(blocks):
            z = s_ref[:, (block + 1) * QB : (block + 2) * QB] + edge_ref[edge_of(block, first_block)]
            p = jnp.exp(z)
            total = p if total is None else total + p
            p_ref[:, block * QB : (block + 1) * QB] = p.astype(jnp.bfloat16)
        total = jnp.sum(total, axis=1, keepdims=True)
        out = jnp.dot(p_ref[...], v_ref[...], preferred_element_type=jnp.float32) / total
        outs.append(out)
        lses.append(jnp.broadcast_to(top + jnp.log(total), (QB, 2 * HEAD_DIM)))
    low = lane < HEAD_DIM
    o_ref[...] = jnp.where(low, outs[0], outs[1]).astype(o_ref.dtype)
    lse_ref[...] = jnp.where(low, lses[0], lses[1])


def attention_forward(position, q, k, v, span):
    rows, width = q.shape
    keys = k.shape[0]
    pairs = width // (2 * HEAD_DIM)
    two = 2 * HEAD_DIM
    row_spec = pl.BlockSpec((QB, two), lambda p, b, pos: (b, p))
    key_spec = pl.BlockSpec((keys, two), lambda p, b, pos: (0, p))
    return pl.pallas_call(
        forward_kernel,
        out_shape=(
            jax.ShapeDtypeStruct((rows, width), jnp.bfloat16),
            jax.ShapeDtypeStruct((rows, width), jnp.float32),
        ),
        grid_spec=pltpu.PrefetchScalarGridSpec(
            num_scalar_prefetch=1,
            grid=(pairs, rows // QB),
            in_specs=[row_spec, key_spec, key_spec, pl.BlockSpec((SPAN, two), lambda p, b, pos: (0, 0))],
            out_specs=(row_spec, row_spec),
            scratch_shapes=[
                pltpu.VMEM((QB, keys + 2 * QB), jnp.float32),
                pltpu.VMEM((3, QB, QB), jnp.float32),
                pltpu.VMEM((QB, keys), jnp.bfloat16),
            ],
        ),
        compiler_params=pltpu.CompilerParams(vmem_limit_bytes=20 << 20),
        cost_estimate=pl.CostEstimate(flops=8 * rows * keys * width, bytes_accessed=4 * (keys + rows) * width, transcendentals=0),
        name="attention_forward",
    )(position.reshape(1), q, k, v, span)


def backward_kernel(pos_ref, q_ref, qt_ref, g_ref, gt_ref, o_ref, lse_ref, k_ref, v_ref, span_ref,
                    dq_ref, dkt_ref, dvt_ref, bins_ref, ends_ref,
                    s_ref, edge_ref, d_ref, p_ref, z_ref, wide_ref, dk_acc, dv_acc):
    keys = k_ref.shape[0]
    blocks = keys // QB
    step = pl.program_id(1)
    first_block = pos_ref[0] * pl.num_programs(1) + step
    lane = lax.broadcasted_iota(jnp.int32, (QB, 2 * HEAD_DIM), 1)

    @pl.when((pl.program_id(0) == 0) & (step == 0))
    def _():
        bins_ref[...] = jnp.zeros_like(bins_ref)
        ends_ref[...] = jnp.zeros_like(ends_ref)

    @pl.when(step == 0)
    def _():
        dk_acc[...] = jnp.zeros_like(dk_acc)
        dv_acc[...] = jnp.zeros_like(dv_acc)
        wide_ref[:, : 2 * HEAD_DIM] = k_ref[...]

    @pl.when((pl.program_id(0) == 0) & (step == 0))
    def _():
        z_ref[:, :QB] = jnp.zeros((QB, QB), jnp.bfloat16)
        z_ref[:, QB + keys :] = jnp.zeros((QB, QB), jnp.bfloat16)

    row_at = lax.broadcasted_iota(jnp.int32, (keys, QB), 0)
    col_at = lax.broadcasted_iota(jnp.int32, (keys, QB), 1)
    below = (row_at < (first_block - 1) * QB) & (col_at == 0)
    above = (row_at >= (first_block + 2) * QB) & (col_at == 1)
    wide_ref[:, 2 * HEAD_DIM :] = jnp.where(below | above, 1.0, 0.0).astype(jnp.bfloat16)

    flip_at = lax.broadcasted_iota(jnp.int32, (QB, QB), 0) + lax.broadcasted_iota(jnp.int32, (QB, QB), 1)
    flip = jnp.where(flip_at == QB - 1, 1.0, 0.0).astype(jnp.bfloat16)
    dqs = []
    for half in range(2):
        rows = slice(half * HEAD_DIM, (half + 1) * HEAD_DIM)
        mine = (lane < HEAD_DIM) if half == 0 else (lane >= HEAD_DIM)
        q_mask = jnp.where(mine, q_ref[...], jnp.zeros_like(q_ref))
        g_mask = jnp.where(mine, g_ref[...], jnp.zeros_like(g_ref))
        fill_scores(first_block, q_mask, k_ref, span_ref, s_ref, edge_ref)
        d_ref[...] = lax.dot_general(g_mask, v_ref[...], NT, preferred_element_type=jnp.float32)
        delta = jnp.sum(g_mask.astype(jnp.float32) * o_ref[...].astype(jnp.float32), axis=1, keepdims=True)
        lse = lse_ref[:, half * HEAD_DIM : half * HEAD_DIM + 1]
        edge_ref[...] = edge_ref[...] - lse[None]
        delta = jnp.broadcast_to(delta, (QB, QB))
        for block in range(blocks):
            here = slice(block * QB, (block + 1) * QB)
            there = slice((block + 1) * QB, (block + 2) * QB)
            p = jnp.exp(s_ref[:, there] + edge_ref[edge_of(block, first_block)])
            p_ref[:, here] = p.astype(jnp.bfloat16)
            z_ref[:, there] = (p * (d_ref[:, here] - delta)).astype(jnp.bfloat16)
        z_all = z_ref[:, QB : QB + keys]
        dv_acc[rows] += jnp.dot(gt_ref[rows], p_ref[...], preferred_element_type=jnp.float32)
        dk_acc[rows] += jnp.dot(qt_ref[rows], z_all, preferred_element_type=jnp.float32)
        dq = jnp.dot(z_all, wide_ref[...], preferred_element_type=jnp.float32)
        at = pl.ds(pl.multiple_of(first_block * QB, QB), BAND)
        band = jnp.dot(flip, z_ref[:, at], preferred_element_type=jnp.float32)
        band = jnp.concatenate([band, jnp.zeros((QB, SPAN - BAND), jnp.float32)], axis=1)
        spread = pltpu.roll(band, 0, 1, stride=1, stride_axis=0).astype(jnp.bfloat16)
        spread = jnp.dot(flip, spread, preferred_element_type=jnp.float32).astype(jnp.bfloat16)
        dq_rel = jnp.dot(spread, span_ref[...], preferred_element_type=jnp.float32)
        below_sum = dq[:, 2 * HEAD_DIM : 2 * HEAD_DIM + 1]
        above_sum = dq[:, 2 * HEAD_DIM + 1 : 2 * HEAD_DIM + 2]
        span_low = span_ref[:1, :].astype(jnp.float32)
        span_high = span_ref[SPAN - 1 :, :].astype(jnp.float32)
        dqs.append(dq[:, : 2 * HEAD_DIM] + dq_rel + below_sum * span_low + above_sum * span_high)
        bins_ref[...] += jnp.dot(qt_ref[rows], spread, preferred_element_type=jnp.float32)
        q_wide = q_mask.astype(jnp.float32)
        ends_ref[0:1, :] += jnp.sum(q_wide * below_sum, axis=0, keepdims=True)
        ends_ref[1:2, :] += jnp.sum(q_wide * above_sum, axis=0, keepdims=True)
    scale = 1.0 / 8.0
    dq_ref[...] = (jnp.where(lane < HEAD_DIM, dqs[0], dqs[1]) * scale).astype(dq_ref.dtype)

    @pl.when(step == pl.num_programs(1) - 1)
    def _():
        dkt_ref[...] = dk_acc[...].astype(dkt_ref.dtype)
        dvt_ref[...] = dv_acc[...].astype(dvt_ref.dtype)


def attention_backward(position, q, q_t, g, g_t, o, lse, k, v, span):
    rows, width = q.shape
    keys = k.shape[0]
    pairs = width // (2 * HEAD_DIM)
    two = 2 * HEAD_DIM
    row_spec = pl.BlockSpec((QB, two), lambda p, b, pos: (b, p))
    col_spec = pl.BlockSpec((two, QB), lambda p, b, pos: (p, b))
    key_spec = pl.BlockSpec((keys, two), lambda p, b, pos: (0, p))
    keyt_spec = pl.BlockSpec((two, keys), lambda p, b, pos: (p, 0))
    fixed = lambda shape: pl.BlockSpec(shape, lambda p, b, pos: (0, 0))
    dq, dkt, dvt, bins, ends = pl.pallas_call(
        backward_kernel,
        out_shape=(
            jax.ShapeDtypeStruct((rows, width), jnp.bfloat16),
            jax.ShapeDtypeStruct((width, keys), jnp.bfloat16),
            jax.ShapeDtypeStruct((width, keys), jnp.bfloat16),
            jax.ShapeDtypeStruct((HEAD_DIM, SPAN), jnp.float32),
            jax.ShapeDtypeStruct((8, two), jnp.float32),
        ),
        grid_spec=pltpu.PrefetchScalarGridSpec(
            num_scalar_prefetch=1,
            grid=(pairs, rows // QB),
            in_specs=[row_spec, col_spec, row_spec, col_spec, row_spec, row_spec, key_spec, key_spec, fixed((SPAN, two))],
            out_specs=(row_spec, keyt_spec, keyt_spec, fixed((HEAD_DIM, SPAN)), fixed((8, two))),
            scratch_shapes=[
                pltpu.VMEM((QB, keys + 2 * QB), jnp.float32),
                pltpu.VMEM((3, QB, QB), jnp.float32),
                pltpu.VMEM((QB, keys), jnp.float32),
                pltpu.VMEM((QB, keys), jnp.bfloat16),
                pltpu.VMEM((QB, keys + 2 * QB), jnp.bfloat16),
                pltpu.VMEM((keys, 2 * two), jnp.bfloat16),
                pltpu.VMEM((two, keys), jnp.float32),
                pltpu.VMEM((two, keys), jnp.float32),
            ],
        ),
        compiler_params=pltpu.CompilerParams(vmem_limit_bytes=20 << 20),
        cost_estimate=pl.CostEstimate(flops=20 * rows * keys * width, bytes_accessed=8 * (keys + rows) * width, transcendentals=0),
        name="attention_backward",
    )(position.reshape(1), q, q_t, g, g_t, o, lse, k, v, span)
    at = 2 * QB - 1 - LEFT
    ends = ends[:2, :HEAD_DIM] + ends[:2, HEAD_DIM:]
    spread = bins.T
    inner = spread[at + 1 : at + LEFT + RIGHT]
    low = jnp.sum(spread[: at + 1], axis=0) + ends[0]
    high = jnp.sum(spread[at + LEFT + RIGHT :], axis=0) + ends[1]
    table = jnp.concatenate([low[None], inner, high[None]], axis=0)
    return dq, dkt, dvt, table


def attend_forward(normed, weight_in, weight_out, relative, position):
    projected = jnp.einsum(
        "td,kde->kte", normed, weight_in, preferred_element_type=jnp.float32
    ).astype(jnp.bfloat16)
    key_rows, value_rows = gather_context(10, projected[1], projected[2])
    queries = projected[0] * jnp.bfloat16(1.0 / math.sqrt(HEAD_DIM))
    span = span_table(relative)
    mixed, log_total = attention_forward(position, queries, key_rows, value_rows, span)
    return (
        dot_rows(mixed, weight_out).astype(jnp.bfloat16),
        (normed, queries, key_rows, value_rows, log_total, mixed, span),
    )


def attend_backward(weight_in, weight_out, position, saved, branch_grad):
    normed, queries, key_rows, value_rows, log_total, mixed, span = saved
    grad_out = dot_inner(mixed, branch_grad)
    mixed_grad = dot_outer(branch_grad, weight_out).astype(jnp.bfloat16)
    query_grad, key_grad, value_grad, table_grad = attention_backward(
        position, queries, queries.T, mixed_grad, mixed_grad.T, mixed, log_total, key_rows, value_rows, span
    )
    key_grad, value_grad = scatter_context(11, key_grad, value_grad)
    stacked = jnp.stack([query_grad, key_grad.T, value_grad.T])
    grad_in = jnp.einsum("td,kte->kde", normed, stacked, preferred_element_type=jnp.float32)
    partial_sum = jnp.einsum("kte,kde->td", stacked, weight_in, preferred_element_type=jnp.float32)
    return (partial_sum.astype(jnp.bfloat16), table_grad, grad_in, grad_out)


TILE = 64


def sliding(ext_ref, tile, lanes):
    window = ext_ref[pl.ds(pl.multiple_of(tile * TILE, TILE), TILE + 32), lanes]
    for low in range(8):
        moved = window[low : low + TILE + 24]
        for high in range(0, 31 - low, 8):
            yield high + low, moved[high : high + TILE]


def tile_loop(rows, width, body):
    def step(tile, carry):
        for at in range(0, width, 128):
            body(tile, slice(at, at + 128))
        return carry

    lax.fori_loop(0, rows // TILE, step, 0)


def extended(before, rows, after):
    pad = -(before.shape[0] + after.shape[0]) % 32
    return jnp.concatenate([before, rows, after, jnp.zeros((pad, rows.shape[1]), rows.dtype)], axis=0)


def depth_forward(ext, depthwise):
    rows, width = ext.shape[0] - 32, ext.shape[1]

    def kernel(ext_ref, depth_ref, out_ref):
        def body(tile, lanes):
            total = None
            for distance, part in sliding(ext_ref, tile, lanes):
                term = depth_ref[distance : distance + 1, lanes] * part
                total = term if total is None else total + term
            out_ref[pl.ds(pl.multiple_of(tile * TILE, TILE), TILE), lanes] = total

        tile_loop(rows, width, body)

    vmem = pl.BlockSpec(memory_space=pltpu.VMEM)
    return pl.pallas_call(
        kernel,
        out_shape=jax.ShapeDtypeStruct((rows, width), jnp.float32),
        in_specs=[vmem] * 2,
        out_specs=vmem,
        compiler_params=pltpu.CompilerParams(vmem_limit_bytes=6 << 20),
        cost_estimate=pl.CostEstimate(flops=1_000_000_000, bytes_accessed=2_000_000, transcendentals=0),
    )(ext, depthwise)


def depth_backward(grad_ext, ext, depthwise):
    rows, width = ext.shape[0] - 32, ext.shape[1]
    reach = depthwise.shape[0] - 1

    def kernel(grad_ref, ext_ref, depth_ref, out_ref, depth_out, sums):
        sums[...] = jnp.zeros_like(sums)

        def body(tile, lanes):
            here = pl.ds(pl.multiple_of(tile * TILE, TILE), TILE)
            total = None
            for distance, part in sliding(grad_ref, tile, lanes):
                term = depth_ref[reach - distance : reach - distance + 1, lanes] * part
                total = term if total is None else total + term
            out_ref[here, lanes] = total
            grad = grad_ref[here, lanes]
            for distance, part in sliding(ext_ref, tile, lanes):
                sums[distance, :, lanes] += gather_eight(grad * part)

        tile_loop(rows, width, body)
        for distance in range(reach + 1):
            depth_out[distance : distance + 1] = jnp.sum(sums[distance], axis=0, keepdims=True)

    vmem = pl.BlockSpec(memory_space=pltpu.VMEM)
    return pl.pallas_call(
        kernel,
        out_shape=(
            jax.ShapeDtypeStruct((rows, width), jnp.float32),
            jax.ShapeDtypeStruct(depthwise.shape, jnp.float32),
        ),
        in_specs=[vmem] * 3,
        out_specs=(vmem, vmem),
        scratch_shapes=[pltpu.VMEM((reach + 1, 8, width), jnp.float32)],
        compiler_params=pltpu.CompilerParams(vmem_limit_bytes=8 << 20),
        cost_estimate=pl.CostEstimate(flops=2_000_000_000, bytes_accessed=4_000_000, transcendentals=0),
    )(grad_ext, ext, depthwise)


def channel_sums(cid, first, second):
    total = line_total(cid, jnp.concatenate([first, second]).reshape(-1, 128)).reshape(2, -1)
    return total[0], total[1]


def conv_forward(normed, weight_in, weight_out, depthwise, gain_middle):
    projected = jnp.einsum("td,kde->kte", normed, weight_in, preferred_element_type=jnp.float32)
    gated = gate_unit(projected[0], projected[1])
    rows_here = gated.shape[0]
    reach_rows = depthwise.shape[0] - 1
    edge_rows = shifted_2(gated[rows_here - reach_rows :], CONTEXT, 1)
    padded = extended(edge_rows, gated, gated[:0])
    mixed = depth_forward(padded, depthwise)
    row_sums, row_squares = channel_sums(12, jnp.sum(mixed, axis=1), jnp.sum(mixed * mixed, axis=1))
    row_mean = row_sums / D
    inverse = lax.rsqrt(row_squares / D - row_mean * row_mean + epsilon)
    scaled = (mixed - row_mean[:, None]) * inverse[:, None]
    shaped = scaled * gain_middle
    active = jax.nn.silu(shaped).astype(jnp.bfloat16)
    return (
        dot_rows(active, weight_out).astype(jnp.bfloat16),
        (normed, projected, padded, scaled, inverse, shaped, active),
    )


def conv_backward(weight_in, weight_out, depthwise, gain_middle, saved, branch_grad):
    normed, projected, padded, scaled, inverse, shaped, active = saved
    reach_rows = depthwise.shape[0] - 1
    grad_out = dot_inner(active, branch_grad)
    unused, pullback = jax.vjp(jax.nn.silu, shaped)
    shaped_grad = pullback(dot_outer(branch_grad, weight_out))[0]
    middle_grad = jnp.sum(shaped_grad * scaled, axis=0)
    scaled_grad = shaped_grad * gain_middle
    first_sum, second_sum = channel_sums(13, jnp.sum(scaled_grad, axis=1), jnp.sum(scaled_grad * scaled, axis=1))
    mixed_grad = inverse[:, None] * (
        scaled_grad - first_sum[:, None] / D - scaled * (second_sum[:, None] / D)
    )
    next_rows = shifted_2(mixed_grad[:reach_rows], CONTEXT, -1)
    gated_grad, depth_grad = depth_backward(extended(mixed_grad[:0], mixed_grad, next_rows), padded, depthwise)
    unused, pullback = jax.vjp(gate_unit, projected[0], projected[1])
    unit_grad, gate_grad = pullback(gated_grad)
    stacked = jnp.stack([unit_grad, gate_grad]).astype(jnp.bfloat16)
    grad_in = jnp.einsum("td,kte->kde", normed, stacked, preferred_element_type=jnp.float32)
    partial_sum = jnp.einsum("kte,kde->td", stacked, weight_in, preferred_element_type=jnp.float32)
    return (partial_sum.astype(jnp.bfloat16), grad_in, grad_out, middle_grad, depth_grad)


def local(
    inputs,
    gain_first,
    first_in,
    first_out,
    gain_attend,
    attend_in,
    attend_out,
    relative,
    gain_convolve,
    convolve_in,
    depthwise,
    gain_middle,
    convolve_out,
    gain_second,
    second_in,
    second_out,
    gain_final,
    cotangent,
):
    position = lax.axis_index(CONTEXT)
    start_rows = inputs[0]
    small_plane = lax.axis_size(CLIPS) == 2
    weights = {
        FIRST: (first_in, first_out),
        ATTEND: (attend_in, attend_out),
        CONVOLVE: (convolve_in, convolve_out),
        SECOND: (second_in, second_out),
    }
    held, grads = {}, {}

    def collecting(name):
        if not small_plane:
            return (), ()
        pair = tuple(weight.astype(jnp.bfloat16) for weight in weights[name])
        return tuple(Gather(wide, weight.shape) for wide, weight in zip((False, True), pair)), pair

    def collect(name, gathered):
        held[name] = gathered if small_plane else fetch(*weights[name])

    def spreading(*sums):
        if not small_plane:
            return (), ()
        sums = tuple(grad.astype(jnp.bfloat16) for grad in sums)
        return tuple(Scatter(at % 2 == 1, grad.shape) for at, grad in enumerate(sums)), sums

    def with_small(rest, kind, *values):
        if not small_plane:
            return rest
        return rest[0] + tuple(kind(value.shape) for value in values), rest[1] + values

    def spread(name, scattered, grad_in, grad_out):
        grads[name] = scattered if small_plane else send_grads(grad_in, grad_out)

    tasks, pair = collecting(FIRST)
    collect(FIRST, plane_call(9, tasks, pair) if small_plane else None)
    normed = layer_norm(start_rows.astype(jnp.float32), gain_first).astype(jnp.bfloat16)
    branch, first_saved = feed(normed, *held[FIRST])
    (after_first, normed), got = forward_sum(1, branch, start_rows, gain_attend, 0.5, *collecting(ATTEND))
    collect(ATTEND, got)
    branch, attend_saved = attend_forward(normed, *held[ATTEND], relative, position)
    (after_attend, normed), got = forward_sum(2, branch, after_first, gain_convolve, 1.0, *collecting(CONVOLVE))
    collect(CONVOLVE, got)
    branch, convolve_saved = conv_forward(normed, *held[CONVOLVE], depthwise, gain_middle)
    (after_convolve, normed), got = forward_sum(3, branch, after_attend, gain_second, 1.0, *collecting(SECOND))
    collect(SECOND, got)
    branch, second_saved = feed(normed, *held[SECOND])
    final_out, upstream, branch_grad, grad_final = turn_sum(4, branch, after_convolve, gain_final, cotangent[0])
    branch, *second_pair = feed_back(*held[SECOND], second_saved, branch_grad)
    (upstream, branch_grad, grad_gain_second), _ = backward_sum(
        5, branch, after_convolve, gain_second, upstream, 1.0
    )
    branch, *convolve_pair, grad_middle, grad_depth = conv_backward(
        *held[CONVOLVE], depthwise, gain_middle, convolve_saved, branch_grad
    )
    (upstream, branch_grad, grad_gain_convolve), got = backward_sum(
        6, branch, after_attend, gain_convolve, upstream, 1.0, *spreading(*second_pair)
    )
    spread(SECOND, got, *second_pair)
    branch, table_grad, *pair = attend_backward(*held[ATTEND], position, attend_saved, branch_grad)
    (upstream, branch_grad, grad_gain_attend), got = backward_sum(
        7, branch, after_first, gain_attend, upstream, 0.5, *with_small(spreading(*convolve_pair, *pair), LineSum, table_grad)
    )
    spread(CONVOLVE, got[:2], *convolve_pair)
    spread(ATTEND, got[2:4], *pair)
    branch, *pair = feed_back(*held[FIRST], first_saved, branch_grad)
    gains = [
        jnp.sum(part, axis=0) for part in (grad_gain_attend, grad_gain_convolve, grad_gain_second, grad_final)
    ]
    if small_plane:
        table_grad = got[4]
    gains = jnp.concatenate([*gains, grad_middle, jnp.zeros((768,), jnp.float32)]).reshape(-1, 128)
    smalls = (gains, grad_depth, table_grad)
    (upstream, branch_grad, grad_gain_first), got = backward_sum(
        8, branch, start_rows, gain_first, upstream, 1.0, *with_small(spreading(*pair), PlaneSum, *smalls)
    )
    spread(FIRST, got[:2], *pair)
    grad_gain_first = jnp.sum(grad_gain_first, axis=0)
    if small_plane:
        gains, grad_depth, table_grad = got[2:]
        (grad_gain_first,) = plane_call(14, (PlaneSum((8, 128)),), (grad_gain_first.reshape(8, 128),))
        grad_gain_first = grad_gain_first.reshape(-1)
    else:
        table_grad = lax.psum(table_grad, (CLIPS, CONTEXT, TENSOR))
        gains, grad_depth, grad_gain_first = lax.psum((gains, grad_depth, grad_gain_first), (CLIPS, CONTEXT))
    smalls = [gains[8 * at : 8 * at + 8].reshape(-1) for at in range(4)] + [gains[32:34].reshape(-1)]
    return (
        final_out[None],
        upstream[None],
        grad_gain_first,
        grads[FIRST][0],
        grads[FIRST][1],
        smalls[0],
        grads[ATTEND][0],
        grads[ATTEND][1],
        table_grad,
        smalls[1],
        grads[CONVOLVE][0],
        grad_depth,
        smalls[4],
        grads[CONVOLVE][1],
        smalls[2],
        grads[SECOND][0],
        grads[SECOND][1],
        smalls[3],
    )


def solution(mesh):
    placed = (
        P(CLIPS, CONTEXT, None),
        P(),
        P((CLIPS, CONTEXT), TENSOR),
        P(TENSOR, (CLIPS, CONTEXT)),
        P(),
        P(None, (CLIPS, CONTEXT), TENSOR),
        P(TENSOR, (CLIPS, CONTEXT)),
        P(),
        P(),
        P(None, (CLIPS, CONTEXT), TENSOR),
        P(None, TENSOR),
        P(TENSOR),
        P(TENSOR, (CLIPS, CONTEXT)),
        P(),
        P((CLIPS, CONTEXT), TENSOR),
        P(TENSOR, (CLIPS, CONTEXT)),
        P(),
        P(CLIPS, CONTEXT, None),
    )
    return jax.shard_map(
        local,
        mesh=mesh,
        in_specs=placed,
        out_specs=(
            P(CLIPS, CONTEXT, None),
            P(CLIPS, CONTEXT, None),
            P(),
            P((CLIPS, CONTEXT), TENSOR),
            P(TENSOR, (CLIPS, CONTEXT)),
            P(),
            P(None, (CLIPS, CONTEXT), TENSOR),
            P(TENSOR, (CLIPS, CONTEXT)),
            P(),
            P(),
            P(None, (CLIPS, CONTEXT), TENSOR),
            P(None, TENSOR),
            P(TENSOR),
            P(TENSOR, (CLIPS, CONTEXT)),
            P(),
            P((CLIPS, CONTEXT), TENSOR),
            P(TENSOR, (CLIPS, CONTEXT)),
            P(),
        ),
        check_vma=False,
    )
```
